128 devices in a mesh: dp: 32 (over x, y, core), mp: 4 (over z).
Axes of the slice: x: 4, y: 4, z: 4, core: 2. Of those that a mesh axis runs over, the one named last changes fastest.
Arguments:
- slab_values: bfloat16 [128, 128, 2048], P(('dp', 'mp')), may hold values from -6 to 6
- row_ids: int32 [128, 128, 32], P(('dp', 'mp')), may hold values from 0 to 4095, as said below
- peer_counts: int32 [128, 128], P(('dp', 'mp')), may hold values from 1 to 32, as said below
- lookup_slots: int32 [32768, 16], P(('dp', 'mp')), may hold values from 0 to 4095, as said below
- labels: int32 [32768], P('dp'), may hold values 0 or 1
- sample_weight: float32 [32768], P('dp'), may hold values from 0.3 to 9
- weight_in: bfloat16 [1024, 8192], P(None, 'mp'), may hold values from -0.1875 to 0.1875
- bias_in: float32 [8192], P('mp'), may hold values from -3 to 3
- weight_out: bfloat16 [8192], P('mp'), may hold values from -0.0625 to 0.0625
- dense_accum: float32 [1024, 8192], P('dp', 'mp'), may hold values from 1e-08 to 1e-06
- table_rows: float32 [524288, 64], P(('dp', 'mp')), may hold values from -0.12 to 0.12
- table_accum: float32 [524288], P(('dp', 'mp')), may hold values from 1e-12 to 1e-05
Outputs:
- weight_new: bfloat16 [1024, 8192], P(None, 'mp')
- accum_new: float32 [1024, 8192], P('dp', 'mp')
- table_new: float32 [524288, 64], P(('dp', 'mp'))
- table_accum_new: float32 [524288], P(('dp', 'mp'))
The draws below stay inside these ranges and needn't reach their ends.
Inputs may be any that keep to these rules, and one draw needn't show every extreme that they name: `row_ids`: the first peer_counts entries of each device's list for an owner are distinct rows of that owner's shard. `peer_counts`: some owner has 32 touched rows on every device, and some device has 32 touched rows of every owner. `lookup_slots`: below the sum of that device's peer_counts; every device has a lookup of its last touched row.
All inputs are finite; a program needn't handle non-finite values. No bound on the sum of `labels` on one device may be relied on, other than what follows from the above.
Results may differ from the reference program's by a relative error of at most 0.0034.
Values may be sent and summed in bfloat16 or wider, within the bound.
A program may use at most 128 MiB of HBM per device.

```python
import math
import jax
import jax.numpy as jnp
from jax import lax

D_EMB = 64
NF = 16
H = 8192
B_DEV = 256
CAP = 32
ROWS_OWN = 4096
K = 1024
PEERS = 128
SAMPLES = 32768
TABLE_ROWS = 524288
N_DP = 32
N_MP = 4


def count_table(key):
    base = jax.random.fold_in(key, 7)
    counts = jax.random.randint(jax.random.fold_in(base, 1), (PEERS, PEERS), max(1, CAP // 4), CAP + 1)
    hot_owner = jax.random.randint(jax.random.fold_in(base, 2), (), 0, PEERS)
    full_device = jax.random.randint(jax.random.fold_in(base, 3), (), 0, PEERS)
    column = jnp.arange(PEERS)[None, :]
    row_number = jnp.arange(PEERS)[:, None]
    counts = jnp.where(column == hot_owner, CAP, counts)
    counts = jnp.where(row_number == full_device, CAP, counts)
    return counts.astype(jnp.int32)


def draw_peer_counts(key, part):
    return count_table(key)


def draw_lookup_slots(key, part):
    counts = count_table(key)
    live = jnp.sum(counts, axis=1)
    raw_draw = jax.random.randint(jax.random.fold_in(key, 11), (SAMPLES, NF), 0, 2 ** 30)
    device = jnp.arange(SAMPLES) // B_DEV
    within = jnp.arange(SAMPLES) % B_DEV
    drawn = raw_draw % live[device][:, None]
    chosen_sample = jax.random.randint(jax.random.fold_in(key, 19), (PEERS,), 0, B_DEV)
    chosen_feature = jax.random.randint(jax.random.fold_in(key, 23), (PEERS,), 0, NF)
    marked = (within == chosen_sample[device])[:, None] & (jnp.arange(NF)[None, :] == chosen_feature[device][:, None])
    return jnp.where(marked, live[device][:, None] - 1, drawn).astype(jnp.int32)


def draw_row_ids(key, part):
    stride = ROWS_OWN // CAP
    offsets = jax.random.randint(jax.random.fold_in(key, 13), (PEERS, PEERS, CAP), 0, stride)
    return (jnp.arange(CAP)[None, None, :] * stride + offsets).astype(jnp.int32)


def draw_sample_weight(key, part):
    position = jnp.arange(SAMPLES).astype(jnp.float32) / SAMPLES
    rising = 1.0 + 2.0 * position
    level = jax.random.uniform(jax.random.fold_in(key, 17), (SAMPLES,), jnp.float32, 0.5, 1.5)
    return (rising * level).astype(jnp.float32)


def with_ends(values, own_key, low, largest):
    spot = [jax.random.randint(jax.random.fold_in(own_key, axis), (), 0, length) for axis, length in enumerate(values.shape)]
    longest = values.shape.index(max(values.shape))
    beside = spot[:longest] + [(spot[longest] + 1) % values.shape[longest]] + spot[longest + 1:]
    return values.at[tuple(spot)].set(low).at[tuple(beside)].set(largest)


def shard_levels(key, dims, split, smallest, high):
    level = 1.0
    for dim, blocks in split:
        steps = jax.random.uniform(jax.random.fold_in(jax.random.fold_in(key, 6), dim), (blocks,), jnp.float32, smallest / len(split), high / len(split))
        level = level * jnp.repeat(jnp.exp(steps), dims[dim] // blocks).reshape((-1,) + (1,) * (len(dims) - 1 - dim))
    return level


def gaussian(key, extent, deviation, reach, split=(), kind=jnp.bfloat16):
    loudness = shard_levels(key, extent, split, -0.22, 0.18) if split else 1.0
    result = jax.random.normal(key, extent, jnp.float32) * deviation * loudness
    return jnp.minimum(jnp.maximum(result, -reach), reach).astype(kind)


def setup_inputs(seed: int = 0) -> dict:
    seeds = jax.random.split(jax.random.key(seed), 13)
    return {
        "slab_values": gaussian(seeds[0], (PEERS, PEERS, CAP * D_EMB), 1.0, 6.0, ((0, 128),)),
        "row_ids": draw_row_ids(jax.random.fold_in(seeds[12], 71), 0),
        "peer_counts": draw_peer_counts(jax.random.fold_in(seeds[12], 71), 0),
        "lookup_slots": draw_lookup_slots(jax.random.fold_in(seeds[12], 71), 0),
        "labels": with_ends((jax.random.randint(seeds[4], (SAMPLES,), 0, 4) < 1).astype(jnp.int32), jax.random.fold_in(seeds[4], 1), 0, 1),
        "sample_weight": draw_sample_weight(jax.random.fold_in(seeds[12], 71), 0),
        "weight_in": gaussian(seeds[6], (K, H), K ** -0.5, 0.1875, ((1, 4),)),
        "bias_in": gaussian(seeds[7], (H,), 0.5, 3.0, ((0, 4),), jnp.float32),
        "weight_out": gaussian(seeds[8], (H,), H ** -0.5, 0.0625, ((0, 4),)),
        "dense_accum": jnp.clip(jnp.exp(math.log(9.999999974752427e-07) - 4.6051702 * jax.random.uniform(seeds[9], (K, H), jnp.float32) ** shard_levels(seeds[9], (K, H), ((0, 32), (1, 4)), -0.2, 0.2)), 9.99999993922529e-09, 9.999999974752427e-07),
        "table_rows": gaussian(seeds[10], (TABLE_ROWS, D_EMB), 0.02, 0.12, ((0, 128),), jnp.float32),
        "table_accum": jnp.clip(jnp.exp(math.log(9.999999747378752e-06) - 16.118096 * jax.random.uniform(seeds[11], (TABLE_ROWS,), jnp.float32) ** shard_levels(seeds[11], (TABLE_ROWS,), ((0, 128),), -0.2, 0.2)), 9.999999960041972e-13, 9.999999747378752e-06),
    }


clip_norm = 1.0
dense_rate = 0.02
table_rate = 0.5
adagrad_eps = 1e-10

def slot_index(compact, counts, capacity):
    slot_ends = jnp.cumsum(counts)
    owner_index = lax.optimization_barrier(jnp.sum((compact[..., None] >= slot_ends).astype(jnp.int32), axis=-1))
    slot_starts = slot_ends - counts
    owner_match = owner_index[..., None] == jnp.arange(counts.shape[0], dtype=jnp.int32)
    owner_begin = lax.optimization_barrier(jnp.sum(jnp.where(owner_match, slot_starts, 0), axis=-1))
    return (owner_index * capacity + compact - owner_begin).astype(jnp.int32)

def reference(slab_values, row_ids, peer_counts, lookup_slots, labels, sample_weight, weight_in, bias_in, weight_out, dense_accum, table_rows, table_accum):
    group_rows = N_MP * B_DEV
    slabs = slab_values.reshape(N_DP, N_MP, PEERS * CAP, D_EMB)
    counts = peer_counts.reshape(N_DP, N_MP, PEERS)
    slots = lookup_slots.reshape(N_DP, N_MP, B_DEV, NF)
    targets = labels.astype(jnp.float32).reshape(N_DP, group_rows)
    weights = sample_weight.reshape(N_DP, group_rows)

    def group_step(carry, inputs):
        grad_in, grad_bias, grad_out = carry
        slab, count, slot, target, weight = inputs

        def pool(one_slab, one_count, one_slot):
            index = slot_index(one_slot, one_count, CAP)
            return (one_slab[index].reshape(B_DEV, K), index)
        pooled, index = jax.vmap(pool)(slab, count, slot)
        pooled = pooled.reshape(group_rows, K)
        act = jnp.dot(pooled, weight_in, preferred_element_type=jnp.float32) + bias_in
        hidden = jax.nn.silu(act).astype(jnp.bfloat16)
        logit = jnp.dot(hidden, weight_out, preferred_element_type=jnp.float32)
        dlogit = weight * (jax.nn.sigmoid(logit) - target)
        sigma = jax.nn.sigmoid(act)
        dact = (dlogit[:, None] * weight_out.astype(jnp.float32)[None, :] * sigma * (1.0 + act * (1.0 - sigma))).astype(jnp.bfloat16)
        grad_in = grad_in + lax.dot_general(pooled, dact, (((0,), (0,)), ((), ())), preferred_element_type=jnp.float32)
        grad_bias = grad_bias + lax.optimization_barrier(jnp.sum(dact.astype(jnp.float32), axis=0))
        grad_out = grad_out + jnp.dot(dlogit, hidden.astype(jnp.float32), precision=lax.Precision.HIGHEST)
        dpooled = lax.dot_general(dact, weight_in, (((1,), (1,)), ((), ())), preferred_element_type=jnp.float32)
        pieces = dpooled.reshape(N_MP, B_DEV * NF, D_EMB)

        def gather_slots(piece, one_index):
            return jax.ops.segment_sum(piece, one_index.reshape(-1), num_segments=PEERS * CAP)
        slot_grad = jax.vmap(gather_slots)(pieces, index)
        return ((grad_in, grad_bias, grad_out), slot_grad)
    start = (jnp.zeros((K, H), jnp.float32), jnp.zeros((H,), jnp.float32), jnp.zeros((H,), jnp.float32))
    (grad_in, grad_bias, grad_out), slot_grad = lax.scan(group_step, start, (slabs, counts, slots, targets, weights))
    slot_grad = slot_grad.reshape(PEERS, PEERS * CAP, D_EMB)
    total = jnp.sum(grad_in * grad_in) + jnp.sum(grad_bias * grad_bias) + jnp.sum(grad_out * grad_out) + jnp.sum(slot_grad * slot_grad)
    scale = clip_norm / jnp.maximum(jnp.sqrt(total), clip_norm)
    clipped = scale * grad_in
    accum_new = dense_accum + clipped * clipped
    weight_new = (weight_in.astype(jnp.float32) - dense_rate * clipped / (jnp.sqrt(accum_new) + adagrad_eps)).astype(jnp.bfloat16)
    owners = jnp.arange(PEERS, dtype=jnp.int32)[None, :, None]
    global_rows = (owners * ROWS_OWN + row_ids).reshape(-1)
    received = scale * jax.ops.segment_sum(slot_grad.reshape(-1, D_EMB), global_rows, num_segments=TABLE_ROWS)
    table_accum_new = table_accum + lax.optimization_barrier(jnp.mean(received * received, axis=1))
    table_new = table_rows - table_rate * received / (jnp.sqrt(table_accum_new)[:, None] + adagrad_eps)
    return (weight_new, accum_new, table_new, table_accum_new)
```

```python
import functools

import jax
import jax.numpy as jnp
from jax import lax
from jax.experimental import pallas as pl
from jax.experimental.pallas import tpu as pltpu
from jax.sharding import Mesh
from jax.sharding import PartitionSpec as P

DP = ("dp_0", "dp_1", "dp_2")
DP_MP = ("dp_0", "dp_1", "dp_2", "mp")

clip_norm = 1.0
dense_rate = 0.02
table_rate = 0.5
adagrad_eps = 1e-10

F32 = jnp.float32
BF16 = jnp.bfloat16
I32 = jnp.int32
MESH = pl.DeviceIdType.MESH
VM = pl.BlockSpec(memory_space=pltpu.VMEM)
ANY = pl.BlockSpec(memory_space=pl.ANY)


def mm(a, b, ca, cb):
    return lax.dot_general(a, b, (((ca,), (cb,)), ((), ())), preferred_element_type=F32)


def iota(shape, dim):
    return lax.broadcasted_iota(I32, shape, dim)


def position():
    return tuple(lax.axis_index(a) for a in DP_MP)


def place(index):
    return {
        "dp_0": index // 32,
        "dp_1": (index // 8) % 4,
        "dp_2": (index // 4) % 2,
        "mp": index % 4,
    }


class Copies:
    def __init__(self, send, recv):
        self.send, self.recv, self.used, self.open = send, recv, 0, []

    def go(self, src, dst, where):
        k = self.used
        self.used += 1
        copy = pltpu.make_async_remote_copy(
            src_ref=src,
            dst_ref=dst,
            send_sem=self.send.at[k],
            recv_sem=self.recv.at[k],
            device_id=where,
            device_id_type=MESH,
        )
        copy.start()
        self.open.append(copy)
        return copy

    def drain(self):
        for copy in self.open:
            copy.wait_send()


def owner_bounds(counts_ref):
    counts = jnp.broadcast_to(counts_ref[...].astype(F32), (128, 128))
    upto = jnp.where(iota((128, 128), 0) <= iota((128, 128), 1), 1.0, 0.0).astype(BF16)
    ends = mm(counts.astype(BF16), upto, 1, 0)
    return (ends - counts).T, ends.T


def slot_rows(lookups, starts, ends):
    q = lookups.astype(F32)
    outs = []
    for part in range(q.shape[1] // 128):
        row = q[:, part * 128 : part * 128 + 128]
        hit = (row >= starts) & (row < ends)
        owner = iota((128, 128), 0).astype(F32)
        shift = jnp.sum(jnp.where(hit, owner * 32.0 - starts, 0.0), axis=0, keepdims=True)
        outs.append(row + shift)
    return jnp.concatenate(outs, axis=1)


def as_column(row):
    parts = []
    for part in range(row.shape[1] // 128):
        piece = row[:, part * 128 : part * 128 + 128]
        parts.append(jnp.broadcast_to(piece, (128, 128)).T)
    return jnp.concatenate(parts, axis=0)


def gather_kernel(lookups_ref, counts_ref, slab_ref, out_ref):
    starts, ends = owner_bounds(counts_ref)
    batch = lookups_ref.shape[1]

    def pair(k, carry):
        lane = iota((batch, 128), 1)
        got = []
        for side in range(2):
            slot = slot_rows(lookups_ref[pl.ds(2 * k + side, 1), :], starts, ends)
            column = as_column(slot).astype(I32)
            half, odd = column // 2, column % 2
            hot = jnp.concatenate(
                [
                    jnp.where(half == lane + 128 * t, 1.0, 0.0).astype(BF16)
                    for t in range(slab_ref.shape[0] // 128)
                ],
                axis=1,
            )
            both = mm(hot, slab_ref[...], 1, 0)
            one = jnp.where((lane >= 64) == (odd == 1), both, 0.0)
            got.append(one + pltpu.roll(one, 64, 1))
        out = jnp.where(lane < 64, got[0], got[1]).astype(BF16)
        out_ref[:, pl.ds(pl.multiple_of(k * 128, 128), 128)] = out
        return carry

    lax.fori_loop(0, lookups_ref.shape[0] // 2, pair, 0)


def segment_kernel(lookups_ref, counts_ref, grad_ref, out_ref, square_ref, acc):
    starts, ends = owner_bounds(counts_ref)
    batch = lookups_ref.shape[1]
    pairs = acc.shape[0]
    acc[...] = jnp.zeros_like(acc)

    def pair(k, carry):
        lane = iota((batch, 128), 1)
        block = grad_ref[:, pl.ds(pl.multiple_of(k * 128, 128), 128)]
        turned = pltpu.roll(block, 64, 1)
        hots, rows = [], []
        for side in range(2):
            slot = slot_rows(lookups_ref[pl.ds(2 * k + side, 1), :], starts, ends).astype(I32)
            hots.append(
                jnp.where(iota((pairs, batch), 0) == slot // 2, 1.0, 0.0).astype(BF16)
            )
            odd = as_column((slot % 2).astype(F32))
            same = jnp.where((lane < 64) == (side == 0), block, turned)
            kept = jnp.where((lane >= 64) == (odd > 0.5), same, 0.0)
            high = kept.astype(BF16)
            low = (kept - high.astype(F32)).astype(BF16)
            rows.append(jnp.concatenate([high, low], axis=1))
        acc[...] += mm(
            jnp.concatenate(hots, axis=1), jnp.concatenate(rows, axis=0), 1, 0
        )
        return carry

    lax.fori_loop(0, lookups_ref.shape[0] // 2, pair, 0)
    total = acc[:, :128] + acc[:, 128:]
    out_ref[...] = total.astype(BF16)
    square_ref[...] = jnp.sum((total * total).reshape(pairs // 8, 8, 128), axis=0)


def table_kernel(
    arrived_ref, even_ref, odd_ref, scale_ref, table_ref, accum_ref, new_ref, accum_new_ref, acc
):
    pairs = acc.shape[0]
    rows = 2 * pairs
    acc[...] = jnp.zeros_like(acc)
    step = 256

    def part(t, carry):
        lane = iota((step, 128), 1)
        base = pl.multiple_of(t * step, step)
        block = arrived_ref[pl.ds(base, step), :].astype(F32)
        turned = pltpu.roll(block, 64, 1)
        hots, values = [], []
        for side, ids_ref in enumerate((even_ref, odd_ref)):
            ids = jnp.concatenate(
                [ids_ref[pl.ds(2 * t, 1), :], ids_ref[pl.ds(2 * t + 1, 1), :]], axis=1
            )
            upper = ids >= pairs
            hots.append(
                jnp.where(
                    iota((pairs, step), 0) == jnp.where(upper, ids - pairs, ids), 1.0, 0.0
                ).astype(BF16)
            )
            high = as_column(jnp.where(upper, 1.0, 0.0))
            same = jnp.where((lane < 64) == (side == 0), block, turned)
            values.append(jnp.where((lane >= 64) == (high > 0.5), same, 0.0).astype(BF16))
        acc[...] += mm(
            jnp.concatenate(hots, axis=1), jnp.concatenate(values, axis=0), 1, 0
        )
        return carry

    lax.fori_loop(0, arrived_ref.shape[0] // step, part, 0)
    scale = scale_ref[0:1, 0:1]
    for p in range(pairs // 128):
        both = acc[128 * p : 128 * p + 128, :].T * scale
        for upper in range(2):
            r = both[64 * upper : 64 * upper + 64, :]
            line = p + upper * (pairs // 128)
            fresh = accum_ref[line : line + 1, :] + jnp.sum(r * r, axis=0, keepdims=True) / 64.0
            accum_new_ref[line : line + 1, :] = fresh
            at = line * 128
            new_ref[:, at : at + 128] = table_ref[:, at : at + 128] - table_rate * r / (
                jnp.sqrt(fresh) + adagrad_eps
            )


N_MAIN = 64


def main_kernel(
    pooled_ref, w_ref, bias_ref, wout_ref, label_ref, sw_ref, ids_ref,
    grad_ref, dp_ref, sq_ref, rids_ref,
    G, fac, hidden, dact, pacc, lg, LR, DL, gb, go, sv, rv,
    ZS, Df, ZRL, ZRR, ZL, ZR,
    GP, R0, SB, RL, RV, Q, RL2, RV2,
    ssem, rsem, bulk,
):
    x, y, c, z = position()
    dp = (x * 4 + y) * 2 + c
    me = dp * 4 + z
    cp = Copies(ssem, rsem)
    go_to = cp.go
    zr, zl, zo = (z + 1) % 4, (z + 3) % 4, (z + 2) % 4

    def send_ids(i, carry):
        p = (me + i) % 128
        pltpu.make_async_remote_copy(
            src_ref=ids_ref.at[p], dst_ref=rids_ref.at[me], send_sem=bulk.at[0],
            recv_sem=bulk.at[1], device_id=place(p), device_id_type=MESH,
        ).start()
        return carry

    a1 = go_to(pooled_ref.at[0:128], G.at[pl.ds(z * 256, 128)], {"mp": zr})
    b1 = go_to(pooled_ref.at[128:256], G.at[pl.ds(z * 256 + 128, 128)], {"mp": zl})
    a2 = go_to(pooled_ref.at[128:256], G.at[pl.ds(z * 256 + 128, 128)], {"mp": zr})
    b2 = go_to(pooled_ref.at[0:128], G.at[pl.ds(z * 256, 128)], {"mp": zl})
    lax.fori_loop(1, 128, send_ids, 0)
    rids_ref[me] = ids_ref[me]
    G[pl.ds(z * 256, 256), :] = pooled_ref[...]

    def forward(src):
        rows = pl.ds(pl.multiple_of(src * 256, 256), 256)
        pacc[...] = jnp.zeros_like(pacc)

        def tile(t, carry):
            cols = pl.ds(pl.multiple_of(t * 512, 512), 512)
            a = mm(G[rows, :], w_ref[:, cols], 1, 0) + bias_ref[:, cols]
            wo = wout_ref[:, cols]
            sg = lax.logistic(a)
            h = (a * sg).astype(BF16)
            hidden[rows, cols] = h
            fac[rows, cols] = wo * sg * (1.0 + a * (1.0 - sg))
            m = h.astype(F32) * wo
            pacc[...] += (m[:, 0:128] + m[:, 128:256]) + (m[:, 256:384] + m[:, 384:512])
            return carry

        lax.fori_loop(0, 4, tile, 0)
        for s in range(2):
            line = jnp.sum(pacc[128 * s : 128 * s + 128, :].T, axis=0, keepdims=True)
            lg[pl.ds(src * 2 + s, 1), :] = line

    forward(z)
    a1.wait_recv()
    a3 = go_to(
        G.at[pl.ds(zl * 256, 128)], G.at[pl.ds(zl * 256, 128)], {"mp": zr}
    )
    b1.wait_recv()
    b3 = go_to(
        G.at[pl.ds(zr * 256 + 128, 128)], G.at[pl.ds(zr * 256 + 128, 128)], {"mp": zl}
    )
    a2.wait_recv()
    forward(zl)
    b2.wait_recv()
    forward(zr)
    a3.wait_recv()
    b3.wait_recv()
    forward(zo)

    sent = [go_to(lg, LR.at[z], {"mp": (z + d) % 4}) for d in (1, 2, 3)]
    LR[z] = lg[...]
    for copy in sent:
        copy.wait_recv()
    logit = (LR[0] + LR[1]) + (LR[2] + LR[3])
    DL[...] = sw_ref[...] * (lax.logistic(logit) - label_ref[...])

    gb[...] = jnp.zeros_like(gb)
    go[...] = jnp.zeros_like(go)

    def dact_part(g, carry):
        rows = pl.ds(pl.multiple_of(g * 128, 128), 128)
        col = jnp.broadcast_to(DL[pl.ds(g, 1), :], (128, 128)).T
        for t in range(16):
            cols = slice(128 * t, 128 * t + 128)
            d = (fac[rows, cols] * col).astype(BF16)
            dact[rows, cols] = d
            gb[:, cols] += jnp.sum(d.astype(F32).reshape(16, 8, 128), axis=0)
            m = hidden[rows, cols].astype(F32) * col
            go[:, cols] += jnp.sum(m.reshape(16, 8, 128), axis=0)
        return carry

    lax.fori_loop(0, 8, dact_part, 0)
    for t in range(16):
        cols = slice(128 * t, 128 * t + 128)
        sv[t] = jnp.sum(gb[:, cols], axis=0, keepdims=True)
        sv[16 + t] = jnp.sum(go[:, cols], axis=0, keepdims=True)

    def send_small(i, carry):
        p = (dp + i) % 32
        where = {"dp_0": p // 8, "dp_1": (p // 2) % 4, "dp_2": p % 2, "mp": z}
        pltpu.make_async_remote_copy(
            src_ref=sv.at[p], dst_ref=rv.at[dp], send_sem=bulk.at[2],
            recv_sem=bulk.at[3], device_id=where, device_id_type=MESH,
        ).start()
        return carry

    lax.fori_loop(1, 32, send_small, 0)
    rv[dp] = sv[dp]

    def dpool(dest, put):
        rows = pl.ds(pl.multiple_of(dest * 256, 256), 256)

        def tile(t, carry):
            at = pl.multiple_of(t * 512, 512)
            put(mm(dact[rows, :], w_ref[pl.ds(at, 512), :], 1, 1), pl.ds(at, 512))
            return carry

        lax.fori_loop(0, 2, tile, 0)

    def put_far(d, cols):
        ZS[0, :, cols] = d.astype(BF16)

    dpool(zo, put_far)
    z1 = go_to(ZS.at[0, 0:128], ZRL, {"mp": zr})
    z2 = go_to(ZS.at[0, 128:256], ZRR, {"mp": zl})

    def put_right(d, cols):
        Df[0, :, cols] = d[0:128]
        ZS[1, 128:256, cols] = d[128:256].astype(BF16)

    dpool(zr, put_right)
    z3 = go_to(ZS.at[1, 128:256], ZL.at[128:256], {"mp": zr})

    def put_left(d, cols):
        ZS[2, 0:128, cols] = d[0:128].astype(BF16)
        Df[1, :, cols] = d[128:256]

    dpool(zl, put_left)
    z4 = go_to(ZS.at[2, 0:128], ZR.at[0:128], {"mp": zl})

    partner = {"dp_2": 1 - c}
    to_core = {}

    def weight_grad(xi, tag):
        at = pl.multiple_of(xi * 256, 256)

        def tile(t, carry):
            cols = pl.ds(pl.multiple_of(t * 512, 512), 512)
            g = mm(G[:, pl.ds(at, 256)], dact[:, cols], 0, 0)
            for yi in range(4):
                for ci in range(2):
                    r = (yi * 2 + ci) * 32
                    GP[xi, yi, ci, :, cols] = g[r : r + 32]
            return carry

        lax.fori_loop(0, 4, tile, 0)
        to_core[tag] = go_to(GP.at[xi, :, 1 - c], R0.at[xi], partner)

    def chip_sum(xi, tag):
        to_core[tag].wait_recv()
        for yi in range(4):
            s = R0[xi, yi] + GP[xi, yi, c]
            R0[xi, yi] = s
            SB[xi, yi] = s.astype(BF16)

    xr, xl, xo = (x + 1) % 4, (x + 3) % 4, (x + 2) % 4
    yr, yl, yo = (y + 1) % 4, (y + 3) % 4, (y + 2) % 4
    LO, HI = slice(0, 1024), slice(1024, 2048)

    weight_grad(xo, "o")
    weight_grad(xr, "r")
    z1.wait_recv()
    ZS[1, 0:128, :] = (Df[0] + ZRL[...].astype(F32)).astype(BF16)
    z5 = go_to(ZS.at[1, 0:128], ZL.at[0:128], {"mp": zr})
    z2.wait_recv()
    ZS[2, 128:256, :] = (Df[1] + ZRR[...].astype(F32)).astype(BF16)
    z6 = go_to(ZS.at[2, 128:256], ZR.at[128:256], {"mp": zl})
    chip_sum(xo, "o")
    h0a = go_to(SB.at[xo, 0:2, :, LO], RL.at[0, 0], {"dp_0": xr})
    h0b = go_to(SB.at[xo, 2:4, :, LO], RL.at[0, 1], {"dp_0": xl})
    weight_grad(xl, "l")
    chip_sum(xr, "r")
    h0c = go_to(SB.at[xr, 2:4, :, LO], RV.at[0, 0, 2:4], {"dp_0": xr})
    weight_grad(x, "m")
    chip_sum(xl, "l")
    h0d = go_to(SB.at[xl, 0:2, :, LO], RV.at[0, 1, 0:2], {"dp_0": xl})
    chip_sum(x, "m")
    h1a = go_to(SB.at[0:2, yo, :, HI], RL.at[1, 0], {"dp_1": yr})
    h1b = go_to(SB.at[2:4, yo, :, HI], RL.at[1, 1], {"dp_1": yl})
    h1c = go_to(SB.at[2:4, yr, :, HI], RV.at[1, 0, 2:4], {"dp_1": yr})
    h1d = go_to(SB.at[0:2, yl, :, HI], RV.at[1, 1, 0:2], {"dp_1": yl})

    def put_own(d, cols):
        dp_ref[:, cols] = d

    dpool(z, put_own)

    h0a.wait_recv()
    for k in range(2):
        SB[xr, k, :, LO] = (R0[xr, k, :, LO] + RL[0, 0, k].astype(F32)).astype(BF16)
    h0e = go_to(SB.at[xr, 0:2, :, LO], RV.at[0, 0, 0:2], {"dp_0": xr})
    h0b.wait_recv()
    for k in range(2):
        SB[xl, 2 + k, :, LO] = (R0[xl, 2 + k, :, LO] + RL[0, 1, k].astype(F32)).astype(BF16)
    h0f = go_to(SB.at[xl, 2:4, :, LO], RV.at[0, 1, 2:4], {"dp_0": xl})
    h1a.wait_recv()
    for k in range(2):
        SB[k, yr, :, HI] = (R0[k, yr, :, HI] + RL[1, 0, k].astype(F32)).astype(BF16)
    h1e = go_to(SB.at[0:2, yr, :, HI], RV.at[1, 0, 0:2], {"dp_1": yr})
    h1b.wait_recv()
    for k in range(2):
        SB[2 + k, yl, :, HI] = (R0[2 + k, yl, :, HI] + RL[1, 1, k].astype(F32)).astype(BF16)
    h1f = go_to(SB.at[2:4, yl, :, HI], RV.at[1, 1, 2:4], {"dp_1": yl})

    def second(h, axis, n):
        nr, nl, no = (n + 1) % 4, (n + 3) % 4, (n + 2) % 4
        s1 = go_to(Q.at[h, no, 0:16], RL2.at[h, 0], {axis: nr})
        s2 = go_to(Q.at[h, no, 16:32], RL2.at[h, 1], {axis: nl})
        s3 = go_to(Q.at[h, nr, 16:32], RV2.at[h, 0, 16:32], {axis: nr})
        s4 = go_to(Q.at[h, nl, 0:16], RV2.at[h, 1, 0:16], {axis: nl})
        return nr, nl, (s1, s2, s3, s4)

    def second_relay(h, axis, state):
        nr, nl, (s1, s2, s3, s4) = state
        s1.wait_recv()
        Q[h, nr, 0:16] = Q[h, nr, 0:16] + RL2[h, 0]
        s5 = go_to(Q.at[h, nr, 0:16], RV2.at[h, 0, 0:16], {axis: nr})
        s2.wait_recv()
        Q[h, nl, 16:32] = Q[h, nl, 16:32] + RL2[h, 1]
        s6 = go_to(Q.at[h, nl, 16:32], RV2.at[h, 1, 16:32], {axis: nl})
        return s3, s4, s5, s6

    for copy in (h0c, h0d, h0e, h0f):
        copy.wait_recv()
    for k in range(4):
        Q[0, k] = R0[x, k, :, LO] + (RV[0, 0, k].astype(F32) + RV[0, 1, k].astype(F32))
    t0 = second(0, "dp_1", y)
    for copy in (h1c, h1d, h1e, h1f):
        copy.wait_recv()
    for k in range(4):
        Q[1, k] = R0[k, y, :, HI] + (RV[1, 0, k].astype(F32) + RV[1, 1, k].astype(F32))
    t1 = second(1, "dp_0", x)
    u0 = second_relay(0, "dp_1", t0)
    u1 = second_relay(1, "dp_0", t1)

    for copy in (z3, z4, z5, z6):
        copy.wait_recv()
    dp_ref[...] = dp_ref[...] + (ZL[...].astype(F32) + ZR[...].astype(F32))

    small = sv.at[pl.ds(0, 31)]
    pltpu.make_async_copy(small, small, bulk.at[2]).wait()
    pltpu.make_async_copy(small, small, bulk.at[3]).wait()
    few = jnp.sum(rv[...], axis=0)
    few = jnp.where(iota((8, 128), 0) == 0, jnp.broadcast_to(few * few, (8, 128)), 0.0)

    for copy in u0 + u1:
        copy.wait_recv()
    left = Q[0, y] + (RV2[0, 0] + RV2[0, 1])
    right = Q[1, x] + (RV2[1, 0] + RV2[1, 1])
    grad_ref[:, LO] = left
    grad_ref[:, HI] = right
    both = left * left + right * right
    both = jnp.sum(both.reshape(4, 8, 1024), axis=0)
    for t in range(8):
        few = few + both[:, 128 * t : 128 * t + 128]
    sq_ref[...] = few

    lot = ids_ref.at[pl.ds(0, 127)]
    pltpu.make_async_copy(lot, lot, bulk.at[0]).wait()
    pltpu.make_async_copy(lot, lot, bulk.at[1]).wait()
    cp.drain()


N_XCHG = 40


def exchange_kernel(
    slot_ref, sqa_ref, sqb_ref, grad_ref, accum_ref, w_ref,
    wn_ref, accum_new_ref, arrived_ref, scale_ref,
    ns, NR, wpart, ssem, rsem, bulk, local,
):
    x, y, c, z = position()
    dp = (x * 4 + y) * 2 + c
    me = dp * 4 + z
    cp = Copies(ssem, rsem)
    go_to = cp.go
    fetch = pltpu.make_async_copy(w_ref.at[pl.ds(dp * 32, 32)], wpart, local)
    fetch.start()
    ns[...] = jnp.sum(sqa_ref[...] + sqb_ref[...], axis=0, keepdims=True)

    def send_norm(i, carry):
        p = (me + i) % 128
        pltpu.make_async_remote_copy(
            src_ref=ns, dst_ref=NR.at[me], send_sem=bulk.at[0],
            recv_sem=bulk.at[1], device_id=place(p), device_id_type=MESH,
        ).start()
        return carry

    def send_slots(i, carry):
        p = (me + i) % 128
        pltpu.make_async_remote_copy(
            src_ref=slot_ref.at[p], dst_ref=arrived_ref.at[me], send_sem=bulk.at[2],
            recv_sem=bulk.at[3], device_id=place(p), device_id_type=MESH,
        ).start()
        return carry

    lax.fori_loop(1, 128, send_norm, 0)
    lax.fori_loop(1, 128, send_slots, 0)
    NR[me] = ns[...]
    arrived_ref[me] = slot_ref[me]

    lot = NR.at[pl.ds(0, 127)]
    pltpu.make_async_copy(lot, lot, bulk.at[1]).wait()
    lanes = jnp.sum(NR[...], axis=0)
    total = jnp.sum(lanes, axis=1, keepdims=True)
    scale = clip_norm / jnp.maximum(jnp.sqrt(total), clip_norm)
    scale_ref[...] = jnp.broadcast_to(scale, (8, 128))
    fetch.wait()
    clipped = scale * grad_ref[...]
    fresh = accum_ref[...] + clipped * clipped
    accum_new_ref[...] = fresh
    wn_ref[x, y, c] = (
        wpart[...].astype(F32) - dense_rate * clipped / (jnp.sqrt(fresh) + adagrad_eps)
    ).astype(BF16)

    xr, xl, xo = (x + 1) % 4, (x + 3) % 4, (x + 2) % 4
    yr, yl, yo = (y + 1) % 4, (y + 3) % 4, (y + 2) % 4
    LO, HI = slice(0, 1024), slice(1024, 2048)
    T, B = slice(0, 16), slice(16, 32)
    partner = {"dp_2": 1 - c}

    def same(ref, where):
        return go_to(ref, ref, where)

    p1 = same(wn_ref.at[x, y, c, :, LO], {"dp_0": xr})
    p2 = same(wn_ref.at[x, y, c, :, LO], {"dp_0": xl})
    q1 = same(wn_ref.at[x, y, c, :, HI], {"dp_1": yr})
    q2 = same(wn_ref.at[x, y, c, :, HI], {"dp_1": yl})
    p1.wait_recv()
    p3 = same(wn_ref.at[xl, y, c, T, LO], {"dp_0": xr})
    p2.wait_recv()
    p4 = same(wn_ref.at[xr, y, c, B, LO], {"dp_0": xl})
    q1.wait_recv()
    q3 = same(wn_ref.at[x, yl, c, T, HI], {"dp_1": yr})
    q2.wait_recv()
    q4 = same(wn_ref.at[x, yr, c, B, HI], {"dp_1": yl})
    p3.wait_recv()
    p4.wait_recv()
    p5 = same(wn_ref.at[:, y, c, :, LO], {"dp_1": yr})
    p6 = same(wn_ref.at[:, y, c, :, LO], {"dp_1": yl})
    q3.wait_recv()
    q4.wait_recv()
    q5 = same(wn_ref.at[x, :, c, :, HI], {"dp_0": xr})
    q6 = same(wn_ref.at[x, :, c, :, HI], {"dp_0": xl})
    d = [same(wn_ref.at[:, y, c, :, LO], partner), same(wn_ref.at[x, :, c, :, HI], partner)]
    p5.wait_recv()
    p7 = same(wn_ref.at[0:2, yl, c, :, LO], {"dp_1": yr})
    p6.wait_recv()
    p8 = same(wn_ref.at[2:4, yr, c, :, LO], {"dp_1": yl})
    q5.wait_recv()
    q7 = same(wn_ref.at[xl, 0:2, c, :, HI], {"dp_0": xr})
    q6.wait_recv()
    q8 = same(wn_ref.at[xr, 2:4, c, :, HI], {"dp_0": xl})
    d += [same(wn_ref.at[:, yl, c, :, LO], partner), same(wn_ref.at[:, yr, c, :, LO], partner)]
    d += [same(wn_ref.at[xl, :, c, :, HI], partner), same(wn_ref.at[xr, :, c, :, HI], partner)]
    for copy in (p7, p8, q7, q8):
        copy.wait_recv()
    d += [same(wn_ref.at[:, yo, c, :, LO], partner), same(wn_ref.at[xo, :, c, :, HI], partner)]
    for copy in d:
        copy.wait_recv()
    pltpu.make_async_copy(lot, lot, bulk.at[0]).wait()
    many = arrived_ref.at[pl.ds(0, 127)]
    pltpu.make_async_copy(many, many, bulk.at[2]).wait()
    pltpu.make_async_copy(many, many, bulk.at[3]).wait()
    cp.drain()


def shape(dims, kind):
    return jax.ShapeDtypeStruct(dims, kind)


def gather_pooled(lookups, counts, slab):
    return pl.pallas_call(
        gather_kernel,
        out_shape=shape((256, 1024), BF16),
        in_specs=[VM] * 3,
        out_specs=VM,
        name="gather_pooled",
    )(lookups, counts, slab)


def segment_slots(lookups, counts, dpooled):
    return pl.pallas_call(
        segment_kernel,
        out_shape=(shape((2048, 128), BF16), shape((8, 128), F32)),
        in_specs=[VM] * 3,
        out_specs=(VM, VM),
        scratch_shapes=[pltpu.VMEM((2048, 256), F32)],
        name="segment_slots",
    )(lookups, counts, dpooled)


def table_update(arrived, even, odd, scale, table, accum):
    return pl.pallas_call(
        table_kernel,
        out_shape=(shape((64, 4096), F32), shape((32, 128), F32)),
        in_specs=[VM] * 6,
        out_specs=(VM, VM),
        scratch_shapes=[pltpu.VMEM((2048, 128), F32)],
        name="table_update",
    )(arrived, even, odd, scale, table, accum)


def tower(pooled, w, bias, wout, labels, sw, ids):
    V = pltpu.VMEM
    return pl.pallas_call(
        main_kernel,
        out_shape=(
            shape((32, 2048), F32),
            shape((256, 1024), F32),
            shape((8, 128), F32),
            shape((128, 1, 128), I32),
        ),
        in_specs=[VM] * 7,
        out_specs=(VM,) * 4,
        scratch_shapes=[
            V((1024, 1024), BF16), V((1024, 2048), F32), V((1024, 2048), BF16),
            V((1024, 2048), BF16), V((256, 128), F32), V((8, 128), F32), V((4, 8, 128), F32),
            V((8, 128), F32), V((8, 2048), F32), V((8, 2048), F32),
            V((32, 1, 128), F32), V((32, 1, 128), F32),
            V((3, 256, 1024), BF16), V((2, 128, 1024), F32),
            V((128, 1024), BF16), V((128, 1024), BF16),
            V((256, 1024), BF16), V((256, 1024), BF16),
            V((4, 4, 2, 32, 2048), F32), V((4, 4, 32, 2048), F32), V((4, 4, 32, 2048), BF16),
            V((2, 2, 2, 32, 1024), BF16), V((2, 2, 4, 32, 1024), BF16),
            V((2, 4, 32, 1024), F32), V((2, 2, 16, 1024), F32), V((2, 2, 32, 1024), F32),
            pltpu.SemaphoreType.DMA((N_MAIN,)), pltpu.SemaphoreType.DMA((N_MAIN,)),
            pltpu.SemaphoreType.DMA((4,)),
        ],
        compiler_params=pltpu.CompilerParams(
            has_side_effects=True, vmem_limit_bytes=62 * 1024 * 1024
        ),
        name="tower",
    )(pooled, w, bias, wout, labels, sw, ids)


def exchange(slots, sqa, sqb, grad, accum, w):
    V = pltpu.VMEM
    return pl.pallas_call(
        exchange_kernel,
        out_shape=(
            shape((4, 4, 2, 32, 2048), BF16),
            shape((32, 2048), F32),
            shape((128, 16, 128), BF16),
            shape((8, 128), F32),
        ),
        in_specs=[VM] * 5 + [ANY],
        out_specs=(VM,) * 4,
        scratch_shapes=[
            V((1, 128), F32), V((128, 1, 128), F32), V((32, 2048), BF16),
            pltpu.SemaphoreType.DMA((N_XCHG,)), pltpu.SemaphoreType.DMA((N_XCHG,)),
            pltpu.SemaphoreType.DMA((4,)), pltpu.SemaphoreType.DMA,
        ],
        compiler_params=pltpu.CompilerParams(has_side_effects=True),
        name="exchange",
    )(slots, sqa, sqb, grad, accum, w)


def body(
    slab_values,
    row_ids,
    peer_counts,
    lookup_slots,
    labels,
    sample_weight,
    weight_in,
    bias_in,
    weight_out,
    dense_accum,
    table_rows,
    table_accum,
):
    lookups = lookup_slots.T
    slab = slab_values[0].reshape(2048, 128)
    ids = row_ids[0]
    ids = jnp.concatenate([ids[:, 0::2], ids[:, 1::2]], axis=1)
    ids = jnp.pad(ids, ((0, 0), (0, 96))).reshape(128, 1, 128)
    pooled = gather_pooled(lookups, peer_counts, slab)
    grad, dpooled, dense_sq, got = tower(
        pooled,
        weight_in,
        bias_in.reshape(1, 2048),
        weight_out.astype(F32).reshape(1, 2048),
        labels.astype(F32).reshape(8, 128),
        sample_weight.reshape(8, 128),
        ids,
    )
    slots, slot_sq = segment_slots(lookups, peer_counts, dpooled)
    wn, accum_new, arrived, scale = exchange(
        slots.reshape(128, 16, 128), dense_sq, slot_sq, grad, dense_accum, weight_in
    )
    even = got[:, 0, 0:16].reshape(16, 128)
    odd = got[:, 0, 16:32].reshape(16, 128)
    table_new, table_accum_new = table_update(
        arrived.reshape(2048, 128), even, odd, scale, table_rows.T,
        table_accum.reshape(32, 128),
    )
    return (
        wn.reshape(1024, 2048), accum_new, table_new.T, table_accum_new.reshape(4096)
    )


def solution(mesh):
    torus = Mesh(mesh.devices.reshape(4, 4, 2, mesh.shape["mp"]), ("dp_0", "dp_1", "dp_2", "mp"))
    placed = (
        P(DP_MP, None, None),
        P(DP_MP, None, None),
        P(DP_MP, None),
        P(DP_MP, None),
        P(DP),
        P(DP),
        P(None, "mp"),
        P("mp"),
        P("mp"),
        P(DP, "mp"),
        P(DP_MP, None),
        P(DP_MP),
    )
    return jax.shard_map(
        body,
        mesh=torus,
        in_specs=placed,
        out_specs=(P(None, "mp"), P(DP, "mp"), P(DP_MP, None), P(DP_MP)),
        check_vma=False,
    )
```

```python
import functools

import jax
import jax.numpy as jnp
from jax import lax
from jax.experimental import pallas as pl
from jax.experimental.pallas import tpu as pltpu
from jax.sharding import Mesh
from jax.sharding import PartitionSpec as P

DP = ("dp_0", "dp_1", "dp_2")
DP_MP = ("dp_0", "dp_1", "dp_2", "mp")

clip_norm = 1.0
dense_rate = 0.02
table_rate = 0.5
adagrad_eps = 1e-10

F32 = jnp.float32
BF16 = jnp.bfloat16
I32 = jnp.int32
MESH = pl.DeviceIdType.MESH
VM = pl.BlockSpec(memory_space=pltpu.VMEM)
ANY = pl.BlockSpec(memory_space=pl.ANY)


def mm(a, b, ca, cb):
    return lax.dot_general(a, b, (((ca,), (cb,)), ((), ())), preferred_element_type=F32)


def iota(shape, dim):
    return lax.broadcasted_iota(I32, shape, dim)


def position():
    return tuple(lax.axis_index(a) for a in DP_MP)


def place(index):
    return {
        "dp_0": index // 32,
        "dp_1": (index // 8) % 4,
        "dp_2": (index // 4) % 2,
        "mp": index % 4,
    }


class Copies:
    def __init__(self, send, recv):
        self.send, self.recv, self.used, self.open = send, recv, 0, []

    def go(self, src, dst, where):
        k = self.used
        self.used += 1
        copy = pltpu.make_async_remote_copy(
            src_ref=src,
            dst_ref=dst,
            send_sem=self.send.at[k],
            recv_sem=self.recv.at[k],
            device_id=where,
            device_id_type=MESH,
        )
        copy.start()
        self.open.append(copy)
        return copy

    def drain(self):
        for copy in self.open:
            copy.wait_send()


def owner_bounds(counts_ref):
    counts = jnp.broadcast_to(counts_ref[...].astype(F32), (128, 128))
    upto = jnp.where(iota((128, 128), 0) <= iota((128, 128), 1), 1.0, 0.0).astype(BF16)
    ends = mm(counts.astype(BF16), upto, 1, 0)
    return (ends - counts).T, ends.T


def slot_rows(lookups, starts, ends):
    q = lookups.astype(F32)
    outs = []
    for part in range(q.shape[1] // 128):
        row = q[:, part * 128 : part * 128 + 128]
        hit = (row >= starts) & (row < ends)
        owner = iota((128, 128), 0).astype(F32)
        shift = jnp.sum(jnp.where(hit, owner * 32.0 - starts, 0.0), axis=0, keepdims=True)
        outs.append(row + shift)
    return jnp.concatenate(outs, axis=1)


def as_column(row):
    parts = []
    for part in range(row.shape[1] // 128):
        piece = row[:, part * 128 : part * 128 + 128]
        parts.append(jnp.broadcast_to(piece, (128, 128)).T)
    return jnp.concatenate(parts, axis=0)


def tiles_over_rows(index, count):
    high = jnp.floor(index * (1.0 / 16.0))
    low = index - 16.0 * high
    n = index.shape[1]
    inner = jnp.where(iota((16, n), 0).astype(F32) == low, 1.0, 0.0).astype(BF16)
    high = jnp.broadcast_to(high, (16, n)).astype(BF16)
    zero = jnp.zeros((16, n), BF16)
    return jnp.concatenate(
        [jnp.where(high == jnp.asarray(t, BF16), inner, zero) for t in range(count)], axis=0
    )


def tiles_over_lanes(column, count):
    high = jnp.floor(column * (1.0 / 128.0))
    low = column - 128.0 * high
    inner = jnp.where(iota(column.shape, 1).astype(F32) == low, 1.0, 0.0).astype(BF16)
    high = high.astype(BF16)
    zero = jnp.zeros(column.shape, BF16)
    return jnp.concatenate(
        [jnp.where(high == jnp.asarray(t, BF16), inner, zero) for t in range(count)], axis=1
    )


class Spread:
    LO, HI = slice(0, 1024), slice(1024, 2048)
    T, B = slice(0, 16), slice(16, 32)

    def __init__(self, ref, go, where):
        self.ref, self.go = ref, go
        self.x, self.y, self.c, _ = where
        self.xr, self.xl, self.xo = ((self.x + d) % 4 for d in (1, 3, 2))
        self.yr, self.yl, self.yo = ((self.y + d) % 4 for d in (1, 3, 2))
        self.partner = {"dp_2": 1 - self.c}
        self.d = []

    def same(self, piece, where):
        ref = self.ref.at[piece]
        return self.go(ref, ref, where)

    def first(self):
        x, y, c = self.x, self.y, self.c
        every = slice(None)
        self.p1 = self.same((x, y, c, every, self.LO), {"dp_0": self.xr})
        self.p2 = self.same((x, y, c, every, self.LO), {"dp_0": self.xl})
        self.q1 = self.same((x, y, c, every, self.HI), {"dp_1": self.yr})
        self.q2 = self.same((x, y, c, every, self.HI), {"dp_1": self.yl})

    def second(self):
        x, y, c = self.x, self.y, self.c
        self.p1.wait_recv()
        self.p3 = self.same((self.xl, y, c, self.T, self.LO), {"dp_0": self.xr})
        self.p2.wait_recv()
        self.p4 = self.same((self.xr, y, c, self.B, self.LO), {"dp_0": self.xl})
        self.q1.wait_recv()
        self.q3 = self.same((x, self.yl, c, self.T, self.HI), {"dp_1": self.yr})
        self.q2.wait_recv()
        self.q4 = self.same((x, self.yr, c, self.B, self.HI), {"dp_1": self.yl})

    def third(self):
        x, y, c = self.x, self.y, self.c
        every = slice(None)
        self.p3.wait_recv()
        self.p4.wait_recv()
        mine, other = (every, y, c, every, self.LO), (x, every, c, every, self.HI)
        self.p5 = self.same(mine, {"dp_1": self.yr})
        self.p6 = self.same(mine, {"dp_1": self.yl})
        self.q3.wait_recv()
        self.q4.wait_recv()
        self.q5 = self.same(other, {"dp_0": self.xr})
        self.q6 = self.same(other, {"dp_0": self.xl})
        self.d += [self.same(mine, self.partner), self.same(other, self.partner)]

    def fourth(self):
        c = self.c
        every = slice(None)
        self.p5.wait_recv()
        self.p7 = self.same((slice(0, 2), self.yl, c, every, self.LO), {"dp_1": self.yr})
        self.p6.wait_recv()
        self.p8 = self.same((slice(2, 4), self.yr, c, every, self.LO), {"dp_1": self.yl})
        self.q5.wait_recv()
        self.q7 = self.same((self.xl, slice(0, 2), c, every, self.HI), {"dp_0": self.xr})
        self.q6.wait_recv()
        self.q8 = self.same((self.xr, slice(2, 4), c, every, self.HI), {"dp_0": self.xl})
        for n in (self.yl, self.yr):
            self.d.append(self.same((every, n, c, every, self.LO), self.partner))
        for n in (self.xl, self.xr):
            self.d.append(self.same((n, every, c, every, self.HI), self.partner))

    def fifth(self):
        c = self.c
        every = slice(None)
        for copy in (self.p7, self.p8, self.q7, self.q8):
            copy.wait_recv()
        self.d.append(self.same((every, self.yo, c, every, self.LO), self.partner))
        self.d.append(self.same((self.xo, every, c, every, self.HI), self.partner))

    def last(self):
        for copy in self.d:
            copy.wait_recv()


N_COPIES = 140


def step_kernel(
    lookups_ref, counts_ref, slab_ref, ids_ref, label_ref, sw_ref, bias_ref, wout_ref,
    w_any, accum_any,
    ga_out, aa_out, arrived_ref, rids_ref, scale_ref, grad_ref,
    W, A, idsend, G, fac, hidden, dact, pacc, lg, LR, DL, gb, go, sv, rv,
    ZS, Df, ZRL, ZRR, ZL, ZR, DPL,
    R0, SB, RL, RV, Q, RL2, RV2,
    GA, AA, acc, slots, ns, NR,
    ssem, rsem, bulk, local,
):
    x, y, c, z = position()
    dp = (x * 4 + y) * 2 + c
    me = dp * 4 + z
    cp = Copies(ssem, rsem)
    go_to = cp.go
    zr, zl, zo = (z + 1) % 4, (z + 3) % 4, (z + 2) % 4
    xr, xl, xo = (x + 1) % 4, (x + 3) % 4, (x + 2) % 4
    yr, yl, yo = (y + 1) % 4, (y + 3) % 4, (y + 2) % 4
    LO, HI = slice(0, 1024), slice(1024, 2048)

    barrier = pltpu.get_barrier_semaphore()

    def greet(i, carry):
        pl.semaphore_signal(
            barrier, inc=1, device_id=place((me + i) % 128), device_id_type=MESH
        )
        return carry

    lax.fori_loop(1, 128, greet, 0)
    fetch_a = pltpu.make_async_copy(accum_any, A, local.at[1])
    fetch_a.start()
    fetch_w = pltpu.make_async_copy(w_any, W, local.at[0])
    fetch_w.start()

    starts, ends = owner_bounds(counts_ref)
    own_rows = pl.ds(pl.multiple_of(z * 256, 256), 256)

    def gather_pair(k):
        lane = iota((256, 128), 1)
        got = []
        for side in range(2):
            slot = slot_rows(lookups_ref[2 * k + side : 2 * k + side + 1, :], starts, ends)
            column = as_column(slot)
            half = jnp.floor(column * 0.5)
            odd = column - 2.0 * half
            both = mm(tiles_over_lanes(half, 16), slab_ref[...], 1, 0)
            one = jnp.where((lane >= 64) == (odd > 0.5), both, 0.0)
            got.append(one + pltpu.roll(one, 64, 1))
        G[own_rows, k * 128 : k * 128 + 128] = jnp.where(lane < 64, got[0], got[1]).astype(BF16)

    def block(src, k):
        return G.at[pl.ds(pl.multiple_of(src * 256, 256), 256), k * 256 : k * 256 + 256]

    def send_ids(i, carry):
        p = (me + i) % 128
        pltpu.make_async_remote_copy(
            src_ref=idsend.at[p], dst_ref=rids_ref.at[me], send_sem=bulk.at[0],
            recv_sem=bulk.at[1], device_id=place(p), device_id_type=MESH,
        ).start()
        return carry

    right, left = {}, {}

    def send_block(k):
        right[k] = go_to(block(z, k), block(z, k), {"mp": zr})
        left[k] = go_to(block(z, k), block(z, k), {"mp": zl})

    gather_pair(0)
    gather_pair(1)
    turned = jnp.concatenate([ids_ref[...].astype(F32), jnp.zeros((96, 128), F32)], axis=0)
    idsend[...] = turned.T.astype(I32).reshape(128, 1, 128)
    fetch_a.wait()
    AA[x, y, c] = A[...].astype(BF16)
    pl.semaphore_wait(barrier, 127)
    send_block(0)
    aa = Spread(AA, go_to, (x, y, c, z))
    aa.first()
    lax.fori_loop(1, 128, send_ids, 0)
    rids_ref[me] = idsend[me]
    gather_pair(4)
    gather_pair(5)
    send_block(2)
    gather_pair(2)
    gather_pair(3)
    send_block(1)
    gather_pair(6)
    gather_pair(7)
    send_block(3)
    fetch_w.wait()

    def forward(src):
        rows = pl.ds(pl.multiple_of(src * 256, 256), 256)
        pacc[...] = jnp.zeros_like(pacc)

        def tile(t, carry):
            cols = pl.ds(pl.multiple_of(t * 512, 512), 512)
            a = mm(G[rows, :], W[:, cols], 1, 0) + bias_ref[:, cols]
            wo = wout_ref[:, cols]
            sg = lax.logistic(a)
            h = (a * sg).astype(BF16)
            hidden[rows, cols] = h
            fac[src, :, :, :, cols] = (wo * sg * (1.0 + a * (1.0 - sg))).reshape(4, 2, 32, 512)
            m = h.astype(F32) * wo
            pacc[...] += (m[:, 0:128] + m[:, 128:256]) + (m[:, 256:384] + m[:, 384:512])
            return carry

        lax.fori_loop(0, 4, tile, 0)
        for s in range(2):
            line = jnp.sum(pacc[128 * s : 128 * s + 128, :].T, axis=0, keepdims=True)
            lg[pl.ds(src * 2 + s, 1), :] = line

    right[0].wait_recv()
    f0 = go_to(block(zl, 0), block(zl, 0), {"mp": zr})
    left[2].wait_recv()
    f2 = go_to(block(zr, 2), block(zr, 2), {"mp": zl})
    forward(z)
    right[1].wait_recv()
    f1 = go_to(block(zl, 1), block(zl, 1), {"mp": zr})
    left[3].wait_recv()
    f3 = go_to(block(zr, 3), block(zr, 3), {"mp": zl})
    aa.second()
    right[2].wait_recv()
    right[3].wait_recv()
    forward(zl)
    aa.third()
    left[0].wait_recv()
    left[1].wait_recv()
    forward(zr)
    aa.fourth()
    for copy in (f0, f1, f2, f3):
        copy.wait_recv()
    forward(zo)

    sent = [go_to(lg, LR.at[z], {"mp": (z + d) % 4}) for d in (1, 2, 3)]
    LR[z] = lg[...]
    for copy in sent:
        copy.wait_recv()
    logit = (LR[0] + LR[1]) + (LR[2] + LR[3])
    DL[...] = sw_ref[...] * (lax.logistic(logit) - label_ref[...].astype(F32))

    gb[...] = jnp.zeros_like(gb)
    go[...] = jnp.zeros_like(go)

    def dact_part(g, carry):
        rows = pl.ds(pl.multiple_of(g * 128, 128), 128)
        col = jnp.broadcast_to(DL[pl.ds(g, 1), :], (128, 128)).T
        for t in range(16):
            cols = slice(128 * t, 128 * t + 128)
            f = fac[g // 2, pl.ds((g % 2) * 2, 2), :, :, cols].reshape(128, 128)
            d = (f * col).astype(BF16)
            dact[rows, cols] = d
            gb[:, cols] += jnp.sum(d.astype(F32).reshape(16, 8, 128), axis=0)
            m = hidden[rows, cols].astype(F32) * col
            go[:, cols] += jnp.sum(m.reshape(16, 8, 128), axis=0)
        return carry

    lax.fori_loop(0, 8, dact_part, 0)

    def dpool(dest, put):
        rows = pl.ds(pl.multiple_of(dest * 256, 256), 256)

        def tile(t, carry):
            at = pl.multiple_of(t * 512, 512)
            put(mm(dact[rows, :], W[pl.ds(at, 512), :], 1, 1), pl.ds(at, 512))
            return carry

        lax.fori_loop(0, 2, tile, 0)

    def put_far(d, cols):
        ZS[0, :, cols] = d.astype(BF16)

    dpool(zo, put_far)
    z1 = go_to(ZS.at[0, 0:128], ZRL, {"mp": zr})
    z2 = go_to(ZS.at[0, 128:256], ZRR, {"mp": zl})

    def put_right(d, cols):
        Df[0, :, cols] = d[0:128]
        ZS[1, 128:256, cols] = d[128:256].astype(BF16)

    dpool(zr, put_right)
    z3 = go_to(ZS.at[1, 128:256], ZL.at[128:256], {"mp": zr})

    def put_left(d, cols):
        ZS[2, 0:128, cols] = d[0:128].astype(BF16)
        Df[1, :, cols] = d[128:256]

    dpool(zl, put_left)
    z4 = go_to(ZS.at[2, 0:128], ZR.at[0:128], {"mp": zl})

    partner = {"dp_2": 1 - c}
    to_core = {}

    def weight_grad(xi, tag):
        at = pl.multiple_of(xi * 256, 256)

        def tile(t, carry):
            cols = pl.ds(pl.multiple_of(t * 512, 512), 512)
            g = mm(G[:, pl.ds(at, 256)], dact[:, cols], 0, 0)
            fac[xi, :, :, :, cols] = g.reshape(4, 2, 32, 512)
            return carry

        lax.fori_loop(0, 4, tile, 0)
        to_core[tag] = go_to(fac.at[xi, :, 1 - c], R0.at[xi], partner)

    def chip_sum(xi, tag):
        to_core[tag].wait_recv()
        for yi in range(4):
            s = R0[xi, yi] + fac[xi, yi, c]
            R0[xi, yi] = s
            SB[xi, yi] = s.astype(BF16)

    weight_grad(xo, "o")
    weight_grad(xr, "r")
    chip_sum(xo, "o")
    h0a = go_to(SB.at[xo, 0:2, :, LO], RL.at[0, 0], {"dp_0": xr})
    h0b = go_to(SB.at[xo, 2:4, :, LO], RL.at[0, 1], {"dp_0": xl})
    z1.wait_recv()
    ZS[1, 0:128, :] = (Df[0] + ZRL[...].astype(F32)).astype(BF16)
    z5 = go_to(ZS.at[1, 0:128], ZL.at[0:128], {"mp": zr})
    z2.wait_recv()
    ZS[2, 128:256, :] = (Df[1] + ZRR[...].astype(F32)).astype(BF16)
    z6 = go_to(ZS.at[2, 128:256], ZR.at[128:256], {"mp": zl})
    weight_grad(xl, "l")
    chip_sum(xr, "r")
    h0c = go_to(SB.at[xr, 2:4, :, LO], RV.at[0, 0, 2:4], {"dp_0": xr})
    weight_grad(x, "m")
    chip_sum(xl, "l")
    h0d = go_to(SB.at[xl, 0:2, :, LO], RV.at[0, 1, 0:2], {"dp_0": xl})
    chip_sum(x, "m")
    h1a = go_to(SB.at[0:2, yo, :, HI], RL.at[1, 0], {"dp_1": yr})
    h1b = go_to(SB.at[2:4, yo, :, HI], RL.at[1, 1], {"dp_1": yl})
    h1c = go_to(SB.at[2:4, yr, :, HI], RV.at[1, 0, 2:4], {"dp_1": yr})
    h1d = go_to(SB.at[0:2, yl, :, HI], RV.at[1, 1, 0:2], {"dp_1": yl})

    h0a.wait_recv()
    for k in range(2):
        SB[xr, k, :, LO] = (R0[xr, k, :, LO] + RL[0, 0, k].astype(F32)).astype(BF16)
    h0e = go_to(SB.at[xr, 0:2, :, LO], RV.at[0, 0, 0:2], {"dp_0": xr})
    h0b.wait_recv()
    for k in range(2):
        SB[xl, 2 + k, :, LO] = (R0[xl, 2 + k, :, LO] + RL[0, 1, k].astype(F32)).astype(BF16)
    h0f = go_to(SB.at[xl, 2:4, :, LO], RV.at[0, 1, 2:4], {"dp_0": xl})

    for t in range(16):
        cols = slice(128 * t, 128 * t + 128)
        sv[t] = jnp.sum(gb[:, cols], axis=0, keepdims=True)
        sv[16 + t] = jnp.sum(go[:, cols], axis=0, keepdims=True)

    def send_small(i, carry):
        p = (dp + i) % 32
        where = {"dp_0": p // 8, "dp_1": (p // 2) % 4, "dp_2": p % 2, "mp": z}
        pltpu.make_async_remote_copy(
            src_ref=sv.at[p], dst_ref=rv.at[dp], send_sem=bulk.at[2],
            recv_sem=bulk.at[3], device_id=where, device_id_type=MESH,
        ).start()
        return carry

    lax.fori_loop(1, 32, send_small, 0)
    rv[dp] = sv[dp]

    def put_own(d, cols):
        DPL[:, cols] = d

    dpool(z, put_own)
    h1a.wait_recv()
    for k in range(2):
        SB[k, yr, :, HI] = (R0[k, yr, :, HI] + RL[1, 0, k].astype(F32)).astype(BF16)
    h1e = go_to(SB.at[0:2, yr, :, HI], RV.at[1, 0, 0:2], {"dp_1": yr})
    h1b.wait_recv()
    for k in range(2):
        SB[2 + k, yl, :, HI] = (R0[2 + k, yl, :, HI] + RL[1, 1, k].astype(F32)).astype(BF16)
    h1f = go_to(SB.at[2:4, yl, :, HI], RV.at[1, 1, 2:4], {"dp_1": yl})
    aa.fifth()

    def ring(h, axis, n):
        nr, nl, no = (n + 1) % 4, (n + 3) % 4, (n + 2) % 4
        s1 = go_to(Q.at[h, no, 0:16], RL2.at[h, 0], {axis: nr})
        s2 = go_to(Q.at[h, no, 16:32], RL2.at[h, 1], {axis: nl})
        s3 = go_to(Q.at[h, nr, 16:32], RV2.at[h, 0, 16:32], {axis: nr})
        s4 = go_to(Q.at[h, nl, 0:16], RV2.at[h, 1, 0:16], {axis: nl})
        return nr, nl, (s1, s2, s3, s4)

    def ring_relay(h, axis, state):
        nr, nl, (s1, s2, s3, s4) = state
        s1.wait_recv()
        Q[h, nr, 0:16] = Q[h, nr, 0:16] + RL2[h, 0]
        s5 = go_to(Q.at[h, nr, 0:16], RV2.at[h, 0, 0:16], {axis: nr})
        s2.wait_recv()
        Q[h, nl, 16:32] = Q[h, nl, 16:32] + RL2[h, 1]
        s6 = go_to(Q.at[h, nl, 16:32], RV2.at[h, 1, 16:32], {axis: nl})
        return s3, s4, s5, s6

    def segment(first, last):
        def pair(k, carry):
            lane = iota((256, 128), 1)
            block = DPL[:, pl.ds(pl.multiple_of(k * 128, 128), 128)]
            turned = pltpu.roll(block, 64, 1)
            hots, rows = [], []
            for side in range(2):
                slot = slot_rows(lookups_ref[pl.ds(2 * k + side, 1), :], starts, ends)
                low = slot - 16.0 * jnp.floor(slot * (1.0 / 16.0))
                upper = jnp.floor(slot * (1.0 / 16.0)) - 2.0 * jnp.floor(slot * (1.0 / 32.0))
                hots.append(
                    tiles_over_rows(16.0 * jnp.floor(slot * (1.0 / 32.0)) + low, 128)
                )
                upper = as_column(upper)
                same = jnp.where((lane < 64) == (side == 0), block, turned)
                kept = jnp.where((lane >= 64) == (upper > 0.5), same, 0.0)
                high = kept.astype(BF16)
                rest = (kept - high.astype(F32)).astype(BF16)
                rows.append(jnp.concatenate([high, rest], axis=1))
            part = mm(jnp.concatenate(hots, axis=1), jnp.concatenate(rows, axis=0), 1, 0)
            acc[...] += part
            return carry

        lax.fori_loop(first, last, pair, 0)

    for copy in (z3, z4, z5, z6):
        copy.wait_recv()
    DPL[...] = DPL[...] + (ZL[...].astype(F32) + ZR[...].astype(F32))
    acc[...] = jnp.zeros_like(acc)
    segment(0, 1)
    for copy in (h0c, h0d, h0e, h0f):
        copy.wait_recv()
    for k in range(4):
        Q[0, k] = R0[x, k, :, LO] + (RV[0, 0, k].astype(F32) + RV[0, 1, k].astype(F32))
    t0 = ring(0, "dp_1", y)
    segment(1, 3)
    for copy in (h1c, h1d, h1e, h1f):
        copy.wait_recv()
    for k in range(4):
        Q[1, k] = R0[k, y, :, HI] + (RV[1, 0, k].astype(F32) + RV[1, 1, k].astype(F32))
    t1 = ring(1, "dp_0", x)
    u0 = ring_relay(0, "dp_1", t0)
    segment(3, 5)
    u1 = ring_relay(1, "dp_0", t1)
    segment(5, 8)
    total = acc[:, :128] + acc[:, 128:]
    slots[...] = total.astype(BF16).reshape(128, 16, 128)
    few = jnp.sum((total * total).reshape(256, 8, 128), axis=0)

    def send_slots(i, carry):
        p = (me + i) % 128
        pltpu.make_async_remote_copy(
            src_ref=slots.at[p], dst_ref=arrived_ref.at[me], send_sem=bulk.at[4],
            recv_sem=bulk.at[5], device_id=place(p), device_id_type=MESH,
        ).start()
        return carry

    for copy in u0 + u1:
        copy.wait_recv()
    lower = Q[0, y] + (RV2[0, 0] + RV2[0, 1])
    upper = Q[1, x] + (RV2[1, 0] + RV2[1, 1])
    grad_ref[:, LO] = lower
    grad_ref[:, HI] = upper
    GA[x, y, c, :, LO] = lower.astype(BF16)
    GA[x, y, c, :, HI] = upper.astype(BF16)
    ga = Spread(GA, go_to, (x, y, c, z))
    ga.first()
    both = lower * lower + upper * upper
    both = jnp.sum(both.reshape(4, 8, 1024), axis=0)
    for t in range(8):
        few = few + both[:, 128 * t : 128 * t + 128]
    small = sv.at[pl.ds(0, 31)]
    pltpu.make_async_copy(small, small, bulk.at[2]).wait()
    pltpu.make_async_copy(small, small, bulk.at[3]).wait()
    bias_sum = jnp.sum(rv[...], axis=0)
    ns[...] = jnp.sum(few, axis=0, keepdims=True) + bias_sum * bias_sum

    def send_norm(i, carry):
        p = (me + i) % 128
        pltpu.make_async_remote_copy(
            src_ref=ns, dst_ref=NR.at[me], send_sem=bulk.at[6],
            recv_sem=bulk.at[7], device_id=place(p), device_id_type=MESH,
        ).start()
        return carry

    lax.fori_loop(1, 128, send_norm, 0)
    lax.fori_loop(1, 128, send_slots, 0)
    NR[me] = ns[...]
    arrived_ref[me] = slots[me]
    aa.last()
    put_aa = pltpu.make_async_copy(AA, aa_out, local.at[2])
    put_aa.start()
    ga.second()
    ga.third()
    ga.fourth()
    lot = NR.at[pl.ds(0, 127)]
    pltpu.make_async_copy(lot, lot, bulk.at[7]).wait()
    lanes = jnp.sum(NR[...], axis=0)
    norm = jnp.sum(lanes, axis=1, keepdims=True)
    scale = clip_norm / jnp.maximum(jnp.sqrt(norm), clip_norm)
    scale_ref[...] = jnp.broadcast_to(scale, (8, 128))
    ga.fifth()
    many = arrived_ref.at[pl.ds(0, 127)]
    pltpu.make_async_copy(many, many, bulk.at[5]).wait()
    ga.last()
    put_ga = pltpu.make_async_copy(GA, ga_out, local.at[3])
    put_ga.start()
    pltpu.make_async_copy(lot, lot, bulk.at[6]).wait()
    pltpu.make_async_copy(many, many, bulk.at[4]).wait()
    lot = idsend.at[pl.ds(0, 127)]
    pltpu.make_async_copy(lot, lot, bulk.at[0]).wait()
    pltpu.make_async_copy(lot, lot, bulk.at[1]).wait()
    cp.drain()
    put_aa.wait()
    put_ga.wait()


def finish_kernel(
    arrived_ref, rids_ref, scale_ref, table_ref, accum_ref, grad_ref, dense_ref,
    ga_any, aa_any, w_any,
    new_ref, accum_new_ref, dense_new_ref, wn_any,
    acc, ids, GA, AA, W, WN, sem, osem,
):
    chunk = 128
    count = 1024 // chunk
    loads = []
    for i in range(count):
        rows = pl.ds(i * chunk, chunk)
        for j, (src, dst) in enumerate(((ga_any, GA), (aa_any, AA), (w_any, W))):
            copy = pltpu.make_async_copy(src.at[rows], dst.at[rows], sem.at[i, j])
            copy.start()
            loads.append(copy)
    scale = scale_ref[0:1, 0:1]
    clipped = scale * grad_ref[...]
    dense_new_ref[...] = dense_ref[...] + clipped * clipped

    lane16 = iota((16, 128), 1) // 16
    for upper in range(2):
        lined = jnp.zeros((16, 128), F32)
        for d in range(8):
            piece = rids_ref[:, d, :].astype(F32)
            lined = jnp.where(lane16 == d, pltpu.roll(piece, (16 * d - 16 * upper) % 128, 1), lined)
        ids[upper] = lined

    pairs = acc.shape[0]
    acc[...] = jnp.zeros_like(acc)
    step = 256

    def part(t, carry):
        lane = iota((step, 128), 1)
        base = pl.multiple_of(t * step, step)
        block = arrived_ref[pl.ds(base, step), :].astype(F32)
        turned = pltpu.roll(block, 64, 1)
        hots, values = [], []
        for side in range(2):
            row = jnp.concatenate(
                [ids[side, pl.ds(2 * t, 1), :], ids[side, pl.ds(2 * t + 1, 1), :]], axis=1
            )
            above = row >= float(pairs)
            hots.append(tiles_over_rows(jnp.where(above, row - float(pairs), row), pairs // 16))
            high = as_column(jnp.where(above, 1.0, 0.0))
            same = jnp.where((lane < 64) == (side == 0), block, turned)
            values.append(jnp.where((lane >= 64) == (high > 0.5), same, 0.0).astype(BF16))
        acc[...] += mm(jnp.concatenate(hots, axis=1), jnp.concatenate(values, axis=0), 1, 0)
        return carry

    lax.fori_loop(0, arrived_ref.shape[0] // step, part, 0)
    for p in range(pairs // 128):
        both = acc[128 * p : 128 * p + 128, :].T * scale
        for upper in range(2):
            r = both[64 * upper : 64 * upper + 64, :]
            line = p + upper * (pairs // 128)
            fresh = accum_ref[line : line + 1, :] + jnp.sum(r * r, axis=0, keepdims=True) / 64.0
            accum_new_ref[line : line + 1, :] = fresh
            at = line * 128
            new_ref[:, at : at + 128] = table_ref[:, at : at + 128] - table_rate * r / (
                jnp.sqrt(fresh) + adagrad_eps
            )

    for copy in loads:
        copy.wait()

    def weights(i, carry):
        rows = pl.ds(pl.multiple_of(i * chunk, chunk), chunk)

        def tile(t, carry):
            cols = pl.ds(pl.multiple_of(t * 512, 512), 512)
            g = scale * GA[rows, cols].astype(F32)
            fresh = AA[rows, cols].astype(F32) + g * g
            WN[rows, cols] = (
                W[rows, cols].astype(F32) - dense_rate * g / (jnp.sqrt(fresh) + adagrad_eps)
            ).astype(BF16)
            return carry

        lax.fori_loop(0, 4, tile, 0)
        pltpu.make_async_copy(WN.at[rows], wn_any.at[rows], osem).start()
        return carry

    lax.fori_loop(0, count, weights, 0)
    pltpu.make_async_copy(WN, wn_any, osem).wait()


def shape(dims, kind):
    return jax.ShapeDtypeStruct(dims, kind)


def body(
    slab_values,
    row_ids,
    peer_counts,
    lookup_slots,
    labels,
    sample_weight,
    weight_in,
    bias_in,
    weight_out,
    dense_accum,
    table_rows,
    table_accum,
):
    V = pltpu.VMEM
    DMA = pltpu.SemaphoreType.DMA
    whole = (4, 4, 2, 32, 2048)
    ga, aa, arrived, rids, scale, grad = pl.pallas_call(
        step_kernel,
        out_shape=(
            shape(whole, BF16), shape(whole, BF16), shape((128, 16, 128), BF16),
            shape((128, 1, 128), I32), shape((8, 128), F32), shape((32, 2048), F32),
        ),
        in_specs=[VM] * 8 + [ANY] * 2,
        out_specs=(ANY, ANY, VM, VM, VM, VM),
        scratch_shapes=[
            V((1024, 2048), BF16), V((32, 2048), F32), V((128, 1, 128), I32),
            V((1024, 1024), BF16), V(whole, F32), V((1024, 2048), BF16),
            V((1024, 2048), BF16), V((256, 128), F32), V((8, 128), F32), V((4, 8, 128), F32),
            V((8, 128), F32), V((8, 2048), F32), V((8, 2048), F32),
            V((32, 1, 128), F32), V((32, 1, 128), F32),
            V((3, 256, 1024), BF16), V((2, 128, 1024), F32),
            V((128, 1024), BF16), V((128, 1024), BF16),
            V((256, 1024), BF16), V((256, 1024), BF16), V((256, 1024), F32),
            V((4, 4, 32, 2048), F32), V((4, 4, 32, 2048), BF16),
            V((2, 2, 2, 32, 1024), BF16), V((2, 2, 4, 32, 1024), BF16),
            V((2, 4, 32, 1024), F32), V((2, 2, 16, 1024), F32), V((2, 2, 32, 1024), F32),
            V(whole, BF16), V(whole, BF16), V((2048, 256), F32), V((128, 16, 128), BF16),
            V((1, 128), F32), V((128, 1, 128), F32),
            DMA((N_COPIES,)), DMA((N_COPIES,)), DMA((8,)), DMA((4,)),
        ],
        compiler_params=pltpu.CompilerParams(
            has_side_effects=True, vmem_limit_bytes=63 * 1024 * 1024, collective_id=0
        ),
        name="step",
    )(
        lookup_slots.T,
        peer_counts,
        slab_values[0].reshape(2048, 128),
        row_ids[0].T,
        labels.reshape(8, 128),
        sample_weight.reshape(8, 128),
        bias_in.reshape(1, 2048),
        weight_out.astype(F32).reshape(1, 2048),
        weight_in,
        dense_accum,
    )
    table_new, table_accum_new, accum_new, weight_new = pl.pallas_call(
        finish_kernel,
        out_shape=(
            shape((64, 4096), F32), shape((32, 128), F32), shape((32, 2048), F32),
            shape((1024, 2048), BF16),
        ),
        in_specs=[VM] * 7 + [ANY] * 3,
        out_specs=(VM, VM, VM, ANY),
        scratch_shapes=[
            V((2048, 128), F32), V((2, 16, 128), F32),
            V((1024, 2048), BF16), V((1024, 2048), BF16), V((1024, 2048), BF16),
            V((1024, 2048), BF16), DMA((8, 3)), DMA,
        ],
        name="finish",
    )(
        arrived.reshape(2048, 128),
        rids.reshape(16, 8, 128),
        scale,
        table_rows.T,
        table_accum.reshape(32, 128),
        grad,
        dense_accum,
        ga.reshape(1024, 2048),
        aa.reshape(1024, 2048),
        weight_in,
    )
    return (weight_new, accum_new, table_new.T, table_accum_new.reshape(4096))


def solution(mesh):
    torus = Mesh(mesh.devices.reshape(4, 4, 2, mesh.shape["mp"]), ("dp_0", "dp_1", "dp_2", "mp"))
    placed = (
        P(DP_MP, None, None),
        P(DP_MP, None, None),
        P(DP_MP, None),
        P(DP_MP, None),
        P(DP),
        P(DP),
        P(None, "mp"),
        P("mp"),
        P("mp"),
        P(DP, "mp"),
        P(DP_MP, None),
        P(DP_MP),
    )
    return jax.shard_map(
        body,
        mesh=torus,
        in_specs=placed,
        out_specs=(P(None, "mp"), P(DP, "mp"), P(DP_MP, None), P(DP_MP)),
        check_vma=False,
    )
```

```python
import functools

import jax
import jax.numpy as jnp
from jax import lax
from jax.experimental import pallas as pl
from jax.experimental.pallas import tpu as pltpu
from jax.sharding import Mesh
from jax.sharding import PartitionSpec as P

DP = ("dp_0", "dp_1", "dp_2")
DP_MP = ("dp_0", "dp_1", "dp_2", "mp")

clip_norm = 1.0
dense_rate = 0.02
table_rate = 0.5
adagrad_eps = 1e-10

F32 = jnp.float32
BF16 = jnp.bfloat16
I32 = jnp.int32
MESH = pl.DeviceIdType.MESH
LOGICAL = pl.DeviceIdType.LOGICAL
VM = pl.BlockSpec(memory_space=pltpu.VMEM)
ANY = pl.BlockSpec(memory_space=pl.ANY)


def mm(a, b, ca, cb):
    return lax.dot_general(a, b, (((ca,), (cb,)), ((), ())), preferred_element_type=F32)


def iota(shape, dim):
    return lax.broadcasted_iota(I32, shape, dim)


def position():
    return tuple(lax.axis_index(a) for a in DP_MP)


def to_all(me, emit):
    for u in range(1, 8):
        emit(lax.rem(me + u, 128))

    def more(j, carry):
        base = me + 8 * j
        for u in range(8):
            emit(lax.rem(base + u, 128))
        return carry

    lax.fori_loop(1, 16, more, 0)


class Copies:
    def __init__(self, send, recv):
        self.send, self.recv, self.used, self.open = send, recv, 0, []

    def go(self, src, dst, where):
        k = self.used
        self.used += 1
        copy = pltpu.make_async_remote_copy(
            src_ref=src,
            dst_ref=dst,
            send_sem=self.send.at[k],
            recv_sem=self.recv.at[k],
            device_id=where,
            device_id_type=MESH,
        )
        copy.start()
        self.open.append(copy)
        return copy

    def drain(self):
        for copy in self.open:
            copy.wait_send()


def owner_bounds(counts_ref):
    counts = jnp.broadcast_to(counts_ref[...].astype(F32), (128, 128))
    upto = jnp.where(iota((128, 128), 0) <= iota((128, 128), 1), 1.0, 0.0).astype(BF16)
    ends = mm(counts.astype(BF16), upto, 1, 0)
    return (ends - counts).T, ends.T


def slot_rows(lookups, starts, ends):
    q = lookups.astype(F32)
    outs = []
    for part in range(q.shape[1] // 128):
        row = q[:, part * 128 : part * 128 + 128]
        hit = (row >= starts) & (row < ends)
        owner = iota((128, 128), 0).astype(F32)
        shift = jnp.sum(jnp.where(hit, owner * 32.0 - starts, 0.0), axis=0, keepdims=True)
        outs.append(row + shift)
    return jnp.concatenate(outs, axis=1)


def as_column(row):
    parts = []
    for part in range(row.shape[1] // 128):
        piece = row[:, part * 128 : part * 128 + 128]
        parts.append(jnp.broadcast_to(piece, (128, 128)).T)
    return jnp.concatenate(parts, axis=0)


def tiles_over_rows(index, count):
    high = jnp.floor(index * (1.0 / 16.0))
    low = index - 16.0 * high
    n = index.shape[1]
    inner = jnp.where(iota((16, n), 0).astype(F32) == low, 1.0, 0.0).astype(BF16)
    high = jnp.broadcast_to(high, (16, n)).astype(BF16)
    zero = jnp.zeros((16, n), BF16)
    return jnp.concatenate(
        [jnp.where(high == jnp.asarray(t, BF16), inner, zero) for t in range(count)], axis=0
    )


def tiles_over_lanes(column, count):
    high = jnp.floor(column * (1.0 / 128.0))
    low = column - 128.0 * high
    inner = jnp.where(iota(column.shape, 1).astype(F32) == low, 1.0, 0.0).astype(BF16)
    high = high.astype(BF16)
    zero = jnp.zeros(column.shape, BF16)
    return jnp.concatenate(
        [jnp.where(high == jnp.asarray(t, BF16), inner, zero) for t in range(count)], axis=1
    )


class Spread:
    LO, HI = slice(0, 1024), slice(1024, 2048)
    T, B = slice(0, 16), slice(16, 32)

    def __init__(self, ref, go, where, out, sem):
        self.ref, self.go, self.out, self.sem, self.written = ref, go, out, sem, []
        self.x, self.y, self.c, _ = where
        self.xr, self.xl, self.xo = ((self.x + d) % 4 for d in (1, 3, 2))
        self.yr, self.yl, self.yo = ((self.y + d) % 4 for d in (1, 3, 2))
        self.partner = {"dp_2": 1 - self.c}
        self.d, self.pieces = [], []

    def across(self, *pieces):
        for piece in pieces:
            self.d.append(self.same(piece, self.partner))
            self.pieces.append(piece)
            self.write(piece)

    def from_partner(self, first, last):
        for k in range(first, last):
            self.d[k].wait_recv()
            a, b, _, rows, cols = self.pieces[k]
            self.write((a, b, 1 - self.c, rows, cols))

    def write(self, piece):
        k = len(self.written)
        copy = pltpu.make_async_copy(self.ref.at[piece], self.out.at[piece], self.sem.at[k])
        copy.start()
        self.written.append(copy)

    def same(self, piece, where):
        ref = self.ref.at[piece]
        return self.go(ref, ref, where)

    def first(self):
        x, y, c = self.x, self.y, self.c
        every = slice(None)
        self.p1 = self.same((x, y, c, every, self.LO), {"dp_0": self.xr})
        self.p2 = self.same((x, y, c, every, self.LO), {"dp_0": self.xl})
        self.q1 = self.same((x, y, c, every, self.HI), {"dp_1": self.yr})
        self.q2 = self.same((x, y, c, every, self.HI), {"dp_1": self.yl})

    def second(self):
        x, y, c = self.x, self.y, self.c
        self.p1.wait_recv()
        self.p3 = self.same((self.xl, y, c, self.T, self.LO), {"dp_0": self.xr})
        self.p2.wait_recv()
        self.p4 = self.same((self.xr, y, c, self.B, self.LO), {"dp_0": self.xl})
        self.q1.wait_recv()
        self.q3 = self.same((x, self.yl, c, self.T, self.HI), {"dp_1": self.yr})
        self.q2.wait_recv()
        self.q4 = self.same((x, self.yr, c, self.B, self.HI), {"dp_1": self.yl})

    def third(self):
        x, y, c = self.x, self.y, self.c
        every = slice(None)
        self.p3.wait_recv()
        self.p4.wait_recv()
        mine, other = (every, y, c, every, self.LO), (x, every, c, every, self.HI)
        self.p5 = self.same(mine, {"dp_1": self.yr})
        self.p6 = self.same(mine, {"dp_1": self.yl})
        self.q3.wait_recv()
        self.q4.wait_recv()
        self.q5 = self.same(other, {"dp_0": self.xr})
        self.q6 = self.same(other, {"dp_0": self.xl})
        self.across(mine, other)

    def fourth(self):
        c = self.c
        every = slice(None)
        self.p5.wait_recv()
        self.p7 = self.same((slice(0, 2), self.yl, c, every, self.LO), {"dp_1": self.yr})
        self.p6.wait_recv()
        self.p8 = self.same((slice(2, 4), self.yr, c, every, self.LO), {"dp_1": self.yl})
        self.q5.wait_recv()
        self.q7 = self.same((self.xl, slice(0, 2), c, every, self.HI), {"dp_0": self.xr})
        self.q6.wait_recv()
        self.q8 = self.same((self.xr, slice(2, 4), c, every, self.HI), {"dp_0": self.xl})
        self.across(*((every, n, c, every, self.LO) for n in (self.yl, self.yr)))
        self.across(*((n, every, c, every, self.HI) for n in (self.xl, self.xr)))
        self.from_partner(0, 2)

    def fifth(self):
        c = self.c
        every = slice(None)
        self.p7.wait_recv()
        self.p8.wait_recv()
        self.across((every, self.yo, c, every, self.LO))
        self.q7.wait_recv()
        self.q8.wait_recv()
        self.across((self.xo, every, c, every, self.HI))
        self.from_partner(2, 6)

    def last(self):
        self.from_partner(6, 8)

    def close(self):
        for copy in self.written:
            copy.wait()


N_COPIES = 140


def step_kernel(
    lookups_ref, counts_ref, slab_ref, ids_ref, label_ref, sw_ref, bias_ref, wout_ref,
    w_any, accum_any,
    ga_out, aa_out, arrived_ref, rids_ref, scale_ref, grad_ref,
    W, A, idsend, G, fac, hidden, dact, pacc, lg, LR, DL, gb, go, sv, rv,
    ZS, Df, ZRL, ZRR, ZL, ZR, DPL,
    R0, SB, RL, RV, Q, RL2, RV2,
    GA, AA, acc, slots, ns, NR, SC, slab, wout,
    ssem, rsem, bulk, local, wsem,
):
    x, y, c, z = position()
    dp = (x * 4 + y) * 2 + c
    me = dp * 4 + z
    cp = Copies(ssem, rsem)
    go_to = cp.go
    zr, zl, zo = (z + 1) % 4, (z + 3) % 4, (z + 2) % 4
    xr, xl, xo = (x + 1) % 4, (x + 3) % 4, (x + 2) % 4
    yr, yl, yo = (y + 1) % 4, (y + 3) % 4, (y + 2) % 4
    LO, HI = slice(0, 1024), slice(1024, 2048)

    barrier = pltpu.get_barrier_semaphore()

    def greet(p):
        pl.semaphore_signal(barrier, inc=1, device_id=p, device_id_type=LOGICAL)

    to_all(me, greet)
    fetch_a = pltpu.make_async_copy(accum_any, A, local.at[1])
    fetch_a.start()
    fetch_w = pltpu.make_async_copy(w_any, W, local.at[0])
    fetch_w.start()

    starts, ends = owner_bounds(counts_ref)
    own_rows = pl.ds(pl.multiple_of(z * 256, 256), 256)

    def gather_pair(k):
        lane = iota((256, 128), 1)
        got = []
        for side in range(2):
            slot = slot_rows(lookups_ref[2 * k + side : 2 * k + side + 1, :], starts, ends)
            column = as_column(slot)
            half = jnp.floor(column * 0.5)
            odd = column - 2.0 * half
            both = mm(tiles_over_lanes(half, 16), slab[...], 1, 0)
            one = jnp.where((lane >= 64) == (odd > 0.5), both, 0.0)
            got.append(one + pltpu.roll(one, 64, 1))
        G[own_rows, k * 128 : k * 128 + 128] = jnp.where(lane < 64, got[0], got[1]).astype(BF16)

    def block(src, k):
        return G.at[pl.ds(pl.multiple_of(src * 256, 256), 256), k * 256 : k * 256 + 256]

    def send_ids(p):
        pltpu.make_async_remote_copy(
            src_ref=idsend.at[p], dst_ref=rids_ref.at[me], send_sem=bulk.at[0],
            recv_sem=bulk.at[1], device_id=p, device_id_type=LOGICAL,
        ).start()

    right, left = {}, {}

    def send_block(k):
        right[k] = go_to(block(z, k), block(z, k), {"mp": zr})
        left[k] = go_to(block(z, k), block(z, k), {"mp": zl})

    for k in range(16):
        acc[pl.ds(k, 128, stride=16), :] = slab_ref[:, k * 128 : k * 128 + 128].astype(F32)
    slab[...] = acc[...].astype(BF16)
    for k in range(16):
        wout[:, k * 128 : k * 128 + 128] = wout_ref[k : k + 1, :].astype(F32)
    gather_pair(0)
    gather_pair(1)
    fetch_a.wait()
    AA[x, y, c] = A[...].astype(BF16)
    pl.semaphore_wait(barrier, 127)
    send_block(0)
    aa = Spread(AA, go_to, (x, y, c, z), aa_out, wsem.at[0])
    aa.first()
    gather_pair(4)
    gather_pair(5)
    send_block(2)
    gather_pair(2)
    gather_pair(3)
    send_block(1)
    gather_pair(6)
    gather_pair(7)
    send_block(3)
    turned = jnp.concatenate([ids_ref[...].astype(F32), jnp.zeros((96, 128), F32)], axis=0)
    idsend[...] = turned.T.astype(I32).reshape(128, 1, 128)
    to_all(me, send_ids)
    rids_ref[me] = idsend[me]
    fetch_w.wait()

    def forward(src):
        rows = pl.ds(pl.multiple_of(src * 256, 256), 256)
        pacc[...] = jnp.zeros_like(pacc)

        def tile(t, carry):
            cols = pl.ds(pl.multiple_of(t * 512, 512), 512)
            a = mm(G[rows, :], W[:, cols], 1, 0) + bias_ref[:, cols]
            wo = wout[:, cols]
            sg = lax.logistic(a)
            h = (a * sg).astype(BF16)
            hidden[rows, cols] = h
            fac[src, :, :, :, cols] = (wo * sg * (1.0 + a * (1.0 - sg))).reshape(4, 2, 32, 512)
            m = h.astype(F32) * wo
            pacc[...] += (m[:, 0:128] + m[:, 128:256]) + (m[:, 256:384] + m[:, 384:512])
            return carry

        lax.fori_loop(0, 4, tile, 0)
        for s in range(2):
            line = jnp.sum(pacc[128 * s : 128 * s + 128, :].T, axis=0, keepdims=True)
            lg[pl.ds(src * 2 + s, 1), :] = line

    right[0].wait_recv()
    f0 = go_to(block(zl, 0), block(zl, 0), {"mp": zr})
    left[2].wait_recv()
    f2 = go_to(block(zr, 2), block(zr, 2), {"mp": zl})
    forward(z)
    right[1].wait_recv()
    f1 = go_to(block(zl, 1), block(zl, 1), {"mp": zr})
    left[3].wait_recv()
    f3 = go_to(block(zr, 3), block(zr, 3), {"mp": zl})
    aa.second()
    right[2].wait_recv()
    right[3].wait_recv()
    forward(zl)
    left[0].wait_recv()
    left[1].wait_recv()
    forward(zr)
    aa.third()
    for copy in (f0, f1, f2, f3):
        copy.wait_recv()
    forward(zo)

    sent = [go_to(lg, LR.at[z], {"mp": (z + d) % 4}) for d in (1, 2, 3)]
    LR[z] = lg[...]
    for copy in sent:
        copy.wait_recv()
    logit = (LR[0] + LR[1]) + (LR[2] + LR[3])
    DL[...] = sw_ref[...] * (lax.logistic(logit) - label_ref[...].astype(F32))

    def column(g):
        return jnp.broadcast_to(DL[pl.ds(g, 1), :], (128, 128)).T

    def dact_part(g, carry):
        rows = pl.ds(pl.multiple_of(g * 128, 128), 128)
        col = column(g)
        for t in range(16):
            cols = slice(128 * t, 128 * t + 128)
            f = fac[g // 2, pl.ds((g % 2) * 2, 2), :, :, cols].reshape(128, 128)
            dact[rows, cols] = (f * col).astype(BF16)
        return carry

    lax.fori_loop(0, 8, dact_part, 0)

    def sums_part(g, carry):
        rows = pl.ds(pl.multiple_of(g * 128, 128), 128)
        col = column(g)
        for t in range(16):
            cols = slice(128 * t, 128 * t + 128)
            d = dact[rows, cols].astype(F32)
            gb[:, cols] += jnp.sum(d.reshape(16, 8, 128), axis=0)
            m = hidden[rows, cols].astype(F32) * col
            go[:, cols] += jnp.sum(m.reshape(16, 8, 128), axis=0)
        return carry

    def dpool(dest, put):
        rows = pl.ds(pl.multiple_of(dest * 256, 256), 256)

        def tile(t, carry):
            at = pl.multiple_of(t * 512, 512)
            put(mm(dact[rows, :], W[pl.ds(at, 512), :], 1, 1), pl.ds(at, 512))
            return carry

        lax.fori_loop(0, 2, tile, 0)

    def put_far(d, cols):
        ZS[0, :, cols] = d.astype(BF16)

    dpool(zo, put_far)
    z1 = go_to(ZS.at[0, 0:128], ZRL, {"mp": zr})
    z2 = go_to(ZS.at[0, 128:256], ZRR, {"mp": zl})

    partner = {"dp_2": 1 - c}
    to_core = {}

    def weight_grad(xi, tag):
        at = pl.multiple_of(xi * 256, 256)

        def tile(t, carry):
            cols = pl.ds(pl.multiple_of(t * 512, 512), 512)
            g = mm(G[:, pl.ds(at, 256)], dact[:, cols], 0, 0)
            fac[xi, :, :, :, cols] = g.reshape(4, 2, 32, 512)
            SC[xi, :, :, cols] = fac[xi, :, 1 - c, :, cols].astype(BF16)
            return carry

        lax.fori_loop(0, 4, tile, 0)
        to_core[tag] = go_to(SC.at[xi], R0.at[xi], partner)

    def chip_sum(xi, tag):
        to_core[tag].wait_recv()
        for yi in range(4):
            s = R0[xi, yi].astype(F32) + fac[xi, yi, c]
            fac[xi, yi, c] = s
            SB[xi, yi] = s.astype(BF16)

    def put_right(d, cols):
        Df[0, :, cols] = d[0:128]
        ZS[1, 128:256, cols] = d[128:256].astype(BF16)

    def put_left(d, cols):
        ZS[2, 0:128, cols] = d[0:128].astype(BF16)
        Df[1, :, cols] = d[128:256]

    weight_grad(xo, "o")
    aa.fourth()
    weight_grad(xr, "r")
    dpool(zr, put_right)
    z3 = go_to(ZS.at[1, 128:256], ZL.at[128:256], {"mp": zr})
    chip_sum(xo, "o")
    h0a = go_to(SB.at[xo, 0:2, :, LO], RL.at[0, 0], {"dp_0": xr})
    h0b = go_to(SB.at[xo, 2:4, :, LO], RL.at[0, 1], {"dp_0": xl})
    weight_grad(xl, "l")
    dpool(zl, put_left)
    z4 = go_to(ZS.at[2, 0:128], ZR.at[0:128], {"mp": zl})
    chip_sum(xr, "r")
    h0c = go_to(SB.at[xr, 2:4, :, LO], RV.at[0, 0, 2:4], {"dp_0": xr})
    weight_grad(x, "m")
    chip_sum(xl, "l")
    h0d = go_to(SB.at[xl, 0:2, :, LO], RV.at[0, 1, 0:2], {"dp_0": xl})
    z1.wait_recv()
    ZS[1, 0:128, :] = (Df[0] + ZRL[...].astype(F32)).astype(BF16)
    z5 = go_to(ZS.at[1, 0:128], ZL.at[0:128], {"mp": zr})
    z2.wait_recv()
    ZS[2, 128:256, :] = (Df[1] + ZRR[...].astype(F32)).astype(BF16)
    z6 = go_to(ZS.at[2, 128:256], ZR.at[128:256], {"mp": zl})
    chip_sum(x, "m")
    h1a = go_to(SB.at[0:2, yo, :, HI], RL.at[1, 0], {"dp_1": yr})
    h1b = go_to(SB.at[2:4, yo, :, HI], RL.at[1, 1], {"dp_1": yl})
    h1c = go_to(SB.at[2:4, yr, :, HI], RV.at[1, 0, 2:4], {"dp_1": yr})
    h1d = go_to(SB.at[0:2, yl, :, HI], RV.at[1, 1, 0:2], {"dp_1": yl})

    h0a.wait_recv()
    for k in range(2):
        SB[xr, k, :, LO] = (fac[xr, k, c, :, LO] + RL[0, 0, k].astype(F32)).astype(BF16)
    h0e = go_to(SB.at[xr, 0:2, :, LO], RV.at[0, 0, 0:2], {"dp_0": xr})
    h0b.wait_recv()
    for k in range(2):
        SB[xl, 2 + k, :, LO] = (fac[xl, 2 + k, c, :, LO] + RL[0, 1, k].astype(F32)).astype(BF16)
    h0f = go_to(SB.at[xl, 2:4, :, LO], RV.at[0, 1, 2:4], {"dp_0": xl})

    gb[...] = jnp.zeros_like(gb)
    go[...] = jnp.zeros_like(go)
    lax.fori_loop(0, 8, sums_part, 0)
    for t in range(16):
        cols = slice(128 * t, 128 * t + 128)
        sv[t] = jnp.sum(gb[:, cols], axis=0, keepdims=True)
        sv[16 + t] = jnp.sum(go[:, cols], axis=0, keepdims=True)

    def send_small(i, carry):
        p = (dp + i) % 32
        where = {"dp_0": p // 8, "dp_1": (p // 2) % 4, "dp_2": p % 2, "mp": z}
        pltpu.make_async_remote_copy(
            src_ref=sv.at[p], dst_ref=rv.at[dp], send_sem=bulk.at[2],
            recv_sem=bulk.at[3], device_id=where, device_id_type=MESH,
        ).start()
        return carry

    lax.fori_loop(1, 32, send_small, 0)
    rv[dp] = sv[dp]

    def put_own(d, cols):
        DPL[:, cols] = d

    dpool(z, put_own)
    h1a.wait_recv()
    for k in range(2):
        SB[k, yr, :, HI] = (fac[k, yr, c, :, HI] + RL[1, 0, k].astype(F32)).astype(BF16)
    h1e = go_to(SB.at[0:2, yr, :, HI], RV.at[1, 0, 0:2], {"dp_1": yr})
    h1b.wait_recv()
    for k in range(2):
        SB[2 + k, yl, :, HI] = (fac[2 + k, yl, c, :, HI] + RL[1, 1, k].astype(F32)).astype(BF16)
    h1f = go_to(SB.at[2:4, yl, :, HI], RV.at[1, 1, 2:4], {"dp_1": yl})
    aa.fifth()

    def ring(h, axis, n):
        nr, nl, no = (n + 1) % 4, (n + 3) % 4, (n + 2) % 4
        s1 = go_to(Q.at[h, no, 0:16], RL2.at[h, 0], {axis: nr})
        s2 = go_to(Q.at[h, no, 16:32], RL2.at[h, 1], {axis: nl})
        s3 = go_to(Q.at[h, nr, 16:32], RV2.at[h, 0, 16:32], {axis: nr})
        s4 = go_to(Q.at[h, nl, 0:16], RV2.at[h, 1, 0:16], {axis: nl})
        return nr, nl, (s1, s2, s3, s4)

    def ring_relay(h, axis, state):
        nr, nl, (s1, s2, s3, s4) = state
        s1.wait_recv()
        Q[h, nr, 0:16] = Q[h, nr, 0:16] + RL2[h, 0]
        s5 = go_to(Q.at[h, nr, 0:16], RV2.at[h, 0, 0:16], {axis: nr})
        s2.wait_recv()
        Q[h, nl, 16:32] = Q[h, nl, 16:32] + RL2[h, 1]
        s6 = go_to(Q.at[h, nl, 16:32], RV2.at[h, 1, 16:32], {axis: nl})
        return s3, s4, s5, s6

    def segment(first, last):
        def pair(k, carry):
            lane = iota((256, 128), 1)
            block = DPL[:, pl.ds(pl.multiple_of(k * 128, 128), 128)]
            turned = pltpu.roll(block, 64, 1)
            hots, rows = [], []
            for side in range(2):
                slot = slot_rows(lookups_ref[pl.ds(2 * k + side, 1), :], starts, ends)
                low = slot - 16.0 * jnp.floor(slot * (1.0 / 16.0))
                upper = jnp.floor(slot * (1.0 / 16.0)) - 2.0 * jnp.floor(slot * (1.0 / 32.0))
                hots.append(
                    tiles_over_rows(16.0 * jnp.floor(slot * (1.0 / 32.0)) + low, 128)
                )
                upper = as_column(upper)
                same = jnp.where((lane < 64) == (side == 0), block, turned)
                kept = jnp.where((lane >= 64) == (upper > 0.5), same, 0.0)
                high = kept.astype(BF16)
                rest = (kept - high.astype(F32)).astype(BF16)
                rows.append(jnp.concatenate([high, rest], axis=1))
            part = mm(jnp.concatenate(hots, axis=1), jnp.concatenate(rows, axis=0), 1, 0)
            acc[...] += part[:, :128] + part[:, 128:]
            return carry

        lax.fori_loop(first, last, pair, 0)

    for copy in (z3, z4, z5, z6):
        copy.wait_recv()
    DPL[...] = DPL[...] + (ZL[...].astype(F32) + ZR[...].astype(F32))
    acc[...] = jnp.zeros_like(acc)
    segment(0, 3)
    for copy in (h0c, h0d, h0e, h0f):
        copy.wait_recv()
    for k in range(4):
        Q[0, k] = fac[x, k, c, :, LO] + (RV[0, 0, k].astype(F32) + RV[0, 1, k].astype(F32))
    t0 = ring(0, "dp_1", y)
    segment(3, 5)
    for copy in (h1c, h1d, h1e, h1f):
        copy.wait_recv()
    for k in range(4):
        Q[1, k] = fac[k, y, c, :, HI] + (RV[1, 0, k].astype(F32) + RV[1, 1, k].astype(F32))
    t1 = ring(1, "dp_0", x)
    u0 = ring_relay(0, "dp_1", t0)
    segment(5, 7)
    u1 = ring_relay(1, "dp_0", t1)
    segment(7, 8)
    total = acc[...]
    slots[...] = total.astype(BF16).reshape(128, 16, 128)
    few = jnp.sum((total * total).reshape(256, 8, 128), axis=0)

    def send_slots(p):
        pltpu.make_async_remote_copy(
            src_ref=slots.at[p], dst_ref=arrived_ref.at[me], send_sem=bulk.at[4],
            recv_sem=bulk.at[5], device_id=p, device_id_type=LOGICAL,
        ).start()

    for copy in u0 + u1:
        copy.wait_recv()
    lower = Q[0, y] + (RV2[0, 0] + RV2[0, 1])
    upper = Q[1, x] + (RV2[1, 0] + RV2[1, 1])
    grad_ref[:, LO] = lower
    grad_ref[:, HI] = upper
    GA[x, y, c, :, LO] = lower.astype(BF16)
    GA[x, y, c, :, HI] = upper.astype(BF16)
    ga = Spread(GA, go_to, (x, y, c, z), ga_out, wsem.at[1])
    ga.first()
    both = lower * lower + upper * upper
    both = jnp.sum(both.reshape(4, 8, 1024), axis=0)
    for t in range(8):
        few = few + both[:, 128 * t : 128 * t + 128]
    small = sv.at[pl.ds(0, 31)]
    pltpu.make_async_copy(small, small, bulk.at[2]).wait()
    pltpu.make_async_copy(small, small, bulk.at[3]).wait()
    bias_sum = jnp.sum(rv[...], axis=0)
    ns[...] = jnp.sum(few, axis=0, keepdims=True) + bias_sum * bias_sum

    def send_norm(p):
        pltpu.make_async_remote_copy(
            src_ref=ns, dst_ref=NR.at[me], send_sem=bulk.at[6],
            recv_sem=bulk.at[7], device_id=p, device_id_type=LOGICAL,
        ).start()

    to_all(me, send_norm)
    ga.second()
    to_all(me, send_slots)
    NR[me] = ns[...]
    arrived_ref[me] = slots[me]
    ga.third()
    aa.last()
    lot = NR.at[pl.ds(0, 127)]
    pltpu.make_async_copy(lot, lot, bulk.at[7]).wait()
    lanes = jnp.sum(NR[...], axis=0)
    norm = jnp.sum(lanes, axis=1, keepdims=True)
    scale = clip_norm / jnp.maximum(jnp.sqrt(norm), clip_norm)
    scale_ref[...] = jnp.broadcast_to(scale, (8, 128))
    ga.fourth()
    ga.fifth()
    many = arrived_ref.at[pl.ds(0, 127)]
    pltpu.make_async_copy(many, many, bulk.at[5]).wait()
    ga.last()
    pltpu.make_async_copy(lot, lot, bulk.at[6]).wait()
    pltpu.make_async_copy(many, many, bulk.at[4]).wait()
    lot = idsend.at[pl.ds(0, 127)]
    pltpu.make_async_copy(lot, lot, bulk.at[0]).wait()
    pltpu.make_async_copy(lot, lot, bulk.at[1]).wait()
    cp.drain()
    aa.close()
    ga.close()


def finish_kernel(
    arrived_ref, rids_ref, scale_ref, table_ref, accum_ref, grad_ref, dense_ref,
    ga_any, aa_any, w_any,
    new_ref, accum_new_ref, dense_new_ref, wn_any,
    acc, ids, GA, AA, W, WN, sem, osem,
):
    chunk = 128
    count = 1024 // chunk
    for i in range(count):
        rows = pl.ds(i * chunk, chunk)
        for j, (src, dst) in enumerate(((ga_any, GA), (aa_any, AA), (w_any, W))):
            copy = pltpu.make_async_copy(src.at[rows], dst.at[rows], sem.at[i, j])
            copy.start()
    scale = scale_ref[0:1, 0:1]
    clipped = scale * grad_ref[...]
    dense_new_ref[...] = dense_ref[...] + clipped * clipped

    lane16 = iota((16, 128), 1) // 16
    for upper in range(2):
        lined = jnp.zeros((16, 128), F32)
        for d in range(8):
            piece = rids_ref[:, d, :].astype(F32)
            lined = jnp.where(lane16 == d, pltpu.roll(piece, (16 * d - 16 * upper) % 128, 1), lined)
        ids[upper] = lined

    pairs = acc.shape[0]
    acc[...] = jnp.zeros_like(acc)
    step = 256

    def part(t, carry):
        lane = iota((step, 128), 1)
        base = pl.multiple_of(t * step, step)
        block = arrived_ref[pl.ds(base, step), :].astype(F32)
        turned = pltpu.roll(block, 64, 1)
        hots, values = [], []
        for side in range(2):
            row = jnp.concatenate(
                [ids[side, pl.ds(2 * t, 1), :], ids[side, pl.ds(2 * t + 1, 1), :]], axis=1
            )
            above = row >= float(pairs)
            hots.append(tiles_over_rows(jnp.where(above, row - float(pairs), row), pairs // 16))
            high = as_column(jnp.where(above, 1.0, 0.0))
            same = jnp.where((lane < 64) == (side == 0), block, turned)
            values.append(jnp.where((lane >= 64) == (high > 0.5), same, 0.0).astype(BF16))
        acc[...] += mm(jnp.concatenate(hots, axis=1), jnp.concatenate(values, axis=0), 1, 0)
        rows = pl.ds(pl.multiple_of(t * chunk, chunk), chunk)
        for j, (src, dst) in enumerate(((ga_any, GA), (aa_any, AA), (w_any, W))):
            pltpu.make_async_copy(src.at[rows], dst.at[rows], sem.at[t, j]).wait()
        for q in range(16):
            cols = slice(128 * q, 128 * q + 128)
            g = scale * GA[rows, cols].astype(F32)
            r = lax.rsqrt(AA[rows, cols].astype(F32) + g * g)
            r = r - (adagrad_eps * r) * r
            WN[rows, cols] = (W[rows, cols].astype(F32) - (dense_rate * g) * r).astype(BF16)
        pltpu.make_async_copy(WN.at[rows], wn_any.at[rows], osem).start()
        return carry

    lax.fori_loop(0, count, part, 0)
    for p in range(pairs // 128):
        both = acc[128 * p : 128 * p + 128, :].T * scale
        for upper in range(2):
            r = both[64 * upper : 64 * upper + 64, :]
            line = p + upper * (pairs // 128)
            fresh = accum_ref[line : line + 1, :] + jnp.sum(r * r, axis=0, keepdims=True) / 64.0
            accum_new_ref[line : line + 1, :] = fresh
            at = line * 128
            rate = table_rate / (jnp.sqrt(fresh) + adagrad_eps)
            new_ref[:, at : at + 128] = table_ref[:, at : at + 128] - r * rate

    pltpu.make_async_copy(WN, wn_any, osem).wait()


def shape(dims, kind):
    return jax.ShapeDtypeStruct(dims, kind)


def body(
    slab_values,
    row_ids,
    peer_counts,
    lookup_slots,
    labels,
    sample_weight,
    weight_in,
    bias_in,
    weight_out,
    dense_accum,
    table_rows,
    table_accum,
):
    V = pltpu.VMEM
    DMA = pltpu.SemaphoreType.DMA
    whole = (4, 4, 2, 32, 2048)
    ga, aa, arrived, rids, scale, grad = pl.pallas_call(
        step_kernel,
        out_shape=(
            shape(whole, BF16), shape(whole, BF16), shape((128, 16, 128), BF16),
            shape((128, 1, 128), I32), shape((8, 128), F32), shape((32, 2048), F32),
        ),
        in_specs=[VM] * 8 + [ANY] * 2,
        out_specs=(ANY, ANY, VM, VM, VM, VM),
        scratch_shapes=[
            V((1024, 2048), BF16), V((32, 2048), F32), V((128, 1, 128), I32),
            V((1024, 1024), BF16), V(whole, F32), V((1024, 2048), BF16),
            V((1024, 2048), BF16), V((256, 128), F32), V((8, 128), F32), V((4, 8, 128), F32),
            V((8, 128), F32), V((8, 2048), F32), V((8, 2048), F32),
            V((32, 1, 128), F32), V((32, 1, 128), F32),
            V((3, 256, 1024), BF16), V((2, 128, 1024), F32),
            V((128, 1024), BF16), V((128, 1024), BF16),
            V((256, 1024), BF16), V((256, 1024), BF16), V((256, 1024), F32),
            V((4, 4, 32, 2048), BF16), V((4, 4, 32, 2048), BF16),
            V((2, 2, 2, 32, 1024), BF16), V((2, 2, 4, 32, 1024), BF16),
            V((2, 4, 32, 1024), F32), V((2, 2, 16, 1024), F32), V((2, 2, 32, 1024), F32),
            V(whole, BF16), V(whole, BF16), V((2048, 128), F32), V((128, 16, 128), BF16),
            V((1, 128), F32), V((128, 1, 128), F32), V((4, 4, 32, 2048), BF16),
            V((2048, 128), BF16), V((1, 2048), F32),
            DMA((N_COPIES,)), DMA((N_COPIES,)), DMA((8,)), DMA((2,)), DMA((2, 16)),
        ],
        compiler_params=pltpu.CompilerParams(
            has_side_effects=True, vmem_limit_bytes=63 * 1024 * 1024, collective_id=0
        ),
        name="step",
    )(
        lookup_slots.T,
        peer_counts,
        slab_values[0],
        row_ids[0].T,
        labels.reshape(8, 128),
        sample_weight.reshape(8, 128),
        bias_in.reshape(1, 2048),
        weight_out.reshape(16, 128),
        weight_in,
        dense_accum,
    )
    table_new, table_accum_new, accum_new, weight_new = pl.pallas_call(
        finish_kernel,
        out_shape=(
            shape((64, 4096), F32), shape((32, 128), F32), shape((32, 2048), F32),
            shape((1024, 2048), BF16),
        ),
        in_specs=[VM] * 7 + [ANY] * 3,
        out_specs=(VM, VM, VM, ANY),
        scratch_shapes=[
            V((2048, 128), F32), V((2, 16, 128), F32),
            V((1024, 2048), BF16), V((1024, 2048), BF16), V((1024, 2048), BF16),
            V((1024, 2048), BF16), DMA((8, 3)), DMA,
        ],
        name="finish",
    )(
        arrived.reshape(2048, 128),
        rids.reshape(16, 8, 128),
        scale,
        table_rows.T,
        table_accum.reshape(32, 128),
        grad,
        dense_accum,
        ga.reshape(1024, 2048),
        aa.reshape(1024, 2048),
        weight_in,
    )
    return (weight_new, accum_new, table_new.T, table_accum_new.reshape(4096))


def solution(mesh):
    torus = Mesh(mesh.devices.reshape(4, 4, 2, mesh.shape["mp"]), ("dp_0", "dp_1", "dp_2", "mp"))
    placed = (
        P(DP_MP, None, None),
        P(DP_MP, None, None),
        P(DP_MP, None),
        P(DP_MP, None),
        P(DP),
        P(DP),
        P(None, "mp"),
        P("mp"),
        P("mp"),
        P(DP, "mp"),
        P(DP_MP, None),
        P(DP_MP),
    )
    return jax.shard_map(
        body,
        mesh=torus,
        in_specs=placed,
        out_specs=(P(None, "mp"), P(DP, "mp"), P(DP_MP, None), P(DP_MP)),
        check_vma=False,
    )
```

```python
import functools

import jax
import jax.numpy as jnp
from jax import lax
from jax.experimental import pallas as pl
from jax.experimental.pallas import tpu as pltpu
from jax.sharding import Mesh
from jax.sharding import PartitionSpec as P

DP = ("dp_0", "dp_1", "dp_2")
DP_MP = ("dp_0", "dp_1", "dp_2", "mp")

clip_norm = 1.0
dense_rate = 0.02
table_rate = 0.5
adagrad_eps = 1e-10

F32 = jnp.float32
BF16 = jnp.bfloat16
I32 = jnp.int32
MESH = pl.DeviceIdType.MESH
LOGICAL = pl.DeviceIdType.LOGICAL
VM = pl.BlockSpec(memory_space=pltpu.VMEM)
ANY = pl.BlockSpec(memory_space=pl.ANY)


def mm(a, b, ca, cb):
    return lax.dot_general(a, b, (((ca,), (cb,)), ((), ())), preferred_element_type=F32)


def iota(shape, dim):
    return lax.broadcasted_iota(I32, shape, dim)


def position():
    return tuple(lax.axis_index(a) for a in DP_MP)


def to_all(me, emit, first=0, last=16):
    if first == 0:
        for u in range(1, 8):
            emit(lax.rem(me + u, 128))

    def more(j, carry):
        base = me + 8 * j
        for u in range(8):
            emit(lax.rem(base + u, 128))
        return carry

    lax.fori_loop(max(first, 1), last, more, 0)


class Copies:
    def __init__(self, send, recv):
        self.send, self.recv, self.used, self.open = send, recv, 0, []

    def go(self, src, dst, where):
        k = self.used
        self.used += 1
        copy = pltpu.make_async_remote_copy(
            src_ref=src,
            dst_ref=dst,
            send_sem=self.send.at[k],
            recv_sem=self.recv.at[k],
            device_id=where,
            device_id_type=MESH,
        )
        copy.start()
        self.open.append(copy)
        return copy

    def drain(self):
        for copy in self.open:
            copy.wait_send()


def owner_bounds(counts_ref):
    counts = jnp.broadcast_to(counts_ref[...].astype(F32), (128, 128))
    upto = jnp.where(iota((128, 128), 0) <= iota((128, 128), 1), 1.0, 0.0).astype(BF16)
    ends = mm(counts.astype(BF16), upto, 1, 0)
    return (ends - counts).T, ends.T


def slot_rows(lookups, starts, ends):
    q = lookups.astype(F32)
    outs = []
    for part in range(q.shape[1] // 128):
        row = q[:, part * 128 : part * 128 + 128]
        hit = (row >= starts) & (row < ends)
        owner = iota((128, 128), 0).astype(F32)
        shift = jnp.sum(jnp.where(hit, owner * 32.0 - starts, 0.0), axis=0, keepdims=True)
        outs.append(row + shift)
    return jnp.concatenate(outs, axis=1)


def as_column(row):
    parts = []
    for part in range(row.shape[1] // 128):
        piece = row[:, part * 128 : part * 128 + 128]
        parts.append(jnp.broadcast_to(piece, (128, 128)).T)
    return jnp.concatenate(parts, axis=0)


def tiles_over_rows(index, count):
    high = jnp.floor(index * (1.0 / 16.0))
    low = index - 16.0 * high
    n = index.shape[1]
    inner = jnp.where(iota((16, n), 0).astype(F32) == low, 1.0, 0.0).astype(BF16)
    high = jnp.broadcast_to(high, (16, n)).astype(BF16)
    zero = jnp.zeros((16, n), BF16)
    return jnp.concatenate(
        [jnp.where(high == jnp.asarray(t, BF16), inner, zero) for t in range(count)], axis=0
    )


def tiles_over_lanes(column, count):
    high = jnp.floor(column * (1.0 / 128.0))
    low = column - 128.0 * high
    inner = jnp.where(iota(column.shape, 1).astype(F32) == low, 1.0, 0.0).astype(BF16)
    high = high.astype(BF16)
    zero = jnp.zeros(column.shape, BF16)
    return jnp.concatenate(
        [jnp.where(high == jnp.asarray(t, BF16), inner, zero) for t in range(count)], axis=1
    )


class Spread:
    LO, HI = slice(0, 1024), slice(1024, 2048)
    T, B = slice(0, 16), slice(16, 32)

    def __init__(self, ref, go, where, out, sem):
        self.ref, self.go, self.out, self.sem, self.written = ref, go, out, sem, []
        self.x, self.y, self.c, _ = where
        self.xr, self.xl, self.xo = ((self.x + d) % 4 for d in (1, 3, 2))
        self.yr, self.yl, self.yo = ((self.y + d) % 4 for d in (1, 3, 2))
        self.partner = {"dp_2": 1 - self.c}
        self.d, self.pieces = [], []

    def across(self, *pieces):
        for piece in pieces:
            self.d.append(self.same(piece, self.partner))
            self.pieces.append(piece)
            self.write(piece)

    def from_partner(self, first, last):
        for k in range(first, last):
            self.d[k].wait_recv()
            a, b, _, rows, cols = self.pieces[k]
            self.write((a, b, 1 - self.c, rows, cols))

    def write(self, piece):
        k = len(self.written)
        copy = pltpu.make_async_copy(self.ref.at[piece], self.out.at[piece], self.sem.at[k])
        copy.start()
        self.written.append(copy)

    def same(self, piece, where):
        ref = self.ref.at[piece]
        return self.go(ref, ref, where)

    def first(self):
        x, y, c = self.x, self.y, self.c
        every = slice(None)
        self.p1 = self.same((x, y, c, every, self.LO), {"dp_0": self.xr})
        self.p2 = self.same((x, y, c, every, self.LO), {"dp_0": self.xl})
        self.q1 = self.same((x, y, c, every, self.HI), {"dp_1": self.yr})
        self.q2 = self.same((x, y, c, every, self.HI), {"dp_1": self.yl})

    def second(self):
        x, y, c = self.x, self.y, self.c
        self.p1.wait_recv()
        self.p3 = self.same((self.xl, y, c, self.T, self.LO), {"dp_0": self.xr})
        self.p2.wait_recv()
        self.p4 = self.same((self.xr, y, c, self.B, self.LO), {"dp_0": self.xl})
        self.q1.wait_recv()
        self.q3 = self.same((x, self.yl, c, self.T, self.HI), {"dp_1": self.yr})
        self.q2.wait_recv()
        self.q4 = self.same((x, self.yr, c, self.B, self.HI), {"dp_1": self.yl})

    def third(self):
        x, y, c = self.x, self.y, self.c
        every = slice(None)
        self.p3.wait_recv()
        self.p4.wait_recv()
        mine, other = (every, y, c, every, self.LO), (x, every, c, every, self.HI)
        self.p5 = self.same(mine, {"dp_1": self.yr})
        self.p6 = self.same(mine, {"dp_1": self.yl})
        self.q3.wait_recv()
        self.q4.wait_recv()
        self.q5 = self.same(other, {"dp_0": self.xr})
        self.q6 = self.same(other, {"dp_0": self.xl})
        self.across(mine, other)

    def fourth(self):
        c = self.c
        every = slice(None)
        self.p5.wait_recv()
        self.p7 = self.same((slice(0, 2), self.yl, c, every, self.LO), {"dp_1": self.yr})
        self.p6.wait_recv()
        self.p8 = self.same((slice(2, 4), self.yr, c, every, self.LO), {"dp_1": self.yl})
        self.q5.wait_recv()
        self.q7 = self.same((self.xl, slice(0, 2), c, every, self.HI), {"dp_0": self.xr})
        self.q6.wait_recv()
        self.q8 = self.same((self.xr, slice(2, 4), c, every, self.HI), {"dp_0": self.xl})
        self.across(*((every, n, c, every, self.LO) for n in (self.yl, self.yr)))
        self.across(*((n, every, c, every, self.HI) for n in (self.xl, self.xr)))
        self.from_partner(0, 2)

    def fifth(self):
        c = self.c
        every = slice(None)
        self.p7.wait_recv()
        self.p8.wait_recv()
        self.across((every, self.yo, c, every, self.LO))
        self.q7.wait_recv()
        self.q8.wait_recv()
        self.across((self.xo, every, c, every, self.HI))
        self.from_partner(2, 6)

    def last(self):
        self.from_partner(6, 8)

    def close(self):
        for copy in self.written:
            copy.wait()


N_COPIES = 140


def step_kernel(
    lookups_any, counts_any, slab_any, ids_any, label_any, sw_any, bias_any, wout_any,
    w_any, accum_any,
    ga_out, aa_out, sums_out, scale_out, grad_out,
    lookups_ref, counts_ref, slab_ref, ids_ref, label_ref, sw_ref, bias_ref, wout_ref,
    arrived_ref, rids_ref, scale_ref, grad_ref, lined,
    W, A, idsend, G, fac, hidden, dact, pacc, lg, LR, DL, gb, go, sv, rv,
    ZS, Df, ZRL, ZRR, ZL, ZR, DPL,
    R0, SB, RL, RV, Q, RL2, RV2,
    GA, AA, acc, slots, ns, NR, SC, slab, wout, strided,
    ssem, rsem, bulk, local, wsem,
):
    x, y, c, z = position()
    dp = (x * 4 + y) * 2 + c
    me = dp * 4 + z
    cp = Copies(ssem, rsem)
    go_to = cp.go
    zr, zl, zo = (z + 1) % 4, (z + 3) % 4, (z + 2) % 4
    xr, xl, xo = (x + 1) % 4, (x + 3) % 4, (x + 2) % 4
    yr, yl, yo = (y + 1) % 4, (y + 3) % 4, (y + 2) % 4
    LO, HI = slice(0, 1024), slice(1024, 2048)

    pairs_of = (
        (counts_any, counts_ref), (lookups_any, lookups_ref), (slab_any, slab_ref),
        (wout_any, wout_ref), (accum_any, A), (bias_any, bias_ref), (ids_any, ids_ref),
        (label_any, label_ref), (sw_any, sw_ref), (w_any, W),
    )
    loads = [pltpu.make_async_copy(a, b, local.at[k]) for k, (a, b) in enumerate(pairs_of)]
    for copy in loads:
        copy.start()
    barrier = pltpu.get_barrier_semaphore()

    def greet(p):
        pl.semaphore_signal(barrier, inc=1, device_id=p, device_id_type=LOGICAL)

    to_all(me, greet)
    for copy in loads[:5]:
        copy.wait()
    starts, ends = owner_bounds(counts_ref)
    own_rows = pl.ds(pl.multiple_of(z * 256, 256), 256)

    def gather_pair(k):
        lane = iota((256, 128), 1)
        got = []
        for side in range(2):
            slot = slot_rows(lookups_ref[2 * k + side : 2 * k + side + 1, :], starts, ends)
            column = as_column(slot)
            half = jnp.floor(column * 0.5)
            odd = column - 2.0 * half
            both = mm(tiles_over_lanes(half, 16), slab[...], 1, 0)
            one = jnp.where((lane >= 64) == (odd > 0.5), both, 0.0)
            got.append(one + pltpu.roll(one, 64, 1))
        G[own_rows, k * 128 : k * 128 + 128] = jnp.where(lane < 64, got[0], got[1]).astype(BF16)

    def block(src, k):
        return G.at[pl.ds(pl.multiple_of(src * 256, 256), 256), k * 256 : k * 256 + 256]

    def send_ids(p):
        pltpu.make_async_remote_copy(
            src_ref=idsend.at[p], dst_ref=rids_ref.at[me], send_sem=bulk.at[0],
            recv_sem=bulk.at[1], device_id=p, device_id_type=LOGICAL,
        ).start()

    right, left = {}, {}

    def send_block(k):
        right[k] = go_to(block(z, k), block(z, k), {"mp": zr})
        left[k] = go_to(block(z, k), block(z, k), {"mp": zl})

    for k in range(16):
        strided[pl.ds(k, 128, stride=16), :] = slab_ref[:, k * 128 : k * 128 + 128].astype(F32)
    slab[...] = strided[...].astype(BF16)
    for k in range(16):
        wout[:, k * 128 : k * 128 + 128] = wout_ref[k : k + 1, :].astype(F32)
    gather_pair(0)
    gather_pair(1)
    AA[x, y, c] = A[...].astype(BF16)
    pl.semaphore_wait(barrier, 127)
    send_block(0)
    aa = Spread(AA, go_to, (x, y, c, z), aa_out, wsem.at[0])
    aa.first()
    gather_pair(4)
    gather_pair(5)
    send_block(2)
    gather_pair(2)
    gather_pair(3)
    send_block(1)
    gather_pair(6)
    gather_pair(7)
    send_block(3)
    for copy in loads[5:9]:
        copy.wait()
    turned = jnp.concatenate([ids_ref[...].astype(F32), jnp.zeros((96, 128), F32)], axis=0)
    idsend[...] = turned.T.astype(I32).reshape(128, 1, 128)
    to_all(me, send_ids)
    rids_ref[me] = idsend[me]
    loads[9].wait()

    def forward(src):
        rows = pl.ds(pl.multiple_of(src * 256, 256), 256)
        pacc[...] = jnp.zeros_like(pacc)

        def tile(t, carry):
            cols = pl.ds(pl.multiple_of(t * 512, 512), 512)
            a = mm(G[rows, :], W[:, cols], 1, 0) + bias_ref[:, cols]
            wo = wout[:, cols]
            sg = lax.logistic(a)
            h = (a * sg).astype(BF16)
            hidden[rows, cols] = h
            fac[src, :, :, :, cols] = (wo * sg * (1.0 + a * (1.0 - sg))).reshape(4, 2, 32, 512)
            m = h.astype(F32) * wo
            pacc[...] += (m[:, 0:128] + m[:, 128:256]) + (m[:, 256:384] + m[:, 384:512])
            return carry

        lax.fori_loop(0, 4, tile, 0, unroll=2)
        for s in range(2):
            line = jnp.sum(pacc[128 * s : 128 * s + 128, :].T, axis=0, keepdims=True)
            lg[pl.ds(src * 2 + s, 1), :] = line

    right[0].wait_recv()
    f0 = go_to(block(zl, 0), block(zl, 0), {"mp": zr})
    left[2].wait_recv()
    f2 = go_to(block(zr, 2), block(zr, 2), {"mp": zl})
    forward(z)
    right[1].wait_recv()
    f1 = go_to(block(zl, 1), block(zl, 1), {"mp": zr})
    left[3].wait_recv()
    f3 = go_to(block(zr, 3), block(zr, 3), {"mp": zl})
    aa.second()
    right[2].wait_recv()
    right[3].wait_recv()
    forward(zl)
    left[0].wait_recv()
    left[1].wait_recv()
    forward(zr)
    aa.third()
    for copy in (f0, f1, f2, f3):
        copy.wait_recv()
    forward(zo)

    sent = [go_to(lg, LR.at[z], {"mp": (z + d) % 4}) for d in (1, 2, 3)]
    LR[z] = lg[...]
    for copy in sent:
        copy.wait_recv()
    logit = (LR[0] + LR[1]) + (LR[2] + LR[3])
    DL[...] = sw_ref[...] * (lax.logistic(logit) - label_ref[...].astype(F32))

    def column(g):
        return jnp.broadcast_to(DL[pl.ds(g, 1), :], (128, 128)).T

    def dact_part(g, carry):
        rows = pl.ds(pl.multiple_of(g * 128, 128), 128)
        col = column(g)
        for t in range(16):
            cols = slice(128 * t, 128 * t + 128)
            f = fac[g // 2, pl.ds((g % 2) * 2, 2), :, :, cols].reshape(128, 128)
            dact[rows, cols] = (f * col).astype(BF16)
        return carry

    lax.fori_loop(0, 8, dact_part, 0)

    def sums_part(g, carry):
        rows = pl.ds(pl.multiple_of(g * 128, 128), 128)
        col = column(g)
        for t in range(16):
            cols = slice(128 * t, 128 * t + 128)
            d = dact[rows, cols].astype(F32)
            gb[:, cols] += jnp.sum(d.reshape(16, 8, 128), axis=0)
            m = hidden[rows, cols].astype(F32) * col
            go[:, cols] += jnp.sum(m.reshape(16, 8, 128), axis=0)
        return carry

    def dpool(dest, put):
        rows = pl.ds(pl.multiple_of(dest * 256, 256), 256)

        def tile(t, carry):
            at = pl.multiple_of(t * 512, 512)
            put(mm(dact[rows, :], W[pl.ds(at, 512), :], 1, 1), pl.ds(at, 512))
            return carry

        lax.fori_loop(0, 2, tile, 0)

    def put_far(d, cols):
        ZS[0, :, cols] = d.astype(BF16)

    dpool(zo, put_far)
    z1 = go_to(ZS.at[0, 0:128], ZRL, {"mp": zr})
    z2 = go_to(ZS.at[0, 128:256], ZRR, {"mp": zl})

    partner = {"dp_2": 1 - c}
    to_core = {}

    def weight_grad(xi, tag):
        at = pl.multiple_of(xi * 256, 256)

        def tile(t, carry):
            cols = pl.ds(pl.multiple_of(t * 1024, 1024), 1024)
            g = mm(G[:, pl.ds(at, 256)], dact[:, cols], 0, 0)
            fac[xi, :, :, :, cols] = g.reshape(4, 2, 32, 1024)
            SC[xi, :, :, cols] = fac[xi, :, 1 - c, :, cols].astype(BF16)
            return carry

        lax.fori_loop(0, 2, tile, 0)
        to_core[tag] = go_to(SC.at[xi], R0.at[xi], partner)

    def chip_sum(xi, tag):
        to_core[tag].wait_recv()
        for yi in range(4):
            s = R0[xi, yi].astype(F32) + fac[xi, yi, c]
            fac[xi, yi, c] = s
            SB[xi, yi] = s.astype(BF16)

    def put_right(d, cols):
        Df[0, :, cols] = d[0:128]
        ZS[1, 128:256, cols] = d[128:256].astype(BF16)

    def put_left(d, cols):
        ZS[2, 0:128, cols] = d[0:128].astype(BF16)
        Df[1, :, cols] = d[128:256]

    weight_grad(xo, "o")
    dpool(zr, put_right)
    z3 = go_to(ZS.at[1, 128:256], ZL.at[128:256], {"mp": zr})
    dpool(zl, put_left)
    z4 = go_to(ZS.at[2, 0:128], ZR.at[0:128], {"mp": zl})
    chip_sum(xo, "o")
    h0a = go_to(SB.at[xo, 0:2, :, LO], RL.at[0, 0], {"dp_0": xr})
    h0b = go_to(SB.at[xo, 2:4, :, LO], RL.at[0, 1], {"dp_0": xl})
    weight_grad(xr, "r")
    weight_grad(xl, "l")
    chip_sum(xr, "r")
    h0c = go_to(SB.at[xr, 2:4, :, LO], RV.at[0, 0, 2:4], {"dp_0": xr})
    weight_grad(x, "m")
    chip_sum(xl, "l")
    h0d = go_to(SB.at[xl, 0:2, :, LO], RV.at[0, 1, 0:2], {"dp_0": xl})
    z1.wait_recv()
    ZS[1, 0:128, :] = (Df[0] + ZRL[...].astype(F32)).astype(BF16)
    z5 = go_to(ZS.at[1, 0:128], ZL.at[0:128], {"mp": zr})
    z2.wait_recv()
    ZS[2, 128:256, :] = (Df[1] + ZRR[...].astype(F32)).astype(BF16)
    z6 = go_to(ZS.at[2, 128:256], ZR.at[128:256], {"mp": zl})
    aa.fourth()

    def put_own(d, cols):
        DPL[:, cols] = d

    dpool(z, put_own)
    chip_sum(x, "m")
    h1a = go_to(SB.at[0:2, yo, :, HI], RL.at[1, 0], {"dp_1": yr})
    h1b = go_to(SB.at[2:4, yo, :, HI], RL.at[1, 1], {"dp_1": yl})
    h1c = go_to(SB.at[2:4, yr, :, HI], RV.at[1, 0, 2:4], {"dp_1": yr})
    h1d = go_to(SB.at[0:2, yl, :, HI], RV.at[1, 1, 0:2], {"dp_1": yl})

    h0a.wait_recv()
    for k in range(2):
        SB[xr, k, :, LO] = (fac[xr, k, c, :, LO] + RL[0, 0, k].astype(F32)).astype(BF16)
    h0e = go_to(SB.at[xr, 0:2, :, LO], RV.at[0, 0, 0:2], {"dp_0": xr})
    h0b.wait_recv()
    for k in range(2):
        SB[xl, 2 + k, :, LO] = (fac[xl, 2 + k, c, :, LO] + RL[0, 1, k].astype(F32)).astype(BF16)
    h0f = go_to(SB.at[xl, 2:4, :, LO], RV.at[0, 1, 2:4], {"dp_0": xl})

    gb[...] = jnp.zeros_like(gb)
    go[...] = jnp.zeros_like(go)
    lax.fori_loop(0, 8, sums_part, 0)
    for t in range(16):
        cols = slice(128 * t, 128 * t + 128)
        sv[t] = jnp.sum(gb[:, cols], axis=0, keepdims=True)
        sv[16 + t] = jnp.sum(go[:, cols], axis=0, keepdims=True)

    def send_small(i, carry):
        p = (dp + i) % 32
        where = {"dp_0": p // 8, "dp_1": (p // 2) % 4, "dp_2": p % 2, "mp": z}
        pltpu.make_async_remote_copy(
            src_ref=sv.at[p], dst_ref=rv.at[dp], send_sem=bulk.at[2],
            recv_sem=bulk.at[3], device_id=where, device_id_type=MESH,
        ).start()
        return carry

    lax.fori_loop(1, 32, send_small, 0)
    rv[dp] = sv[dp]

    h1a.wait_recv()
    for k in range(2):
        SB[k, yr, :, HI] = (fac[k, yr, c, :, HI] + RL[1, 0, k].astype(F32)).astype(BF16)
    h1e = go_to(SB.at[0:2, yr, :, HI], RV.at[1, 0, 0:2], {"dp_1": yr})
    h1b.wait_recv()
    for k in range(2):
        SB[2 + k, yl, :, HI] = (fac[2 + k, yl, c, :, HI] + RL[1, 1, k].astype(F32)).astype(BF16)
    h1f = go_to(SB.at[2:4, yl, :, HI], RV.at[1, 1, 2:4], {"dp_1": yl})
    aa.fifth()

    def ring(h, axis, n):
        nr, nl, no = (n + 1) % 4, (n + 3) % 4, (n + 2) % 4
        s1 = go_to(Q.at[h, no, 0:16], RL2.at[h, 0], {axis: nr})
        s2 = go_to(Q.at[h, no, 16:32], RL2.at[h, 1], {axis: nl})
        s3 = go_to(Q.at[h, nr, 16:32], RV2.at[h, 0, 16:32], {axis: nr})
        s4 = go_to(Q.at[h, nl, 0:16], RV2.at[h, 1, 0:16], {axis: nl})
        return nr, nl, (s1, s2, s3, s4)

    def ring_relay(h, axis, state):
        nr, nl, (s1, s2, s3, s4) = state
        s1.wait_recv()
        Q[h, nr, 0:16] = Q[h, nr, 0:16] + RL2[h, 0]
        s5 = go_to(Q.at[h, nr, 0:16], RV2.at[h, 0, 0:16], {axis: nr})
        s2.wait_recv()
        Q[h, nl, 16:32] = Q[h, nl, 16:32] + RL2[h, 1]
        s6 = go_to(Q.at[h, nl, 16:32], RV2.at[h, 1, 16:32], {axis: nl})
        return s3, s4, s5, s6

    def segment(first, last):
        def pair(k, carry):
            lane = iota((256, 128), 1)
            block = DPL[:, pl.ds(pl.multiple_of(k * 128, 128), 128)]
            turned = pltpu.roll(block, 64, 1)
            hots, rows = [], []
            for side in range(2):
                slot = slot_rows(lookups_ref[pl.ds(2 * k + side, 1), :], starts, ends)
                slot = as_column(slot)
                sixteen = jnp.floor(slot * (1.0 / 16.0))
                both = jnp.floor(slot * (1.0 / 32.0))
                upper = sixteen - 2.0 * both
                hots.append(tiles_over_lanes(slot - 16.0 * (sixteen - both), 16))
                same = jnp.where((lane < 64) == (side == 0), block, turned)
                kept = jnp.where((lane >= 64) == (upper > 0.5), same, 0.0)
                rows.append(kept.astype(BF16))
            acc[...] += mm(jnp.concatenate(rows, axis=0), jnp.concatenate(hots, axis=0), 0, 0)
            return carry

        lax.fori_loop(first, last, pair, 0)

    def rows_of_table(first, last):
        def part(t, carry):
            lane = iota((256, 128), 1)
            block = arrived_ref[pl.ds(16 * t, 16)].reshape(256, 128).astype(F32)
            turned = pltpu.roll(block, 64, 1)
            hots, values = [], []
            for side in range(2):
                row = jnp.concatenate(
                    [lined[side, pl.ds(2 * t, 1), :], lined[side, pl.ds(2 * t + 1, 1), :]], axis=1
                )
                row = as_column(row)
                above = row >= 2048.0
                hots.append(tiles_over_lanes(jnp.where(above, row - 2048.0, row), 16))
                same = jnp.where((lane < 64) == (side == 0), block, turned)
                values.append(jnp.where((lane >= 64) == above, same, 0.0).astype(BF16))
            acc[...] += mm(
                jnp.concatenate(values, axis=0), jnp.concatenate(hots, axis=0), 0, 0
            )
            return carry

        lax.fori_loop(first, last, part, 0)

    for copy in (z3, z4, z5, z6):
        copy.wait_recv()
    DPL[...] = DPL[...] + (ZL[...].astype(F32) + ZR[...].astype(F32))
    acc[...] = jnp.zeros_like(acc)
    segment(0, 2)
    for copy in (h0c, h0d, h0e, h0f):
        copy.wait_recv()
    for k in range(4):
        Q[0, k] = fac[x, k, c, :, LO] + (RV[0, 0, k].astype(F32) + RV[0, 1, k].astype(F32))
    t0 = ring(0, "dp_1", y)
    segment(2, 4)
    for copy in (h1c, h1d, h1e, h1f):
        copy.wait_recv()
    for k in range(4):
        Q[1, k] = fac[k, y, c, :, HI] + (RV[1, 0, k].astype(F32) + RV[1, 1, k].astype(F32))
    t1 = ring(1, "dp_0", x)
    u0 = ring_relay(0, "dp_1", t0)
    segment(4, 6)
    u1 = ring_relay(1, "dp_0", t1)
    segment(6, 8)
    few = jnp.zeros((8, 128), F32)
    for t in range(16):
        piece = acc[:, 128 * t : 128 * t + 128]
        few = few + jnp.sum((piece * piece).reshape(16, 8, 128), axis=0)
        slots[8 * t : 8 * t + 8] = piece.T.astype(BF16).reshape(8, 16, 128)

    def send_slots(p):
        pltpu.make_async_remote_copy(
            src_ref=slots.at[p], dst_ref=arrived_ref.at[me], send_sem=bulk.at[4],
            recv_sem=bulk.at[5], device_id=p, device_id_type=LOGICAL,
        ).start()

    to_all(me, send_slots)
    arrived_ref[me] = slots[me]

    for copy in u0 + u1:
        copy.wait_recv()
    lower = Q[0, y] + (RV2[0, 0] + RV2[0, 1])
    upper = Q[1, x] + (RV2[1, 0] + RV2[1, 1])
    grad_ref[:, LO] = lower
    grad_ref[:, HI] = upper
    GA[x, y, c, :, LO] = lower.astype(BF16)
    GA[x, y, c, :, HI] = upper.astype(BF16)
    ga = Spread(GA, go_to, (x, y, c, z), ga_out, wsem.at[1])
    ga.first()
    both = lower * lower + upper * upper
    both = jnp.sum(both.reshape(4, 8, 1024), axis=0)
    for t in range(8):
        few = few + both[:, 128 * t : 128 * t + 128]
    small = sv.at[pl.ds(0, 31)]
    pltpu.make_async_copy(small, small, bulk.at[2]).wait()
    pltpu.make_async_copy(small, small, bulk.at[3]).wait()
    bias_sum = jnp.sum(rv[...], axis=0)
    ns[...] = jnp.sum(few, axis=0, keepdims=True) + bias_sum * bias_sum

    def send_norm(p):
        pltpu.make_async_remote_copy(
            src_ref=ns, dst_ref=NR.at[me], send_sem=bulk.at[6],
            recv_sem=bulk.at[7], device_id=p, device_id_type=LOGICAL,
        ).start()

    to_all(me, send_norm)
    put_grad = pltpu.make_async_copy(grad_ref, grad_out, local.at[10])
    put_grad.start()
    NR[me] = ns[...]
    ga.second()

    heard = idsend.at[pl.ds(0, 127)]
    pltpu.make_async_copy(heard, heard, bulk.at[1]).wait()
    lane16 = iota((16, 128), 1) // 16
    numbers = rids_ref[...].astype(F32).reshape(16, 8, 128)
    for side in range(2):
        line = jnp.zeros((16, 128), F32)
        for d in range(8):
            shift = (16 * d - 16 * side) % 128
            line = jnp.where(lane16 == d, pltpu.roll(numbers[:, d, :], shift, 1), line)
        lined[side] = line
    acc[...] = jnp.zeros_like(acc)
    aa.last()
    ga.third()
    many = arrived_ref.at[pl.ds(0, 127)]
    pltpu.make_async_copy(many, many, bulk.at[5]).wait()
    rows_of_table(0, 5)
    ga.fourth()
    rows_of_table(5, 8)
    put_sums = pltpu.make_async_copy(acc, sums_out, local.at[11])
    put_sums.start()
    lot = NR.at[pl.ds(0, 127)]
    pltpu.make_async_copy(lot, lot, bulk.at[7]).wait()
    lanes = jnp.sum(NR[...], axis=0)
    norm = jnp.sum(lanes, axis=1, keepdims=True)
    scale = clip_norm / jnp.maximum(jnp.sqrt(norm), clip_norm)
    scale_ref[...] = jnp.broadcast_to(scale, (8, 128))
    put_scale = pltpu.make_async_copy(scale_ref, scale_out, local.at[12])
    put_scale.start()
    ga.fifth()
    ga.last()
    pltpu.make_async_copy(lot, lot, bulk.at[6]).wait()
    pltpu.make_async_copy(many, many, bulk.at[4]).wait()
    pltpu.make_async_copy(heard, heard, bulk.at[0]).wait()
    put_grad.wait()
    put_sums.wait()
    put_scale.wait()
    cp.drain()
    aa.close()
    ga.close()


def finish_kernel(
    sums_any, scale_ref, table_any, accum_any, grad_any, dense_any,
    ga_any, aa_any, w_any,
    new_any, accum_new_any, dense_new_any, wn_any,
    GA, AA, W, WN, sums, table, accum, grad, dense, new, accum_new, dense_new, sem, isem, osem,
):
    chunk = 128
    count = 1024 // chunk

    def load(i):
        rows = pl.ds(i * chunk, chunk)
        for j, (src, dst) in enumerate(((ga_any, GA), (aa_any, AA), (w_any, W))):
            pltpu.make_async_copy(src.at[rows], dst.at[rows], sem.at[i, j]).start()

    small = [
        pltpu.make_async_copy(src, dst, isem.at[k])
        for k, (src, dst) in enumerate(
            (
                (grad_any, grad), (dense_any, dense), (accum_any, accum),
                (sums_any, sums), (table_any, table),
            )
        )
    ]
    load(0)
    load(1)
    for copy in small:
        copy.start()
    for i in range(2, count):
        load(i)
    scale = scale_ref[0:1, 0:1]

    def part(t, carry):
        rows = pl.ds(pl.multiple_of(t * chunk, chunk), chunk)
        for j, (src, dst) in enumerate(((ga_any, GA), (aa_any, AA), (w_any, W))):
            pltpu.make_async_copy(src.at[rows], dst.at[rows], sem.at[t, j]).wait()
        for q in range(16):
            cols = slice(128 * q, 128 * q + 128)
            g = scale * GA[rows, cols].astype(F32)
            r = lax.rsqrt(AA[rows, cols].astype(F32) + g * g)
            r = r - (adagrad_eps * r) * r
            WN[rows, cols] = (W[rows, cols].astype(F32) - (dense_rate * g) * r).astype(BF16)
        pltpu.make_async_copy(WN.at[rows], wn_any.at[rows], osem.at[0]).start()
        return carry

    lax.fori_loop(0, count, part, 0)
    for copy in small:
        copy.wait()
    clipped = scale * grad[...]
    dense_new[...] = dense[...] + clipped * clipped
    puts = [pltpu.make_async_copy(dense_new, dense_new_any, osem.at[1])]
    puts[0].start()
    for upper in range(2):
        for p in range(16):
            r = sums[64 * upper : 64 * upper + 64, 128 * p : 128 * p + 128] * scale
            line = p + upper * 16
            fresh = accum[line : line + 1, :] + jnp.sum(r * r, axis=0, keepdims=True) / 64.0
            accum_new[line : line + 1, :] = fresh
            at = line * 128
            rate = table_rate / (jnp.sqrt(fresh) + adagrad_eps)
            new[:, at : at + 128] = table[:, at : at + 128] - r * rate
        cols = pl.ds(2048 * upper, 2048)
        puts.append(
            pltpu.make_async_copy(new.at[:, cols], new_any.at[:, cols], osem.at[2 + upper])
        )
        puts[-1].start()
    puts.append(pltpu.make_async_copy(accum_new, accum_new_any, osem.at[4]))
    puts[-1].start()
    pltpu.make_async_copy(WN, wn_any, osem.at[0]).wait()
    for copy in puts:
        copy.wait()


def shape(dims, kind):
    return jax.ShapeDtypeStruct(dims, kind)


def body(
    slab_values,
    row_ids,
    peer_counts,
    lookup_slots,
    labels,
    sample_weight,
    weight_in,
    bias_in,
    weight_out,
    dense_accum,
    table_rows,
    table_accum,
):
    V = pltpu.VMEM
    DMA = pltpu.SemaphoreType.DMA
    whole = (4, 4, 2, 32, 2048)
    ga, aa, sums, scale, grad = pl.pallas_call(
        step_kernel,
        out_shape=(
            shape(whole, BF16), shape(whole, BF16), shape((128, 2048), F32),
            shape((8, 128), F32), shape((32, 2048), F32),
        ),
        in_specs=[ANY] * 10,
        out_specs=(ANY,) * 5,
        scratch_shapes=[
            V((16, 256), I32), V((1, 128), I32), V((128, 2048), BF16), V((32, 128), I32),
            V((8, 128), I32), V((8, 128), F32), V((1, 2048), F32), V((16, 128), BF16),
            V((128, 16, 128), BF16), V((128, 1, 128), I32), V((8, 128), F32), V((32, 2048), F32),
            V((2, 16, 128), F32),
            V((1024, 2048), BF16), V((32, 2048), F32), V((128, 1, 128), I32),
            V((1024, 1024), BF16), V(whole, F32), V((1024, 2048), BF16),
            V((1024, 2048), BF16), V((256, 128), F32), V((8, 128), F32), V((4, 8, 128), F32),
            V((8, 128), F32), V((8, 2048), F32), V((8, 2048), F32),
            V((32, 1, 128), F32), V((32, 1, 128), F32),
            V((3, 256, 1024), BF16), V((2, 128, 1024), F32),
            V((128, 1024), BF16), V((128, 1024), BF16),
            V((256, 1024), BF16), V((256, 1024), BF16), V((256, 1024), F32),
            V((4, 4, 32, 2048), BF16), V((4, 4, 32, 2048), BF16),
            V((2, 2, 2, 32, 1024), BF16), V((2, 2, 4, 32, 1024), BF16),
            V((2, 4, 32, 1024), F32), V((2, 2, 16, 1024), F32), V((2, 2, 32, 1024), F32),
            V(whole, BF16), V(whole, BF16), V((128, 2048), F32), V((128, 16, 128), BF16),
            V((1, 128), F32), V((128, 1, 128), F32), V((4, 4, 32, 2048), BF16),
            V((2048, 128), BF16), V((1, 2048), F32), V((2048, 128), F32),
            DMA((N_COPIES,)), DMA((N_COPIES,)), DMA((8,)), DMA((13,)), DMA((2, 16)),
        ],
        compiler_params=pltpu.CompilerParams(
            has_side_effects=True, vmem_limit_bytes=63 * 1024 * 1024, collective_id=0
        ),
        name="step",
    )(
        lookup_slots.T,
        peer_counts,
        slab_values[0],
        row_ids[0].T,
        labels.reshape(8, 128),
        sample_weight.reshape(8, 128),
        bias_in.reshape(1, 2048),
        weight_out.reshape(16, 128),
        weight_in,
        dense_accum,
    )
    table_new, table_accum_new, accum_new, weight_new = pl.pallas_call(
        finish_kernel,
        out_shape=(
            shape((64, 4096), F32), shape((32, 128), F32), shape((32, 2048), F32),
            shape((1024, 2048), BF16),
        ),
        in_specs=[ANY, VM] + [ANY] * 7,
        out_specs=(ANY,) * 4,
        scratch_shapes=[
            V((1024, 2048), BF16), V((1024, 2048), BF16), V((1024, 2048), BF16),
            V((1024, 2048), BF16), V((128, 2048), F32), V((64, 4096), F32), V((32, 128), F32),
            V((32, 2048), F32), V((32, 2048), F32), V((64, 4096), F32), V((32, 128), F32),
            V((32, 2048), F32), DMA((8, 3)), DMA((5,)), DMA((5,)),
        ],
        name="finish",
    )(
        sums,
        scale,
        table_rows.T,
        table_accum.reshape(32, 128),
        grad,
        dense_accum,
        ga.reshape(1024, 2048),
        aa.reshape(1024, 2048),
        weight_in,
    )
    return (weight_new, accum_new, table_new.T, table_accum_new.reshape(4096))


def solution(mesh):
    torus = Mesh(mesh.devices.reshape(4, 4, 2, mesh.shape["mp"]), ("dp_0", "dp_1", "dp_2", "mp"))
    placed = (
        P(DP_MP, None, None),
        P(DP_MP, None, None),
        P(DP_MP, None),
        P(DP_MP, None),
        P(DP),
        P(DP),
        P(None, "mp"),
        P("mp"),
        P("mp"),
        P(DP, "mp"),
        P(DP_MP, None),
        P(DP_MP),
    )
    return jax.shard_map(
        body,
        mesh=torus,
        in_specs=placed,
        out_specs=(P(None, "mp"), P(DP, "mp"), P(DP_MP, None), P(DP_MP)),
        check_vma=False,
    )
```

```python
import functools

import jax
import jax.numpy as jnp
from jax import lax
from jax.experimental import pallas as pl
from jax.experimental.pallas import tpu as pltpu
from jax.sharding import Mesh
from jax.sharding import PartitionSpec as P

DP = ("dp_0", "dp_1", "dp_2")
DP_MP = ("dp_0", "dp_1", "dp_2", "mp")

clip_norm = 1.0
dense_rate = 0.02
table_rate = 0.5
adagrad_eps = 1e-10

F32 = jnp.float32
BF16 = jnp.bfloat16
I32 = jnp.int32
MESH = pl.DeviceIdType.MESH
LOGICAL = pl.DeviceIdType.LOGICAL
VM = pl.BlockSpec(memory_space=pltpu.VMEM)
ANY = pl.BlockSpec(memory_space=pl.ANY)


def mm(a, b, ca, cb):
    return lax.dot_general(a, b, (((ca,), (cb,)), ((), ())), preferred_element_type=F32)


def iota(shape, dim):
    return lax.broadcasted_iota(I32, shape, dim)


def position():
    return tuple(lax.axis_index(a) for a in DP_MP)


def to_all(me, emit):
    for u in range(1, 8):
        emit(lax.rem(me + u, 128))

    def more(j, carry):
        base = me + 8 * j
        for u in range(8):
            emit(lax.rem(base + u, 128))
        return carry

    lax.fori_loop(1, 16, more, 0)


class Copies:
    def __init__(self, send, recv):
        self.send, self.recv, self.used, self.sent = send, recv, 0, [0]

    def go(self, src, dst, where, send=None):
        if send is None:
            rows = src.size * (4 if src.dtype == F32 else 2) // 4096
            if self.sent[-1] + rows > 1024:
                self.sent.append(0)
            self.sent[-1] += rows
            send = self.send.at[len(self.sent) - 1]
        copy = pltpu.make_async_remote_copy(
            src_ref=src,
            dst_ref=dst,
            send_sem=send,
            recv_sem=self.recv.at[self.used],
            device_id=where,
            device_id_type=MESH,
        )
        self.used += 1
        copy.start()
        return copy

    def drain(self, rows_of_4k):
        for k, count in enumerate(self.sent):
            some = rows_of_4k.at[pl.ds(0, count)]
            pltpu.make_async_copy(some, some, self.send.at[k]).wait()


def owner_bounds(counts_ref):
    counts = jnp.broadcast_to(counts_ref[...].astype(F32), (128, 128))
    upto = jnp.where(iota((128, 128), 0) <= iota((128, 128), 1), 1.0, 0.0).astype(BF16)
    ends = mm(counts.astype(BF16), upto, 1, 0)
    return (ends - counts).T, ends.T


def slot_rows(lookups, starts, ends):
    q = lookups.astype(F32)
    outs = []
    for part in range(q.shape[1] // 128):
        row = q[:, part * 128 : part * 128 + 128]
        hit = (row >= starts) & (row < ends)
        owner = iota((128, 128), 0).astype(F32)
        shift = jnp.sum(jnp.where(hit, owner * 32.0 - starts, 0.0), axis=0, keepdims=True)
        outs.append(row + shift)
    return jnp.concatenate(outs, axis=1)


def as_column(row):
    parts = []
    for part in range(row.shape[1] // 128):
        piece = row[:, part * 128 : part * 128 + 128]
        parts.append(jnp.broadcast_to(piece, (128, 128)).T)
    return jnp.concatenate(parts, axis=0)


def tiles_over_rows(index, count):
    high = jnp.floor(index * (1.0 / 16.0))
    low = index - 16.0 * high
    n = index.shape[1]
    inner = jnp.where(iota((16, n), 0).astype(F32) == low, 1.0, 0.0).astype(BF16)
    high = jnp.broadcast_to(high, (16, n)).astype(BF16)
    zero = jnp.zeros((16, n), BF16)
    return jnp.concatenate(
        [jnp.where(high == jnp.asarray(t, BF16), inner, zero) for t in range(count)], axis=0
    )


def tiles_over_lanes(column, count):
    high = jnp.floor(column * (1.0 / 128.0))
    low = column - 128.0 * high
    inner = jnp.where(iota(column.shape, 1).astype(F32) == low, 1.0, 0.0).astype(BF16)
    high = high.astype(BF16)
    zero = jnp.zeros(column.shape, BF16)
    return jnp.concatenate(
        [jnp.where(high == jnp.asarray(t, BF16), inner, zero) for t in range(count)], axis=1
    )


class Spread:
    LO, HI = slice(0, 1024), slice(1024, 2048)
    T, B = slice(0, 16), slice(16, 32)

    def __init__(self, ref, go, where, out, sem):
        self.ref, self.go, self.out, self.sem = ref, go, out, sem
        self.x, self.y, self.c, _ = where
        self.xr, self.xl, self.xo = ((self.x + d) % 4 for d in (1, 3, 2))
        self.yr, self.yl, self.yo = ((self.y + d) % 4 for d in (1, 3, 2))
        self.partner = {"dp_2": 1 - self.c}
        self.d, self.pieces = [], []

    def across(self, *pieces):
        for piece in pieces:
            self.d.append(self.same(piece, self.partner))
            self.pieces.append(piece)
            self.write(piece)

    def from_partner(self, first, last):
        for k in range(first, last):
            self.d[k].wait_recv()
            a, b, _, rows, cols = self.pieces[k]
            self.write((a, b, 1 - self.c, rows, cols))

    def write(self, piece):
        pltpu.make_async_copy(self.ref.at[piece], self.out.at[piece], self.sem).start()

    def same(self, piece, where):
        ref = self.ref.at[piece]
        return self.go(ref, ref, where)

    def first(self):
        x, y, c = self.x, self.y, self.c
        every = slice(None)
        self.p1 = self.same((x, y, c, every, self.LO), {"dp_0": self.xr})
        self.p2 = self.same((x, y, c, every, self.LO), {"dp_0": self.xl})
        self.q1 = self.same((x, y, c, every, self.HI), {"dp_1": self.yr})
        self.q2 = self.same((x, y, c, every, self.HI), {"dp_1": self.yl})

    def second(self):
        x, y, c = self.x, self.y, self.c
        self.p1.wait_recv()
        self.p3 = self.same((self.xl, y, c, self.T, self.LO), {"dp_0": self.xr})
        self.p2.wait_recv()
        self.p4 = self.same((self.xr, y, c, self.B, self.LO), {"dp_0": self.xl})
        self.q1.wait_recv()
        self.q3 = self.same((x, self.yl, c, self.T, self.HI), {"dp_1": self.yr})
        self.q2.wait_recv()
        self.q4 = self.same((x, self.yr, c, self.B, self.HI), {"dp_1": self.yl})

    def third(self):
        x, y, c = self.x, self.y, self.c
        every = slice(None)
        self.p3.wait_recv()
        self.p4.wait_recv()
        mine, other = (every, y, c, every, self.LO), (x, every, c, every, self.HI)
        self.p5 = self.same(mine, {"dp_1": self.yr})
        self.p6 = self.same(mine, {"dp_1": self.yl})
        self.q3.wait_recv()
        self.q4.wait_recv()
        self.q5 = self.same(other, {"dp_0": self.xr})
        self.q6 = self.same(other, {"dp_0": self.xl})
        self.across(mine, other)

    def fourth(self):
        c = self.c
        every = slice(None)
        self.p5.wait_recv()
        self.p7 = self.same((slice(0, 2), self.yl, c, every, self.LO), {"dp_1": self.yr})
        self.p6.wait_recv()
        self.p8 = self.same((slice(2, 4), self.yr, c, every, self.LO), {"dp_1": self.yl})
        self.q5.wait_recv()
        self.q7 = self.same((self.xl, slice(0, 2), c, every, self.HI), {"dp_0": self.xr})
        self.q6.wait_recv()
        self.q8 = self.same((self.xr, slice(2, 4), c, every, self.HI), {"dp_0": self.xl})
        self.across(*((every, n, c, every, self.LO) for n in (self.yl, self.yr)))
        self.across(*((n, every, c, every, self.HI) for n in (self.xl, self.xr)))
        self.from_partner(0, 2)

    def fifth(self):
        c = self.c
        every = slice(None)
        self.p7.wait_recv()
        self.p8.wait_recv()
        self.across((every, self.yo, c, every, self.LO))
        self.q7.wait_recv()
        self.q8.wait_recv()
        self.across((self.xo, every, c, every, self.HI))
        self.from_partner(2, 6)

    def last(self):
        self.from_partner(6, 8)

    def close(self):
        pltpu.make_async_copy(self.ref, self.out, self.sem).wait()


class Flow(Spread):
    def part(self, h, i, j, rows):
        if h == 0:
            return (i, j, self.c, rows, self.LO)
        return (j, i, self.c, rows, self.HI)

    def send(self, h, axis, step, i, j, rows):
        along_x = (h == 0) == (axis == 0)
        n = self.x if along_x else self.y
        return self.same(
            self.part(h, i, j, rows), {"dp_0" if along_x else "dp_1": (n + step) % 4}
        )

    def start(self):
        every = slice(None)
        self.n = ((self.x, self.y), (self.y, self.x))
        self.hop1, self.own, self.side, self.opp = {}, {}, {}, {}
        for h in range(2):
            i, j = self.n[h]
            for step in (1, 3):
                self.hop1[h, step] = self.send(h, 0, step, i, j, every)
        for h in range(2):
            i, j = self.n[h]
            for step in (1, 3):
                self.own[h, step] = self.send(h, 1, step, i, j, every)

    def sides(self):
        every = slice(None)
        self.hop2 = {}
        for h in range(2):
            i, j = self.n[h]
            for step, rows in ((1, self.T), (3, self.B)):
                self.hop1[h, step].wait_recv()
                k = (i - step) % 4
                self.hop2[h, step] = self.send(h, 0, step, k, j, rows)
                for way in (1, 3):
                    self.side[h, step, way] = self.send(h, 1, way, k, j, every)

    def owns_on(self):
        self.own_on = {}
        for h in range(2):
            i, j = self.n[h]
            for step, rows in ((1, self.T), (3, self.B)):
                self.own[h, step].wait_recv()
                self.own_on[h, step] = self.send(h, 1, step, i, (j - step) % 4, rows)

    def opposites(self):
        every = slice(None)
        for h in range(2):
            i, j = self.n[h]
            for step, rows in ((1, self.T), (3, self.B)):
                self.hop2[h, step].wait_recv()
                for way in (1, 3):
                    self.opp[h, step, way] = self.send(h, 1, way, (i + 2) % 4, j, rows)
            self.across(self.part(h, every, j, every))

    def sides_on(self):
        self.side_on = {}
        for h in range(2):
            i, j = self.n[h]
            for step in (1, 3):
                for way, rows in ((1, self.T), (3, self.B)):
                    self.side[h, step, way].wait_recv()
                    self.side_on[h, step, way] = self.send(
                        h, 1, way, (i - step) % 4, (j - way) % 4, rows
                    )

    def opposites_on(self):
        every = slice(None)
        self.opp_on = {}
        for h in range(2):
            i, j = self.n[h]
            for step, rows in ((1, self.T), (3, self.B)):
                self.opp[h, step, step].wait_recv()
                self.opp_on[h, step] = self.send(
                    h, 1, step, (i + 2) % 4, (j - step) % 4, rows
                )
        for h in range(2):
            i, j = self.n[h]
            for step in (1, 3):
                self.opp[h, step, 4 - step].wait_recv()
            for way in (1, 3):
                self.across(self.part(h, every, (j - way) % 4, every))

    def finals(self):
        every = slice(None)
        self.from_partner(0, 2)
        for h in range(2):
            i, j = self.n[h]
            far = (j + 2) % 4
            for step in (1, 3):
                self.own_on[h, step].wait_recv()
            self.across(self.part(h, i, far, every))
        for h in range(2):
            i, j = self.n[h]
            far = (j + 2) % 4
            for step in (1, 3):
                for way in (1, 3):
                    self.side_on[h, step, way].wait_recv()
                self.across(self.part(h, (i - step) % 4, far, every))
        self.from_partner(2, 6)
        for h in range(2):
            i, j = self.n[h]
            for step in (1, 3):
                self.opp_on[h, step].wait_recv()
            self.across(self.part(h, (i + 2) % 4, (j + 2) % 4, every))
        self.from_partner(6, 14)


N_COPIES = 131


def step_kernel(
    lookups_any, counts_any, slab_any, ids_any, label_any, sw_any, bias_any, wout_any,
    w_any, accum_any,
    ga_out, aa_out, sums_out, scale_out, grad_out,
    lookups_ref, counts_ref, slab_ref, ids_ref, label_ref, sw_ref, bias_ref, wout_ref,
    arrived_ref, rids_ref, scale_ref, grad_ref, lined,
    W, A, idsend, G, fac, hidden, dact, pacc, lg, LR, DL, gb, go, sv, rv,
    ZS, Df, ZRL, ZRR, ZL, ZR, DPL,
    R0, SB, RL, RV, Q, RL2, RV2,
    GA, AA, acc, slots, ns, NR, SC, slab, wout, strided,
    ssem, rsem, bulk, local, wsem,
):
    x, y, c, z = position()
    dp = (x * 4 + y) * 2 + c
    me = dp * 4 + z
    cp = Copies(ssem, rsem)
    go_to = cp.go
    zr, zl, zo = (z + 1) % 4, (z + 3) % 4, (z + 2) % 4
    xr, xl, xo = (x + 1) % 4, (x + 3) % 4, (x + 2) % 4
    yr, yl, yo = (y + 1) % 4, (y + 3) % 4, (y + 2) % 4
    LO, HI = slice(0, 1024), slice(1024, 2048)

    pairs_of = (
        (counts_any, counts_ref), (lookups_any, lookups_ref), (slab_any, slab_ref),
        (wout_any, wout_ref), (accum_any, A), (bias_any, bias_ref), (ids_any, ids_ref),
        (label_any, label_ref), (sw_any, sw_ref), (w_any, W),
    )
    loads = [pltpu.make_async_copy(a, b, local.at[k]) for k, (a, b) in enumerate(pairs_of)]
    for copy in loads:
        copy.start()
    barrier = pltpu.get_barrier_semaphore()

    def greet(p):
        pl.semaphore_signal(barrier, inc=1, device_id=p, device_id_type=LOGICAL)

    to_all(me, greet)
    for copy in loads[:5]:
        copy.wait()
    starts, ends = owner_bounds(counts_ref)
    own_rows = pl.ds(pl.multiple_of(z * 256, 256), 256)

    def gather_pair(k):
        lane = iota((256, 128), 1)
        got = []
        for side in range(2):
            slot = slot_rows(lookups_ref[2 * k + side : 2 * k + side + 1, :], starts, ends)
            column = as_column(slot)
            half = jnp.floor(column * 0.5)
            odd = column - 2.0 * half
            both = mm(tiles_over_lanes(half, 16), slab[...], 1, 0)
            one = jnp.where((lane >= 64) == (odd > 0.5), both, 0.0)
            got.append(one + pltpu.roll(one, 64, 1))
        G[own_rows, k * 128 : k * 128 + 128] = jnp.where(lane < 64, got[0], got[1]).astype(BF16)

    def block(src, k):
        return G.at[pl.ds(pl.multiple_of(src * 256, 256), 256), k * 256 : k * 256 + 256]

    def send_ids(p):
        pltpu.make_async_remote_copy(
            src_ref=idsend.at[p], dst_ref=rids_ref.at[me], send_sem=bulk.at[0],
            recv_sem=bulk.at[1], device_id=p, device_id_type=LOGICAL,
        ).start()

    right, left = {}, {}

    def send_block(k):
        right[k] = go_to(block(z, k), block(z, k), {"mp": zr})
        left[k] = go_to(block(z, k), block(z, k), {"mp": zl})

    for k in range(16):
        strided[pl.ds(k, 128, stride=16), :] = slab_ref[:, k * 128 : k * 128 + 128].astype(F32)
    slab[...] = strided[...].astype(BF16)
    for k in range(16):
        wout[:, k * 128 : k * 128 + 128] = wout_ref[k : k + 1, :].astype(F32)
    gather_pair(0)
    gather_pair(1)
    AA[x, y, c] = A[...].astype(BF16)
    pl.semaphore_wait(barrier, 127)
    send_block(0)
    aa = Spread(AA, go_to, (x, y, c, z), aa_out, wsem.at[0])
    aa.first()
    gather_pair(4)
    gather_pair(5)
    send_block(2)
    gather_pair(2)
    gather_pair(3)
    send_block(1)
    gather_pair(6)
    gather_pair(7)
    send_block(3)
    for copy in loads[5:9]:
        copy.wait()
    turned = jnp.concatenate([ids_ref[...].astype(F32), jnp.zeros((96, 128), F32)], axis=0)
    idsend[...] = turned.T.astype(I32).reshape(128, 1, 128)
    to_all(me, send_ids)
    rids_ref[me] = idsend[me]
    loads[9].wait()

    def forward(src):
        rows = pl.ds(pl.multiple_of(src * 256, 256), 256)
        pacc[...] = jnp.zeros_like(pacc)

        def tile(t, carry):
            cols = pl.ds(pl.multiple_of(t * 512, 512), 512)
            a = mm(G[rows, :], W[:, cols], 1, 0) + bias_ref[:, cols]
            wo = wout[:, cols]
            sg = lax.logistic(a)
            h = (a * sg).astype(BF16)
            hidden[rows, cols] = h
            fac[src, :, :, :, cols] = (wo * sg * (1.0 + a * (1.0 - sg))).reshape(4, 2, 32, 512)
            m = h.astype(F32) * wo
            pacc[...] += (m[:, 0:128] + m[:, 128:256]) + (m[:, 256:384] + m[:, 384:512])
            return carry

        lax.fori_loop(0, 4, tile, 0, unroll=2)
        for s in range(2):
            line = jnp.sum(pacc[128 * s : 128 * s + 128, :].T, axis=0, keepdims=True)
            lg[pl.ds(src * 2 + s, 1), :] = line

    right[0].wait_recv()
    f0 = go_to(block(zl, 0), block(zl, 0), {"mp": zr})
    left[2].wait_recv()
    f2 = go_to(block(zr, 2), block(zr, 2), {"mp": zl})
    forward(z)
    right[1].wait_recv()
    f1 = go_to(block(zl, 1), block(zl, 1), {"mp": zr})
    left[3].wait_recv()
    f3 = go_to(block(zr, 3), block(zr, 3), {"mp": zl})
    aa.second()
    right[2].wait_recv()
    right[3].wait_recv()
    forward(zl)
    left[0].wait_recv()
    left[1].wait_recv()
    forward(zr)
    aa.third()
    for copy in (f0, f1, f2, f3):
        copy.wait_recv()
    forward(zo)

    sent = [go_to(lg, LR.at[z], {"mp": (z + d) % 4}, bulk.at[8]) for d in (1, 2, 3)]
    LR[z] = lg[...]
    for copy in sent:
        copy.wait_recv()
    logit = (LR[0] + LR[1]) + (LR[2] + LR[3])
    DL[...] = sw_ref[...] * (lax.logistic(logit) - label_ref[...].astype(F32))

    def column(g):
        return jnp.broadcast_to(DL[pl.ds(g, 1), :], (128, 128)).T

    def dact_part(g, carry):
        rows = pl.ds(pl.multiple_of(g * 128, 128), 128)
        col = column(g)
        for t in range(16):
            cols = slice(128 * t, 128 * t + 128)
            f = fac[g // 2, pl.ds((g % 2) * 2, 2), :, :, cols].reshape(128, 128)
            dact[rows, cols] = (f * col).astype(BF16)
        return carry

    lax.fori_loop(0, 8, dact_part, 0)

    def sums_part(g, carry):
        rows = pl.ds(pl.multiple_of(g * 128, 128), 128)
        col = column(g)
        for t in range(16):
            cols = slice(128 * t, 128 * t + 128)
            d = dact[rows, cols].astype(F32)
            gb[:, cols] += jnp.sum(d.reshape(16, 8, 128), axis=0)
            m = hidden[rows, cols].astype(F32) * col
            go[:, cols] += jnp.sum(m.reshape(16, 8, 128), axis=0)
        return carry

    def dpool(dest, put):
        rows = pl.ds(pl.multiple_of(dest * 256, 256), 256)

        def tile(t, carry):
            at = pl.multiple_of(t * 512, 512)
            put(mm(dact[rows, :], W[pl.ds(at, 512), :], 1, 1), pl.ds(at, 512))
            return carry

        lax.fori_loop(0, 2, tile, 0)

    def put_far(d, cols):
        ZS[0, :, cols] = d.astype(BF16)

    dpool(zo, put_far)
    z1 = go_to(ZS.at[0, 0:128], ZRL, {"mp": zr})
    z2 = go_to(ZS.at[0, 128:256], ZRR, {"mp": zl})

    partner = {"dp_2": 1 - c}
    to_core = {}

    def weight_grad(xi, tag):
        at = pl.multiple_of(xi * 256, 256)

        def tile(t, carry):
            cols = pl.ds(pl.multiple_of(t * 1024, 1024), 1024)
            g = mm(G[:, pl.ds(at, 256)], dact[:, cols], 0, 0)
            fac[xi, :, :, :, cols] = g.reshape(4, 2, 32, 1024)
            SC[xi, :, :, cols] = fac[xi, :, 1 - c, :, cols].astype(BF16)
            return carry

        lax.fori_loop(0, 2, tile, 0)
        to_core[tag] = go_to(SC.at[xi], R0.at[xi], partner)

    def chip_sum(xi, tag):
        to_core[tag].wait_recv()
        for yi in range(4):
            s = R0[xi, yi].astype(F32) + fac[xi, yi, c]
            fac[xi, yi, c] = s
            SB[xi, yi] = s.astype(BF16)

    def put_right(d, cols):
        Df[0, :, cols] = d[0:128]
        ZS[1, 128:256, cols] = d[128:256].astype(BF16)

    def put_left(d, cols):
        ZS[2, 0:128, cols] = d[0:128].astype(BF16)
        Df[1, :, cols] = d[128:256]

    weight_grad(xo, "o")
    dpool(zr, put_right)
    z3 = go_to(ZS.at[1, 128:256], ZL.at[128:256], {"mp": zr})
    dpool(zl, put_left)
    z4 = go_to(ZS.at[2, 0:128], ZR.at[0:128], {"mp": zl})
    chip_sum(xo, "o")
    h0a = go_to(SB.at[xo, 0:2, :, LO], RL.at[0, 0], {"dp_0": xr})
    h0b = go_to(SB.at[xo, 2:4, :, LO], RL.at[0, 1], {"dp_0": xl})
    weight_grad(xr, "r")
    weight_grad(xl, "l")
    chip_sum(xr, "r")
    h0c = go_to(SB.at[xr, 2:4, :, LO], RV.at[0, 0, 2:4], {"dp_0": xr})
    weight_grad(x, "m")
    chip_sum(xl, "l")
    h0d = go_to(SB.at[xl, 0:2, :, LO], RV.at[0, 1, 0:2], {"dp_0": xl})
    z1.wait_recv()
    ZS[1, 0:128, :] = (Df[0] + ZRL[...].astype(F32)).astype(BF16)
    z5 = go_to(ZS.at[1, 0:128], ZL.at[0:128], {"mp": zr})
    z2.wait_recv()
    ZS[2, 128:256, :] = (Df[1] + ZRR[...].astype(F32)).astype(BF16)
    z6 = go_to(ZS.at[2, 128:256], ZR.at[128:256], {"mp": zl})
    aa.fourth()

    def put_own(d, cols):
        DPL[:, cols] = d

    dpool(z, put_own)
    chip_sum(x, "m")
    h1a = go_to(SB.at[0:2, yo, :, HI], RL.at[1, 0], {"dp_1": yr})
    h1b = go_to(SB.at[2:4, yo, :, HI], RL.at[1, 1], {"dp_1": yl})
    h1c = go_to(SB.at[2:4, yr, :, HI], RV.at[1, 0, 2:4], {"dp_1": yr})
    h1d = go_to(SB.at[0:2, yl, :, HI], RV.at[1, 1, 0:2], {"dp_1": yl})

    h0a.wait_recv()
    for k in range(2):
        SB[xr, k, :, LO] = (fac[xr, k, c, :, LO] + RL[0, 0, k].astype(F32)).astype(BF16)
    h0e = go_to(SB.at[xr, 0:2, :, LO], RV.at[0, 0, 0:2], {"dp_0": xr})
    h0b.wait_recv()
    for k in range(2):
        SB[xl, 2 + k, :, LO] = (fac[xl, 2 + k, c, :, LO] + RL[0, 1, k].astype(F32)).astype(BF16)
    h0f = go_to(SB.at[xl, 2:4, :, LO], RV.at[0, 1, 2:4], {"dp_0": xl})

    gb[...] = jnp.zeros_like(gb)
    go[...] = jnp.zeros_like(go)
    lax.fori_loop(0, 8, sums_part, 0)
    for t in range(16):
        cols = slice(128 * t, 128 * t + 128)
        sv[t] = jnp.sum(gb[:, cols], axis=0, keepdims=True)
        sv[16 + t] = jnp.sum(go[:, cols], axis=0, keepdims=True)

    def send_small(i, carry):
        p = (dp + i) % 32
        where = {"dp_0": p // 8, "dp_1": (p // 2) % 4, "dp_2": p % 2, "mp": z}
        pltpu.make_async_remote_copy(
            src_ref=sv.at[p], dst_ref=rv.at[dp], send_sem=bulk.at[2],
            recv_sem=bulk.at[3], device_id=where, device_id_type=MESH,
        ).start()
        return carry

    lax.fori_loop(1, 32, send_small, 0)
    rv[dp] = sv[dp]

    h1a.wait_recv()
    for k in range(2):
        SB[k, yr, :, HI] = (fac[k, yr, c, :, HI] + RL[1, 0, k].astype(F32)).astype(BF16)
    h1e = go_to(SB.at[0:2, yr, :, HI], RV.at[1, 0, 0:2], {"dp_1": yr})
    h1b.wait_recv()
    for k in range(2):
        SB[2 + k, yl, :, HI] = (fac[2 + k, yl, c, :, HI] + RL[1, 1, k].astype(F32)).astype(BF16)
    h1f = go_to(SB.at[2:4, yl, :, HI], RV.at[1, 1, 2:4], {"dp_1": yl})
    aa.fifth()

    def ring(h, axis, n):
        nr, nl, no = (n + 1) % 4, (n + 3) % 4, (n + 2) % 4
        s1 = go_to(Q.at[h, no, 0:16], RL2.at[h, 0], {axis: nr})
        s2 = go_to(Q.at[h, no, 16:32], RL2.at[h, 1], {axis: nl})
        s3 = go_to(Q.at[h, nr, 16:32], RV2.at[h, 0, 16:32], {axis: nr})
        s4 = go_to(Q.at[h, nl, 0:16], RV2.at[h, 1, 0:16], {axis: nl})
        return nr, nl, (s1, s2, s3, s4)

    def ring_relay(h, axis, state):
        nr, nl, (s1, s2, s3, s4) = state
        s1.wait_recv()
        Q[h, nr, 0:16] = Q[h, nr, 0:16] + RL2[h, 0]
        s5 = go_to(Q.at[h, nr, 0:16], RV2.at[h, 0, 0:16], {axis: nr})
        s2.wait_recv()
        Q[h, nl, 16:32] = Q[h, nl, 16:32] + RL2[h, 1]
        s6 = go_to(Q.at[h, nl, 16:32], RV2.at[h, 1, 16:32], {axis: nl})
        return s3, s4, s5, s6

    def segment(first, last):
        def pair(k, carry):
            lane = iota((256, 128), 1)
            block = DPL[:, pl.ds(pl.multiple_of(k * 128, 128), 128)]
            turned = pltpu.roll(block, 64, 1)
            hots, rows = [], []
            for side in range(2):
                slot = slot_rows(lookups_ref[pl.ds(2 * k + side, 1), :], starts, ends)
                slot = as_column(slot)
                sixteen = jnp.floor(slot * (1.0 / 16.0))
                both = jnp.floor(slot * (1.0 / 32.0))
                upper = sixteen - 2.0 * both
                hots.append(tiles_over_lanes(slot - 16.0 * (sixteen - both), 16))
                same = jnp.where((lane < 64) == (side == 0), block, turned)
                kept = jnp.where((lane >= 64) == (upper > 0.5), same, 0.0)
                rows.append(kept.astype(BF16))
            acc[...] += mm(jnp.concatenate(rows, axis=0), jnp.concatenate(hots, axis=0), 0, 0)
            return carry

        lax.fori_loop(first, last, pair, 0)

    def rows_of_table(first, last):
        def part(t, carry):
            lane = iota((256, 128), 1)
            block = arrived_ref[pl.ds(16 * t, 16)].reshape(256, 128).astype(F32)
            turned = pltpu.roll(block, 64, 1)
            hots, values = [], []
            for side in range(2):
                row = jnp.concatenate(
                    [lined[side, pl.ds(2 * t, 1), :], lined[side, pl.ds(2 * t + 1, 1), :]], axis=1
                )
                row = as_column(row)
                above = row >= 2048.0
                hots.append(tiles_over_lanes(jnp.where(above, row - 2048.0, row), 16))
                same = jnp.where((lane < 64) == (side == 0), block, turned)
                values.append(jnp.where((lane >= 64) == above, same, 0.0).astype(BF16))
            acc[...] += mm(
                jnp.concatenate(values, axis=0), jnp.concatenate(hots, axis=0), 0, 0
            )
            return carry

        lax.fori_loop(first, last, part, 0)

    for copy in (z3, z4, z5, z6):
        copy.wait_recv()
    DPL[...] = DPL[...] + (ZL[...].astype(F32) + ZR[...].astype(F32))
    acc[...] = jnp.zeros_like(acc)
    segment(0, 2)
    for copy in (h0c, h0d, h0e, h0f):
        copy.wait_recv()
    for k in range(4):
        Q[0, k] = fac[x, k, c, :, LO] + (RV[0, 0, k].astype(F32) + RV[0, 1, k].astype(F32))
    t0 = ring(0, "dp_1", y)
    segment(2, 4)
    for copy in (h1c, h1d, h1e, h1f):
        copy.wait_recv()
    for k in range(4):
        Q[1, k] = fac[k, y, c, :, HI] + (RV[1, 0, k].astype(F32) + RV[1, 1, k].astype(F32))
    t1 = ring(1, "dp_0", x)
    u0 = ring_relay(0, "dp_1", t0)
    segment(4, 6)
    u1 = ring_relay(1, "dp_0", t1)
    segment(6, 8)
    few = jnp.zeros((8, 128), F32)
    for t in range(16):
        piece = acc[:, 128 * t : 128 * t + 128]
        few = few + jnp.sum((piece * piece).reshape(16, 8, 128), axis=0)
        slots[8 * t : 8 * t + 8] = piece.T.astype(BF16).reshape(8, 16, 128)

    def send_slots(p):
        pltpu.make_async_remote_copy(
            src_ref=slots.at[p], dst_ref=arrived_ref.at[me], send_sem=bulk.at[4],
            recv_sem=bulk.at[5], device_id=p, device_id_type=LOGICAL,
        ).start()

    to_all(me, send_slots)
    arrived_ref[me] = slots[me]

    for copy in u0 + u1:
        copy.wait_recv()
    lower = Q[0, y] + (RV2[0, 0] + RV2[0, 1])
    upper = Q[1, x] + (RV2[1, 0] + RV2[1, 1])
    grad_ref[:, LO] = lower
    grad_ref[:, HI] = upper
    GA[x, y, c, :, LO] = lower.astype(BF16)
    GA[x, y, c, :, HI] = upper.astype(BF16)
    ga = Flow(GA, go_to, (x, y, c, z), ga_out, wsem.at[1])
    ga.start()
    both = lower * lower + upper * upper
    both = jnp.sum(both.reshape(4, 8, 1024), axis=0)
    for t in range(8):
        few = few + both[:, 128 * t : 128 * t + 128]
    small = sv.at[pl.ds(0, 31)]
    pltpu.make_async_copy(small, small, bulk.at[2]).wait()
    pltpu.make_async_copy(small, small, bulk.at[3]).wait()
    bias_sum = jnp.sum(rv[...], axis=0)
    ns[...] = jnp.sum(few, axis=0, keepdims=True) + bias_sum * bias_sum

    def send_norm(p):
        pltpu.make_async_remote_copy(
            src_ref=ns, dst_ref=NR.at[me], send_sem=bulk.at[6],
            recv_sem=bulk.at[7], device_id=p, device_id_type=LOGICAL,
        ).start()

    to_all(me, send_norm)
    put_grad = pltpu.make_async_copy(grad_ref, grad_out, local.at[10])
    put_grad.start()
    NR[me] = ns[...]
    ga.sides()

    heard = idsend.at[pl.ds(0, 127)]
    pltpu.make_async_copy(heard, heard, bulk.at[1]).wait()
    lane16 = iota((16, 128), 1) // 16
    numbers = rids_ref[...].astype(F32).reshape(16, 8, 128)
    for side in range(2):
        line = jnp.zeros((16, 128), F32)
        for d in range(8):
            shift = (16 * d - 16 * side) % 128
            line = jnp.where(lane16 == d, pltpu.roll(numbers[:, d, :], shift, 1), line)
        lined[side] = line
    acc[...] = jnp.zeros_like(acc)
    aa.last()
    ga.owns_on()
    ga.opposites()
    ga.sides_on()
    many = arrived_ref.at[pl.ds(0, 127)]
    pltpu.make_async_copy(many, many, bulk.at[5]).wait()
    rows_of_table(0, 4)
    ga.opposites_on()
    rows_of_table(4, 8)
    put_sums = pltpu.make_async_copy(acc, sums_out, local.at[11])
    put_sums.start()
    lot = NR.at[pl.ds(0, 127)]
    pltpu.make_async_copy(lot, lot, bulk.at[7]).wait()
    lanes = jnp.sum(NR[...], axis=0)
    norm = jnp.sum(lanes, axis=1, keepdims=True)
    scale = clip_norm / jnp.maximum(jnp.sqrt(norm), clip_norm)
    scale_ref[...] = jnp.broadcast_to(scale, (8, 128))
    put_scale = pltpu.make_async_copy(scale_ref, scale_out, local.at[12])
    put_scale.start()
    ga.finals()
    pltpu.make_async_copy(lot, lot, bulk.at[6]).wait()
    pltpu.make_async_copy(many, many, bulk.at[4]).wait()
    pltpu.make_async_copy(heard, heard, bulk.at[0]).wait()
    put_grad.wait()
    put_sums.wait()
    put_scale.wait()
    pltpu.make_async_copy(LR.at[0:3], LR.at[0:3], bulk.at[8]).wait()
    cp.drain(W)
    aa.close()
    ga.close()


def finish_kernel(
    sums_any, scale_ref, table_any, accum_any, grad_any, dense_any,
    ga_any, aa_any, w_any,
    new_any, accum_new_any, dense_new_any, wn_any,
    GA, AA, W, WN, sums, table, accum, grad, dense, new, accum_new, dense_new, sem, isem, osem,
):
    chunk = 128
    count = 1024 // chunk

    def load(i):
        rows = pl.ds(i * chunk, chunk)
        for j, (src, dst) in enumerate(((ga_any, GA), (aa_any, AA), (w_any, W))):
            pltpu.make_async_copy(src.at[rows], dst.at[rows], sem.at[i, j]).start()

    small = [
        pltpu.make_async_copy(src, dst, isem.at[k])
        for k, (src, dst) in enumerate(
            (
                (grad_any, grad), (dense_any, dense), (accum_any, accum),
                (sums_any, sums), (table_any, table),
            )
        )
    ]
    load(0)
    load(1)
    for copy in small:
        copy.start()
    for i in range(2, count):
        load(i)
    scale = scale_ref[0:1, 0:1]

    def part(t, carry):
        rows = pl.ds(pl.multiple_of(t * chunk, chunk), chunk)
        for j, (src, dst) in enumerate(((ga_any, GA), (aa_any, AA), (w_any, W))):
            pltpu.make_async_copy(src.at[rows], dst.at[rows], sem.at[t, j]).wait()
        for q in range(16):
            cols = slice(128 * q, 128 * q + 128)
            g = scale * GA[rows, cols].astype(F32)
            r = lax.rsqrt(AA[rows, cols].astype(F32) + g * g)
            r = r - (adagrad_eps * r) * r
            WN[rows, cols] = (W[rows, cols].astype(F32) - (dense_rate * g) * r).astype(BF16)
        pltpu.make_async_copy(WN.at[rows], wn_any.at[rows], osem.at[0]).start()
        return carry

    lax.fori_loop(0, count, part, 0)
    for copy in small:
        copy.wait()
    clipped = scale * grad[...]
    dense_new[...] = dense[...] + clipped * clipped
    puts = [pltpu.make_async_copy(dense_new, dense_new_any, osem.at[1])]
    puts[0].start()
    for upper in range(2):
        for p in range(16):
            r = sums[64 * upper : 64 * upper + 64, 128 * p : 128 * p + 128] * scale
            line = p + upper * 16
            fresh = accum[line : line + 1, :] + jnp.sum(r * r, axis=0, keepdims=True) / 64.0
            accum_new[line : line + 1, :] = fresh
            at = line * 128
            rate = table_rate / (jnp.sqrt(fresh) + adagrad_eps)
            new[:, at : at + 128] = table[:, at : at + 128] - r * rate
        cols = pl.ds(2048 * upper, 2048)
        puts.append(
            pltpu.make_async_copy(new.at[:, cols], new_any.at[:, cols], osem.at[2 + upper])
        )
        puts[-1].start()
    puts.append(pltpu.make_async_copy(accum_new, accum_new_any, osem.at[4]))
    puts[-1].start()
    pltpu.make_async_copy(WN, wn_any, osem.at[0]).wait()
    for copy in puts:
        copy.wait()


def shape(dims, kind):
    return jax.ShapeDtypeStruct(dims, kind)


def body(
    slab_values,
    row_ids,
    peer_counts,
    lookup_slots,
    labels,
    sample_weight,
    weight_in,
    bias_in,
    weight_out,
    dense_accum,
    table_rows,
    table_accum,
):
    V = pltpu.VMEM
    DMA = pltpu.SemaphoreType.DMA
    whole = (4, 4, 2, 32, 2048)
    ga, aa, sums, scale, grad = pl.pallas_call(
        step_kernel,
        out_shape=(
            shape(whole, BF16), shape(whole, BF16), shape((128, 2048), F32),
            shape((8, 128), F32), shape((32, 2048), F32),
        ),
        in_specs=[ANY] * 10,
        out_specs=(ANY,) * 5,
        scratch_shapes=[
            V((16, 256), I32), V((1, 128), I32), V((128, 2048), BF16), V((32, 128), I32),
            V((8, 128), I32), V((8, 128), F32), V((1, 2048), F32), V((16, 128), BF16),
            V((128, 16, 128), BF16), V((128, 1, 128), I32), V((8, 128), F32), V((32, 2048), F32),
            V((2, 16, 128), F32),
            V((1024, 2048), BF16), V((32, 2048), F32), V((128, 1, 128), I32),
            V((1024, 1024), BF16), V(whole, F32), V((1024, 2048), BF16),
            V((1024, 2048), BF16), V((256, 128), F32), V((8, 128), F32), V((4, 8, 128), F32),
            V((8, 128), F32), V((8, 2048), F32), V((8, 2048), F32),
            V((32, 1, 128), F32), V((32, 1, 128), F32),
            V((3, 256, 1024), BF16), V((2, 128, 1024), F32),
            V((128, 1024), BF16), V((128, 1024), BF16),
            V((256, 1024), BF16), V((256, 1024), BF16), V((256, 1024), F32),
            V((4, 4, 32, 2048), BF16), V((4, 4, 32, 2048), BF16),
            V((2, 2, 2, 32, 1024), BF16), V((2, 2, 4, 32, 1024), BF16),
            V((2, 4, 32, 1024), F32), V((2, 2, 16, 1024), F32), V((2, 2, 32, 1024), F32),
            V(whole, BF16), V(whole, BF16), V((128, 2048), F32), V((128, 16, 128), BF16),
            V((1, 128), F32), V((128, 1, 128), F32), V((4, 4, 32, 2048), BF16),
            V((2048, 128), BF16), V((1, 2048), F32), V((2048, 128), F32),
            DMA((4,)), DMA((N_COPIES,)), DMA((9,)), DMA((13,)), DMA((2,)),
        ],
        compiler_params=pltpu.CompilerParams(
            has_side_effects=True, vmem_limit_bytes=63 * 1024 * 1024, collective_id=0
        ),
        name="step",
    )(
        lookup_slots.T,
        peer_counts,
        slab_values[0],
        row_ids[0].T,
        labels.reshape(8, 128),
        sample_weight.reshape(8, 128),
        bias_in.reshape(1, 2048),
        weight_out.reshape(16, 128),
        weight_in,
        dense_accum,
    )
    table_new, table_accum_new, accum_new, weight_new = pl.pallas_call(
        finish_kernel,
        out_shape=(
            shape((64, 4096), F32), shape((32, 128), F32), shape((32, 2048), F32),
            shape((1024, 2048), BF16),
        ),
        in_specs=[ANY, VM] + [ANY] * 7,
        out_specs=(ANY,) * 4,
        scratch_shapes=[
            V((1024, 2048), BF16), V((1024, 2048), BF16), V((1024, 2048), BF16),
            V((1024, 2048), BF16), V((128, 2048), F32), V((64, 4096), F32), V((32, 128), F32),
            V((32, 2048), F32), V((32, 2048), F32), V((64, 4096), F32), V((32, 128), F32),
            V((32, 2048), F32), DMA((8, 3)), DMA((5,)), DMA((5,)),
        ],
        name="finish",
    )(
        sums,
        scale,
        table_rows.T,
        table_accum.reshape(32, 128),
        grad,
        dense_accum,
        ga.reshape(1024, 2048),
        aa.reshape(1024, 2048),
        weight_in,
    )
    return (weight_new, accum_new, table_new.T, table_accum_new.reshape(4096))


def solution(mesh):
    torus = Mesh(mesh.devices.reshape(4, 4, 2, mesh.shape["mp"]), ("dp_0", "dp_1", "dp_2", "mp"))
    placed = (
        P(DP_MP, None, None),
        P(DP_MP, None, None),
        P(DP_MP, None),
        P(DP_MP, None),
        P(DP),
        P(DP),
        P(None, "mp"),
        P("mp"),
        P("mp"),
        P(DP, "mp"),
        P(DP_MP, None),
        P(DP_MP),
    )
    return jax.shard_map(
        body,
        mesh=torus,
        in_specs=placed,
        out_specs=(P(None, "mp"), P(DP, "mp"), P(DP_MP, None), P(DP_MP)),
        check_vma=False,
    )
```

```python
import functools

import jax
import jax.numpy as jnp
from jax import lax
from jax.experimental import pallas as pl
from jax.experimental.pallas import tpu as pltpu
from jax.sharding import Mesh
from jax.sharding import PartitionSpec as P

DP = ("dp_0", "dp_1", "dp_2")
DP_MP = ("dp_0", "dp_1", "dp_2", "mp")

clip_norm = 1.0
dense_rate = 0.02
table_rate = 0.5
adagrad_eps = 1e-10

F32 = jnp.float32
BF16 = jnp.bfloat16
I32 = jnp.int32
MESH = pl.DeviceIdType.MESH
LOGICAL = pl.DeviceIdType.LOGICAL
VM = pl.BlockSpec(memory_space=pltpu.VMEM)
ANY = pl.BlockSpec(memory_space=pl.ANY)


def mm(a, b, ca, cb):
    return lax.dot_general(a, b, (((ca,), (cb,)), ((), ())), preferred_element_type=F32)


def iota(shape, dim):
    return lax.broadcasted_iota(I32, shape, dim)


def position():
    return tuple(lax.axis_index(a) for a in DP_MP)


def to_all(me, emit):
    for u in range(1, 8):
        emit(lax.rem(me + u, 128))

    def more(j, carry):
        base = me + 8 * j
        for u in range(8):
            emit(lax.rem(base + u, 128))
        return carry

    lax.fori_loop(1, 16, more, 0)


class Copies:
    def __init__(self, send, recv):
        self.send, self.recv, self.used, self.sent = send, recv, 0, [0]

    def go(self, src, dst, where, send=None):
        if send is None:
            rows = src.size * (4 if src.dtype == F32 else 2) // 4096
            if self.sent[-1] + rows > 1024:
                self.sent.append(0)
            self.sent[-1] += rows
            send = self.send.at[len(self.sent) - 1]
        copy = pltpu.make_async_remote_copy(
            src_ref=src,
            dst_ref=dst,
            send_sem=send,
            recv_sem=self.recv.at[self.used],
            device_id=where,
            device_id_type=MESH,
        )
        self.used += 1
        copy.start()
        return copy

    def drain(self, rows_of_4k):
        for k, count in enumerate(self.sent):
            some = rows_of_4k.at[pl.ds(0, count)]
            pltpu.make_async_copy(some, some, self.send.at[k]).wait()


def owner_bounds(counts_ref):
    counts = jnp.broadcast_to(counts_ref[...].astype(F32), (128, 128))
    upto = jnp.where(iota((128, 128), 0) <= iota((128, 128), 1), 1.0, 0.0).astype(BF16)
    ends = mm(counts.astype(BF16), upto, 1, 0)
    return (ends - counts).T, ends.T


def slot_rows(lookups, starts, ends):
    q = lookups.astype(F32)
    outs = []
    for part in range(q.shape[1] // 128):
        row = q[:, part * 128 : part * 128 + 128]
        hit = (row >= starts) & (row < ends)
        owner = iota((128, 128), 0).astype(F32)
        shift = jnp.sum(jnp.where(hit, owner * 32.0 - starts, 0.0), axis=0, keepdims=True)
        outs.append(row + shift)
    return jnp.concatenate(outs, axis=1)


def as_column(row):
    parts = []
    for part in range(row.shape[1] // 128):
        piece = row[:, part * 128 : part * 128 + 128]
        parts.append(jnp.broadcast_to(piece, (128, 128)).T)
    return jnp.concatenate(parts, axis=0)


def tiles_over_rows(index, count):
    high = jnp.floor(index * (1.0 / 16.0))
    low = index - 16.0 * high
    n = index.shape[1]
    inner = jnp.where(iota((16, n), 0).astype(F32) == low, 1.0, 0.0).astype(BF16)
    high = jnp.broadcast_to(high, (16, n)).astype(BF16)
    zero = jnp.zeros((16, n), BF16)
    return jnp.concatenate(
        [jnp.where(high == jnp.asarray(t, BF16), inner, zero) for t in range(count)], axis=0
    )


def tiles_over_lanes(column, count):
    high = jnp.floor(column * (1.0 / 128.0))
    low = column - 128.0 * high
    inner = jnp.where(iota(column.shape, 1).astype(F32) == low, 1.0, 0.0).astype(BF16)
    high = high.astype(BF16)
    zero = jnp.zeros(column.shape, BF16)
    return jnp.concatenate(
        [jnp.where(high == jnp.asarray(t, BF16), inner, zero) for t in range(count)], axis=1
    )


class Spread:
    LO, HI = slice(0, 1024), slice(1024, 2048)
    T, B = slice(0, 16), slice(16, 32)

    def __init__(self, ref, go, where, out, sem):
        self.ref, self.go, self.out, self.sem = ref, go, out, sem
        self.x, self.y, self.c, _ = where
        self.xr, self.xl, self.xo = ((self.x + d) % 4 for d in (1, 3, 2))
        self.yr, self.yl, self.yo = ((self.y + d) % 4 for d in (1, 3, 2))
        self.partner = {"dp_2": 1 - self.c}
        self.d, self.pieces = [], []

    def across(self, *pieces):
        for piece in pieces:
            self.d.append(self.same(piece, self.partner))
            self.pieces.append(piece)
            self.write(piece)

    def from_partner(self, first, last):
        for k in range(first, last):
            self.d[k].wait_recv()
            a, b, _, rows, cols = self.pieces[k]
            self.write((a, b, 1 - self.c, rows, cols))

    def write(self, piece):
        pltpu.make_async_copy(self.ref.at[piece], self.out.at[piece], self.sem).start()

    def same(self, piece, where):
        ref = self.ref.at[piece]
        return self.go(ref, ref, where)

    def first(self):
        x, y, c = self.x, self.y, self.c
        every = slice(None)
        self.p1 = self.same((x, y, c, every, self.LO), {"dp_0": self.xr})
        self.p2 = self.same((x, y, c, every, self.LO), {"dp_0": self.xl})
        self.q1 = self.same((x, y, c, every, self.HI), {"dp_1": self.yr})
        self.q2 = self.same((x, y, c, every, self.HI), {"dp_1": self.yl})

    def second(self):
        x, y, c = self.x, self.y, self.c
        self.p1.wait_recv()
        self.p3 = self.same((self.xl, y, c, self.T, self.LO), {"dp_0": self.xr})
        self.p2.wait_recv()
        self.p4 = self.same((self.xr, y, c, self.B, self.LO), {"dp_0": self.xl})
        self.q1.wait_recv()
        self.q3 = self.same((x, self.yl, c, self.T, self.HI), {"dp_1": self.yr})
        self.q2.wait_recv()
        self.q4 = self.same((x, self.yr, c, self.B, self.HI), {"dp_1": self.yl})

    def third(self):
        x, y, c = self.x, self.y, self.c
        every = slice(None)
        self.p3.wait_recv()
        self.p4.wait_recv()
        mine, other = (every, y, c, every, self.LO), (x, every, c, every, self.HI)
        self.p5 = self.same(mine, {"dp_1": self.yr})
        self.p6 = self.same(mine, {"dp_1": self.yl})
        self.q3.wait_recv()
        self.q4.wait_recv()
        self.q5 = self.same(other, {"dp_0": self.xr})
        self.q6 = self.same(other, {"dp_0": self.xl})
        self.across(mine, other)

    def fourth(self):
        c = self.c
        every = slice(None)
        self.p5.wait_recv()
        self.p7 = self.same((slice(0, 2), self.yl, c, every, self.LO), {"dp_1": self.yr})
        self.p6.wait_recv()
        self.p8 = self.same((slice(2, 4), self.yr, c, every, self.LO), {"dp_1": self.yl})
        self.q5.wait_recv()
        self.q7 = self.same((self.xl, slice(0, 2), c, every, self.HI), {"dp_0": self.xr})
        self.q6.wait_recv()
        self.q8 = self.same((self.xr, slice(2, 4), c, every, self.HI), {"dp_0": self.xl})
        self.across(*((every, n, c, every, self.LO) for n in (self.yl, self.yr)))
        self.across(*((n, every, c, every, self.HI) for n in (self.xl, self.xr)))
        self.from_partner(0, 2)

    def fifth(self):
        c = self.c
        every = slice(None)
        self.p7.wait_recv()
        self.p8.wait_recv()
        self.across((every, self.yo, c, every, self.LO))
        self.q7.wait_recv()
        self.q8.wait_recv()
        self.across((self.xo, every, c, every, self.HI))
        self.from_partner(2, 6)

    def last(self):
        self.from_partner(6, 8)

    def close(self):
        pltpu.make_async_copy(self.ref, self.out, self.sem).wait()


class Flow(Spread):
    def part(self, h, i, j, rows):
        if h == 0:
            return (i, j, self.c, rows, self.LO)
        return (j, i, self.c, rows, self.HI)

    def send(self, h, axis, step, i, j, rows):
        along_x = (h == 0) == (axis == 0)
        n = self.x if along_x else self.y
        return self.same(
            self.part(h, i, j, rows), {"dp_0" if along_x else "dp_1": (n + step) % 4}
        )

    def start(self):
        every = slice(None)
        self.n = ((self.x, self.y), (self.y, self.x))
        self.hop1, self.own, self.side, self.opp = {}, {}, {}, {}
        for h in range(2):
            i, j = self.n[h]
            for step in (1, 3):
                self.hop1[h, step] = self.send(h, 0, step, i, j, every)
        for h in range(2):
            i, j = self.n[h]
            for step in (1, 3):
                self.own[h, step] = self.send(h, 1, step, i, j, every)

    def sides(self):
        every = slice(None)
        self.hop2 = {}
        for h in range(2):
            i, j = self.n[h]
            for step, rows in ((1, self.T), (3, self.B)):
                self.hop1[h, step].wait_recv()
                k = (i - step) % 4
                self.hop2[h, step] = self.send(h, 0, step, k, j, rows)
                for way in (1, 3):
                    self.side[h, step, way] = self.send(h, 1, way, k, j, every)

    def owns_on(self):
        self.own_on = {}
        for h in range(2):
            i, j = self.n[h]
            for step, rows in ((1, self.T), (3, self.B)):
                self.own[h, step].wait_recv()
                self.own_on[h, step] = self.send(h, 1, step, i, (j - step) % 4, rows)

    def opposites(self):
        every = slice(None)
        for h in range(2):
            i, j = self.n[h]
            for step, rows in ((1, self.T), (3, self.B)):
                self.hop2[h, step].wait_recv()
                for way in (1, 3):
                    self.opp[h, step, way] = self.send(h, 1, way, (i + 2) % 4, j, rows)
            self.across(self.part(h, every, j, every))

    def sides_on(self):
        self.side_on = {}
        for h in range(2):
            i, j = self.n[h]
            for step in (1, 3):
                for way, rows in ((1, self.T), (3, self.B)):
                    self.side[h, step, way].wait_recv()
                    self.side_on[h, step, way] = self.send(
                        h, 1, way, (i - step) % 4, (j - way) % 4, rows
                    )

    def opposites_on(self):
        every = slice(None)
        self.opp_on = {}
        for h in range(2):
            i, j = self.n[h]
            for step, rows in ((1, self.T), (3, self.B)):
                self.opp[h, step, step].wait_recv()
                self.opp_on[h, step] = self.send(
                    h, 1, step, (i + 2) % 4, (j - step) % 4, rows
                )
        for h in range(2):
            i, j = self.n[h]
            for step in (1, 3):
                self.opp[h, step, 4 - step].wait_recv()
            for way in (1, 3):
                self.across(self.part(h, every, (j - way) % 4, every))

    def finals(self):
        every = slice(None)
        self.from_partner(0, 2)
        for h in range(2):
            i, j = self.n[h]
            far = (j + 2) % 4
            for step in (1, 3):
                self.own_on[h, step].wait_recv()
            self.across(self.part(h, i, far, every))
        for h in range(2):
            i, j = self.n[h]
            far = (j + 2) % 4
            for step in (1, 3):
                for way in (1, 3):
                    self.side_on[h, step, way].wait_recv()
                self.across(self.part(h, (i - step) % 4, far, every))
        self.from_partner(2, 6)
        for h in range(2):
            i, j = self.n[h]
            for step in (1, 3):
                self.opp_on[h, step].wait_recv()
            self.across(self.part(h, (i + 2) % 4, (j + 2) % 4, every))
        self.from_partner(6, 14)


N_COPIES = 131


def step_kernel(
    lookups_any, counts_any, slab_any, ids_any, label_any, sw_any, bias_any, wout_any,
    w_any, accum_any,
    ga_out, aa_out, sums_out, scale_out, grad_out,
    lookups_ref, counts_ref, slab_ref, ids_ref, label_ref, sw_ref, bias_ref, wout_ref,
    arrived_ref, rids_ref, scale_ref, grad_ref, lined,
    W, A, idsend, G, fac, hidden, dact, pacc, lg, LR, DL, gb, go, sv, rv,
    ZS, Df, ZRL, ZRR, ZL, ZR, DPL,
    R0, SB, RL, RV, Q, RL2, RV2,
    GA, AA, acc, slots, ns, NR, GT, slab, wout, strided,
    ssem, rsem, bulk, local, wsem,
):
    x, y, c, z = position()
    dp = (x * 4 + y) * 2 + c
    me = dp * 4 + z
    cp = Copies(ssem, rsem)
    go_to = cp.go
    zr, zl, zo = (z + 1) % 4, (z + 3) % 4, (z + 2) % 4
    xr, xl, xo = (x + 1) % 4, (x + 3) % 4, (x + 2) % 4
    yr, yl, yo = (y + 1) % 4, (y + 3) % 4, (y + 2) % 4
    LO, HI = slice(0, 1024), slice(1024, 2048)

    pairs_of = (
        (counts_any, counts_ref), (lookups_any, lookups_ref), (slab_any, slab_ref),
        (wout_any, wout_ref), (accum_any, A), (bias_any, bias_ref), (ids_any, ids_ref),
        (label_any, label_ref), (sw_any, sw_ref), (w_any, W),
    )
    loads = [pltpu.make_async_copy(a, b, local.at[k]) for k, (a, b) in enumerate(pairs_of)]
    for copy in loads:
        copy.start()
    barrier = pltpu.get_barrier_semaphore()

    def greet(p):
        pl.semaphore_signal(barrier, inc=1, device_id=p, device_id_type=LOGICAL)

    to_all(me, greet)
    for copy in loads[:5]:
        copy.wait()
    starts, ends = owner_bounds(counts_ref)
    own_rows = pl.ds(pl.multiple_of(z * 256, 256), 256)

    def gather_pair(k):
        lane = iota((256, 128), 1)
        got = []
        for side in range(2):
            slot = slot_rows(lookups_ref[2 * k + side : 2 * k + side + 1, :], starts, ends)
            column = as_column(slot)
            half = jnp.floor(column * 0.5)
            odd = column - 2.0 * half
            both = mm(tiles_over_lanes(half, 16), slab[...], 1, 0)
            one = jnp.where((lane >= 64) == (odd > 0.5), both, 0.0)
            got.append(one + pltpu.roll(one, 64, 1))
        G[own_rows, k * 128 : k * 128 + 128] = jnp.where(lane < 64, got[0], got[1]).astype(BF16)

    def block(src, k):
        return G.at[pl.ds(pl.multiple_of(src * 256, 256), 256), k * 256 : k * 256 + 256]

    def send_ids(p):
        pltpu.make_async_remote_copy(
            src_ref=idsend.at[p], dst_ref=rids_ref.at[me], send_sem=bulk.at[0],
            recv_sem=bulk.at[1], device_id=p, device_id_type=LOGICAL,
        ).start()

    right, left = {}, {}

    def send_block(k):
        right[k] = go_to(block(z, k), block(z, k), {"mp": zr})
        left[k] = go_to(block(z, k), block(z, k), {"mp": zl})

    for k in range(16):
        strided[pl.ds(k, 128, stride=16), :] = slab_ref[:, k * 128 : k * 128 + 128].astype(F32)
    slab[...] = strided[...].astype(BF16)
    for k in range(16):
        wout[:, k * 128 : k * 128 + 128] = wout_ref[k : k + 1, :].astype(F32)
    gather_pair(0)
    gather_pair(1)
    AA[x, y, c] = A[...].astype(BF16)
    pl.semaphore_wait(barrier, 127)
    send_block(0)
    aa = Spread(AA, go_to, (x, y, c, z), aa_out, wsem.at[0])
    aa.first()
    gather_pair(4)
    gather_pair(5)
    send_block(2)
    gather_pair(2)
    gather_pair(3)
    send_block(1)
    gather_pair(6)
    gather_pair(7)
    send_block(3)
    for copy in loads[5:9]:
        copy.wait()
    turned = jnp.concatenate([ids_ref[...].astype(F32), jnp.zeros((96, 128), F32)], axis=0)
    idsend[...] = turned.T.astype(I32).reshape(128, 1, 128)
    to_all(me, send_ids)
    rids_ref[me] = idsend[me]
    loads[9].wait()

    def forward(src):
        rows = pl.ds(pl.multiple_of(src * 256, 256), 256)
        pacc[...] = jnp.zeros_like(pacc)

        def tile(t, carry):
            cols = pl.ds(pl.multiple_of(t * 512, 512), 512)
            a = mm(G[rows, :], W[:, cols], 1, 0) + bias_ref[:, cols]
            wo = wout[:, cols]
            sg = lax.logistic(a)
            h = (a * sg).astype(BF16)
            hidden[rows, cols] = h
            fac[src, :, :, :, cols] = (wo * sg * (1.0 + a * (1.0 - sg))).reshape(4, 2, 32, 512)
            m = h.astype(F32) * wo
            pacc[...] += (m[:, 0:128] + m[:, 128:256]) + (m[:, 256:384] + m[:, 384:512])
            return carry

        lax.fori_loop(0, 4, tile, 0, unroll=2)
        for s in range(2):
            line = jnp.sum(pacc[128 * s : 128 * s + 128, :].T, axis=0, keepdims=True)
            lg[pl.ds(src * 2 + s, 1), :] = line

    def turn(src):
        rows = pl.ds(pl.multiple_of(src * 256, 256), 256)
        for t in range(4):
            GT[256 * t : 256 * t + 256, rows] = G[rows, 256 * t : 256 * t + 256].T

    right[0].wait_recv()
    f0 = go_to(block(zl, 0), block(zl, 0), {"mp": zr})
    left[2].wait_recv()
    f2 = go_to(block(zr, 2), block(zr, 2), {"mp": zl})
    forward(z)
    turn(z)
    right[1].wait_recv()
    f1 = go_to(block(zl, 1), block(zl, 1), {"mp": zr})
    left[3].wait_recv()
    f3 = go_to(block(zr, 3), block(zr, 3), {"mp": zl})
    aa.second()
    right[2].wait_recv()
    right[3].wait_recv()
    forward(zl)
    left[0].wait_recv()
    left[1].wait_recv()
    forward(zr)
    turn(zl)
    aa.third()
    for copy in (f0, f1, f2, f3):
        copy.wait_recv()
    forward(zo)

    sent = [go_to(lg, LR.at[z], {"mp": (z + d) % 4}, bulk.at[8]) for d in (1, 2, 3)]
    LR[z] = lg[...]
    turn(zr)
    turn(zo)
    for copy in sent:
        copy.wait_recv()
    logit = (LR[0] + LR[1]) + (LR[2] + LR[3])
    DL[...] = sw_ref[...] * (lax.logistic(logit) - label_ref[...].astype(F32))

    def column(g):
        return jnp.broadcast_to(DL[pl.ds(g, 1), :], (128, 128)).T

    def dact_part(g, carry):
        rows = pl.ds(pl.multiple_of(g * 128, 128), 128)
        col = column(g)
        for t in range(16):
            cols = slice(128 * t, 128 * t + 128)
            f = fac[g // 2, pl.ds((g % 2) * 2, 2), :, :, cols].reshape(128, 128)
            dact[rows, cols] = (f * col).astype(BF16)
        return carry

    lax.fori_loop(0, 8, dact_part, 0)

    def sums_part(g, carry):
        rows = pl.ds(pl.multiple_of(g * 128, 128), 128)
        col = column(g)
        for t in range(16):
            cols = slice(128 * t, 128 * t + 128)
            d = dact[rows, cols].astype(F32)
            gb[:, cols] += jnp.sum(d.reshape(16, 8, 128), axis=0)
            m = hidden[rows, cols].astype(F32) * col
            go[:, cols] += jnp.sum(m.reshape(16, 8, 128), axis=0)
        return carry

    def dpool(dest, put):
        rows = pl.ds(pl.multiple_of(dest * 256, 256), 256)

        def tile(t, carry):
            at = pl.multiple_of(t * 512, 512)
            put(mm(dact[rows, :], W[pl.ds(at, 512), :], 1, 1), pl.ds(at, 512))
            return carry

        lax.fori_loop(0, 2, tile, 0)

    def put_far(d, cols):
        ZS[0, :, cols] = d.astype(BF16)

    dpool(zo, put_far)
    z1 = go_to(ZS.at[0, 0:128], ZRL, {"mp": zr})
    z2 = go_to(ZS.at[0, 128:256], ZRR, {"mp": zl})

    partner = {"dp_2": 1 - c}
    to_core = {}

    def weight_grad(xi, tag):
        at = pl.multiple_of(xi * 256, 256)

        def tile(t, carry):
            cols = pl.ds(pl.multiple_of(t * 1024, 1024), 1024)
            g = mm(GT[pl.ds(at, 256), :], dact[:, cols], 1, 0)
            fac[xi, :, :, :, cols] = g.reshape(4, 2, 32, 1024)
            return carry

        lax.fori_loop(0, 2, tile, 0)
        to_core[tag] = go_to(fac.at[xi, :, 1 - c], R0.at[xi], partner)

    def chip_sum(xi, tag):
        to_core[tag].wait_recv()
        for yi in range(4):
            s = R0[xi, yi] + fac[xi, yi, c]
            fac[xi, yi, c] = s
            SB[xi, yi] = s.astype(BF16)

    def put_right(d, cols):
        Df[0, :, cols] = d[0:128]
        ZS[1, 128:256, cols] = d[128:256].astype(BF16)

    def put_left(d, cols):
        ZS[2, 0:128, cols] = d[0:128].astype(BF16)
        Df[1, :, cols] = d[128:256]

    weight_grad(xo, "o")
    dpool(zr, put_right)
    z3 = go_to(ZS.at[1, 128:256], ZL.at[128:256], {"mp": zr})
    dpool(zl, put_left)
    z4 = go_to(ZS.at[2, 0:128], ZR.at[0:128], {"mp": zl})
    chip_sum(xo, "o")
    h0a = go_to(SB.at[xo, 0:2, :, LO], RL.at[0, 0], {"dp_0": xr})
    h0b = go_to(SB.at[xo, 2:4, :, LO], RL.at[0, 1], {"dp_0": xl})
    weight_grad(xr, "r")
    weight_grad(xl, "l")
    chip_sum(xr, "r")
    h0c = go_to(SB.at[xr, 2:4, :, LO], RV.at[0, 0, 2:4], {"dp_0": xr})
    weight_grad(x, "m")
    chip_sum(xl, "l")
    h0d = go_to(SB.at[xl, 0:2, :, LO], RV.at[0, 1, 0:2], {"dp_0": xl})
    z1.wait_recv()
    ZS[1, 0:128, :] = (Df[0] + ZRL[...].astype(F32)).astype(BF16)
    z5 = go_to(ZS.at[1, 0:128], ZL.at[0:128], {"mp": zr})
    z2.wait_recv()
    ZS[2, 128:256, :] = (Df[1] + ZRR[...].astype(F32)).astype(BF16)
    z6 = go_to(ZS.at[2, 128:256], ZR.at[128:256], {"mp": zl})
    aa.fourth()

    def put_own(d, cols):
        DPL[:, cols] = d

    dpool(z, put_own)
    chip_sum(x, "m")
    h1a = go_to(SB.at[0:2, yo, :, HI], RL.at[1, 0], {"dp_1": yr})
    h1b = go_to(SB.at[2:4, yo, :, HI], RL.at[1, 1], {"dp_1": yl})
    h1c = go_to(SB.at[2:4, yr, :, HI], RV.at[1, 0, 2:4], {"dp_1": yr})
    h1d = go_to(SB.at[0:2, yl, :, HI], RV.at[1, 1, 0:2], {"dp_1": yl})

    h0a.wait_recv()
    for k in range(2):
        SB[xr, k, :, LO] = (fac[xr, k, c, :, LO] + RL[0, 0, k].astype(F32)).astype(BF16)
    h0e = go_to(SB.at[xr, 0:2, :, LO], RV.at[0, 0, 0:2], {"dp_0": xr})
    h0b.wait_recv()
    for k in range(2):
        SB[xl, 2 + k, :, LO] = (fac[xl, 2 + k, c, :, LO] + RL[0, 1, k].astype(F32)).astype(BF16)
    h0f = go_to(SB.at[xl, 2:4, :, LO], RV.at[0, 1, 2:4], {"dp_0": xl})

    gb[...] = jnp.zeros_like(gb)
    go[...] = jnp.zeros_like(go)
    lax.fori_loop(0, 8, sums_part, 0)
    for t in range(16):
        cols = slice(128 * t, 128 * t + 128)
        sv[t] = jnp.sum(gb[:, cols], axis=0, keepdims=True)
        sv[16 + t] = jnp.sum(go[:, cols], axis=0, keepdims=True)

    def send_small(i, carry):
        p = (dp + i) % 32
        where = {"dp_0": p // 8, "dp_1": (p // 2) % 4, "dp_2": p % 2, "mp": z}
        pltpu.make_async_remote_copy(
            src_ref=sv.at[p], dst_ref=rv.at[dp], send_sem=bulk.at[2],
            recv_sem=bulk.at[3], device_id=where, device_id_type=MESH,
        ).start()
        return carry

    lax.fori_loop(1, 32, send_small, 0)
    rv[dp] = sv[dp]

    h1a.wait_recv()
    for k in range(2):
        SB[k, yr, :, HI] = (fac[k, yr, c, :, HI] + RL[1, 0, k].astype(F32)).astype(BF16)
    h1e = go_to(SB.at[0:2, yr, :, HI], RV.at[1, 0, 0:2], {"dp_1": yr})
    h1b.wait_recv()
    for k in range(2):
        SB[2 + k, yl, :, HI] = (fac[2 + k, yl, c, :, HI] + RL[1, 1, k].astype(F32)).astype(BF16)
    h1f = go_to(SB.at[2:4, yl, :, HI], RV.at[1, 1, 2:4], {"dp_1": yl})
    aa.fifth()

    def ring(h, axis, n):
        nr, nl, no = (n + 1) % 4, (n + 3) % 4, (n + 2) % 4
        s1 = go_to(Q.at[h, no, 0:16], RL2.at[h, 0], {axis: nr})
        s2 = go_to(Q.at[h, no, 16:32], RL2.at[h, 1], {axis: nl})
        s3 = go_to(Q.at[h, nr, 16:32], RV2.at[h, 0, 16:32], {axis: nr})
        s4 = go_to(Q.at[h, nl, 0:16], RV2.at[h, 1, 0:16], {axis: nl})
        return nr, nl, (s1, s2, s3, s4)

    def ring_relay(h, axis, state):
        nr, nl, (s1, s2, s3, s4) = state
        s1.wait_recv()
        Q[h, nr, 0:16] = Q[h, nr, 0:16] + RL2[h, 0]
        s5 = go_to(Q.at[h, nr, 0:16], RV2.at[h, 0, 0:16], {axis: nr})
        s2.wait_recv()
        Q[h, nl, 16:32] = Q[h, nl, 16:32] + RL2[h, 1]
        s6 = go_to(Q.at[h, nl, 16:32], RV2.at[h, 1, 16:32], {axis: nl})
        return s3, s4, s5, s6

    def segment(first, last):
        def pair(k, carry):
            lane = iota((256, 128), 1)
            block = DPL[:, pl.ds(pl.multiple_of(k * 128, 128), 128)]
            turned = pltpu.roll(block, 64, 1)
            hots, rows = [], []
            for side in range(2):
                slot = slot_rows(lookups_ref[pl.ds(2 * k + side, 1), :], starts, ends)
                slot = as_column(slot)
                sixteen = jnp.floor(slot * (1.0 / 16.0))
                both = jnp.floor(slot * (1.0 / 32.0))
                upper = sixteen - 2.0 * both
                hots.append(tiles_over_lanes(slot - 16.0 * (sixteen - both), 16))
                same = jnp.where((lane < 64) == (side == 0), block, turned)
                kept = jnp.where((lane >= 64) == (upper > 0.5), same, 0.0)
                rows.append(kept.astype(BF16))
            acc[...] += mm(jnp.concatenate(rows, axis=0), jnp.concatenate(hots, axis=0), 0, 0)
            return carry

        lax.fori_loop(first, last, pair, 0)

    def rows_of_table(first, last):
        def part(t, carry):
            lane = iota((256, 128), 1)
            block = arrived_ref[pl.ds(16 * t, 16)].reshape(256, 128).astype(F32)
            turned = pltpu.roll(block, 64, 1)
            hots, values = [], []
            for side in range(2):
                row = jnp.concatenate(
                    [lined[side, pl.ds(2 * t, 1), :], lined[side, pl.ds(2 * t + 1, 1), :]], axis=1
                )
                row = as_column(row)
                above = row >= 2048.0
                hots.append(tiles_over_lanes(jnp.where(above, row - 2048.0, row), 16))
                same = jnp.where((lane < 64) == (side == 0), block, turned)
                values.append(jnp.where((lane >= 64) == above, same, 0.0).astype(BF16))
            acc[...] += mm(
                jnp.concatenate(values, axis=0), jnp.concatenate(hots, axis=0), 0, 0
            )
            return carry

        lax.fori_loop(first, last, part, 0)

    for copy in (z3, z4, z5, z6):
        copy.wait_recv()
    DPL[...] = DPL[...] + (ZL[...].astype(F32) + ZR[...].astype(F32))
    acc[...] = jnp.zeros_like(acc)
    segment(0, 2)
    for copy in (h0c, h0d, h0e, h0f):
        copy.wait_recv()
    for k in range(4):
        Q[0, k] = fac[x, k, c, :, LO] + (RV[0, 0, k].astype(F32) + RV[0, 1, k].astype(F32))
    t0 = ring(0, "dp_1", y)
    segment(2, 4)
    for copy in (h1c, h1d, h1e, h1f):
        copy.wait_recv()
    for k in range(4):
        Q[1, k] = fac[k, y, c, :, HI] + (RV[1, 0, k].astype(F32) + RV[1, 1, k].astype(F32))
    t1 = ring(1, "dp_0", x)
    u0 = ring_relay(0, "dp_1", t0)
    segment(4, 6)
    u1 = ring_relay(1, "dp_0", t1)
    segment(6, 8)
    few = jnp.zeros((8, 128), F32)
    for t in range(16):
        piece = acc[:, 128 * t : 128 * t + 128]
        few = few + jnp.sum((piece * piece).reshape(16, 8, 128), axis=0)
        slots[8 * t : 8 * t + 8] = piece.T.astype(BF16).reshape(8, 16, 128)

    def send_slots(p):
        pltpu.make_async_remote_copy(
            src_ref=slots.at[p], dst_ref=arrived_ref.at[me], send_sem=bulk.at[4],
            recv_sem=bulk.at[5], device_id=p, device_id_type=LOGICAL,
        ).start()

    to_all(me, send_slots)
    arrived_ref[me] = slots[me]

    for copy in u0 + u1:
        copy.wait_recv()
    lower = Q[0, y] + (RV2[0, 0] + RV2[0, 1])
    upper = Q[1, x] + (RV2[1, 0] + RV2[1, 1])
    grad_ref[:, LO] = lower
    grad_ref[:, HI] = upper
    GA[x, y, c, :, LO] = lower.astype(BF16)
    GA[x, y, c, :, HI] = upper.astype(BF16)
    ga = Flow(GA, go_to, (x, y, c, z), ga_out, wsem.at[1])
    ga.start()
    both = lower * lower + upper * upper
    both = jnp.sum(both.reshape(4, 8, 1024), axis=0)
    for t in range(8):
        few = few + both[:, 128 * t : 128 * t + 128]
    small = sv.at[pl.ds(0, 31)]
    pltpu.make_async_copy(small, small, bulk.at[2]).wait()
    pltpu.make_async_copy(small, small, bulk.at[3]).wait()
    bias_sum = jnp.sum(rv[...], axis=0)
    ns[...] = jnp.sum(few, axis=0, keepdims=True) + bias_sum * bias_sum

    def send_norm(p):
        pltpu.make_async_remote_copy(
            src_ref=ns, dst_ref=NR.at[me], send_sem=bulk.at[6],
            recv_sem=bulk.at[7], device_id=p, device_id_type=LOGICAL,
        ).start()

    to_all(me, send_norm)
    put_grad = pltpu.make_async_copy(grad_ref, grad_out, local.at[10])
    put_grad.start()
    NR[me] = ns[...]
    ga.sides()

    heard = idsend.at[pl.ds(0, 127)]
    pltpu.make_async_copy(heard, heard, bulk.at[1]).wait()
    lane16 = iota((16, 128), 1) // 16
    numbers = rids_ref[...].astype(F32).reshape(16, 8, 128)
    for side in range(2):
        line = jnp.zeros((16, 128), F32)
        for d in range(8):
            shift = (16 * d - 16 * side) % 128
            line = jnp.where(lane16 == d, pltpu.roll(numbers[:, d, :], shift, 1), line)
        lined[side] = line
    acc[...] = jnp.zeros_like(acc)
    aa.last()
    ga.owns_on()
    many = arrived_ref.at[pl.ds(0, 127)]
    pltpu.make_async_copy(many, many, bulk.at[5]).wait()
    rows_of_table(0, 2)
    ga.opposites()
    ga.sides_on()
    rows_of_table(2, 5)
    ga.opposites_on()
    rows_of_table(5, 8)
    put_sums = pltpu.make_async_copy(acc, sums_out, local.at[11])
    put_sums.start()
    lot = NR.at[pl.ds(0, 127)]
    pltpu.make_async_copy(lot, lot, bulk.at[7]).wait()
    lanes = jnp.sum(NR[...], axis=0)
    norm = jnp.sum(lanes, axis=1, keepdims=True)
    scale = clip_norm / jnp.maximum(jnp.sqrt(norm), clip_norm)
    scale_ref[...] = jnp.broadcast_to(scale, (8, 128))
    put_scale = pltpu.make_async_copy(scale_ref, scale_out, local.at[12])
    put_scale.start()
    ga.finals()
    pltpu.make_async_copy(lot, lot, bulk.at[6]).wait()
    pltpu.make_async_copy(many, many, bulk.at[4]).wait()
    pltpu.make_async_copy(heard, heard, bulk.at[0]).wait()
    put_grad.wait()
    put_sums.wait()
    put_scale.wait()
    pltpu.make_async_copy(LR.at[0:3], LR.at[0:3], bulk.at[8]).wait()
    cp.drain(W)
    aa.close()
    ga.close()


def finish_kernel(
    sums_any, scale_ref, table_any, accum_any, grad_any, dense_any,
    ga_any, aa_any, w_any,
    new_any, accum_new_any, dense_new_any, wn_any,
    GA, AA, W, WN, sums, table, accum, grad, dense, new, accum_new, dense_new, sem, isem, osem,
):
    chunk = 128
    count = 1024 // chunk

    def load(i):
        rows = pl.ds(i * chunk, chunk)
        for j, (src, dst) in enumerate(((ga_any, GA), (aa_any, AA), (w_any, W))):
            pltpu.make_async_copy(src.at[rows], dst.at[rows], sem.at[i, j]).start()

    small = [
        pltpu.make_async_copy(src, dst, isem.at[k])
        for k, (src, dst) in enumerate(
            (
                (grad_any, grad), (dense_any, dense), (accum_any, accum),
                (sums_any, sums), (table_any, table),
            )
        )
    ]
    load(0)
    load(1)
    for copy in small:
        copy.start()
    for i in range(2, count):
        load(i)
    scale = scale_ref[0:1, 0:1]

    def part(t, carry):
        rows = pl.ds(pl.multiple_of(t * chunk, chunk), chunk)
        for j, (src, dst) in enumerate(((ga_any, GA), (aa_any, AA), (w_any, W))):
            pltpu.make_async_copy(src.at[rows], dst.at[rows], sem.at[t, j]).wait()
        for q in range(16):
            cols = slice(128 * q, 128 * q + 128)
            g = scale * GA[rows, cols].astype(F32)
            r = lax.rsqrt(AA[rows, cols].astype(F32) + g * g)
            r = r - (adagrad_eps * r) * r
            WN[rows, cols] = (W[rows, cols].astype(F32) - (dense_rate * g) * r).astype(BF16)
        pltpu.make_async_copy(WN.at[rows], wn_any.at[rows], osem.at[0]).start()
        return carry

    lax.fori_loop(0, count, part, 0)
    for copy in small:
        copy.wait()
    clipped = scale * grad[...]
    dense_new[...] = dense[...] + clipped * clipped
    puts = [pltpu.make_async_copy(dense_new, dense_new_any, osem.at[1])]
    puts[0].start()
    for upper in range(2):
        for p in range(16):
            r = sums[64 * upper : 64 * upper + 64, 128 * p : 128 * p + 128] * scale
            line = p + upper * 16
            fresh = accum[line : line + 1, :] + jnp.sum(r * r, axis=0, keepdims=True) / 64.0
            accum_new[line : line + 1, :] = fresh
            at = line * 128
            rate = table_rate / (jnp.sqrt(fresh) + adagrad_eps)
            new[:, at : at + 128] = table[:, at : at + 128] - r * rate
        cols = pl.ds(2048 * upper, 2048)
        puts.append(
            pltpu.make_async_copy(new.at[:, cols], new_any.at[:, cols], osem.at[2 + upper])
        )
        puts[-1].start()
    puts.append(pltpu.make_async_copy(accum_new, accum_new_any, osem.at[4]))
    puts[-1].start()
    pltpu.make_async_copy(WN, wn_any, osem.at[0]).wait()
    for copy in puts:
        copy.wait()


def shape(dims, kind):
    return jax.ShapeDtypeStruct(dims, kind)


def body(
    slab_values,
    row_ids,
    peer_counts,
    lookup_slots,
    labels,
    sample_weight,
    weight_in,
    bias_in,
    weight_out,
    dense_accum,
    table_rows,
    table_accum,
):
    V = pltpu.VMEM
    DMA = pltpu.SemaphoreType.DMA
    whole = (4, 4, 2, 32, 2048)
    ga, aa, sums, scale, grad = pl.pallas_call(
        step_kernel,
        out_shape=(
            shape(whole, BF16), shape(whole, BF16), shape((128, 2048), F32),
            shape((8, 128), F32), shape((32, 2048), F32),
        ),
        in_specs=[ANY] * 10,
        out_specs=(ANY,) * 5,
        scratch_shapes=[
            V((16, 256), I32), V((1, 128), I32), V((128, 2048), BF16), V((32, 128), I32),
            V((8, 128), I32), V((8, 128), F32), V((1, 2048), F32), V((16, 128), BF16),
            V((128, 16, 128), BF16), V((128, 1, 128), I32), V((8, 128), F32), V((32, 2048), F32),
            V((2, 16, 128), F32),
            V((1024, 2048), BF16), V((32, 2048), F32), V((128, 1, 128), I32),
            V((1024, 1024), BF16), V(whole, F32), V((1024, 2048), BF16),
            V((1024, 2048), BF16), V((256, 128), F32), V((8, 128), F32), V((4, 8, 128), F32),
            V((8, 128), F32), V((8, 2048), F32), V((8, 2048), F32),
            V((32, 1, 128), F32), V((32, 1, 128), F32),
            V((3, 256, 1024), BF16), V((2, 128, 1024), F32),
            V((128, 1024), BF16), V((128, 1024), BF16),
            V((256, 1024), BF16), V((256, 1024), BF16), V((256, 1024), F32),
            V((4, 4, 32, 2048), F32), V((4, 4, 32, 2048), BF16),
            V((2, 2, 2, 32, 1024), BF16), V((2, 2, 4, 32, 1024), BF16),
            V((2, 4, 32, 1024), F32), V((2, 2, 16, 1024), F32), V((2, 2, 32, 1024), F32),
            V(whole, BF16), V(whole, BF16), V((128, 2048), F32), V((128, 16, 128), BF16),
            V((1, 128), F32), V((128, 1, 128), F32), V((1024, 1024), BF16),
            V((2048, 128), BF16), V((1, 2048), F32), V((2048, 128), F32),
            DMA((5,)), DMA((N_COPIES,)), DMA((9,)), DMA((13,)), DMA((2,)),
        ],
        compiler_params=pltpu.CompilerParams(
            has_side_effects=True, vmem_limit_bytes=63 * 1024 * 1024, collective_id=0
        ),
        name="step",
    )(
        lookup_slots.T,
        peer_counts,
        slab_values[0],
        row_ids[0].T,
        labels.reshape(8, 128),
        sample_weight.reshape(8, 128),
        bias_in.reshape(1, 2048),
        weight_out.reshape(16, 128),
        weight_in,
        dense_accum,
    )
    table_new, table_accum_new, accum_new, weight_new = pl.pallas_call(
        finish_kernel,
        out_shape=(
            shape((64, 4096), F32), shape((32, 128), F32), shape((32, 2048), F32),
            shape((1024, 2048), BF16),
        ),
        in_specs=[ANY, VM] + [ANY] * 7,
        out_specs=(ANY,) * 4,
        scratch_shapes=[
            V((1024, 2048), BF16), V((1024, 2048), BF16), V((1024, 2048), BF16),
            V((1024, 2048), BF16), V((128, 2048), F32), V((64, 4096), F32), V((32, 128), F32),
            V((32, 2048), F32), V((32, 2048), F32), V((64, 4096), F32), V((32, 128), F32),
            V((32, 2048), F32), DMA((8, 3)), DMA((5,)), DMA((5,)),
        ],
        name="finish",
    )(
        sums,
        scale,
        table_rows.T,
        table_accum.reshape(32, 128),
        grad,
        dense_accum,
        ga.reshape(1024, 2048),
        aa.reshape(1024, 2048),
        weight_in,
    )
    return (weight_new, accum_new, table_new.T, table_accum_new.reshape(4096))


def solution(mesh):
    torus = Mesh(mesh.devices.reshape(4, 4, 2, mesh.shape["mp"]), ("dp_0", "dp_1", "dp_2", "mp"))
    placed = (
        P(DP_MP, None, None),
        P(DP_MP, None, None),
        P(DP_MP, None),
        P(DP_MP, None),
        P(DP),
        P(DP),
        P(None, "mp"),
        P("mp"),
        P("mp"),
        P(DP, "mp"),
        P(DP_MP, None),
        P(DP_MP),
    )
    return jax.shard_map(
        body,
        mesh=torus,
        in_specs=placed,
        out_specs=(P(None, "mp"), P(DP, "mp"), P(DP_MP, None), P(DP_MP)),
        check_vma=False,
    )
```
